32 devices in a mesh: dp: 4 (over y, z), ws: 8 (over x, core).
Axes of the slice: x: 4, y: 2, z: 2, core: 2. Of those that a mesh axis runs over, the one named last changes fastest.
The devices are a block of a 4x4x8 slice.
Arguments:
- hidden: bfloat16 [512, 768], P(('dp', 'ws')), parts along dimension 0
- self_k: bfloat16 [512, 12, 384, 64], P(('dp', 'ws')), parts along dimension 0
- self_v: bfloat16 [512, 12, 384, 64], P(('dp', 'ws')), parts along dimension 0
- cross_k: bfloat16 [512, 12, 192, 64], P(('dp', 'ws')), parts along dimension 0
- cross_v: bfloat16 [512, 12, 192, 64], P(('dp', 'ws')), parts along dimension 0
- positions: int32 [512], P(('dp', 'ws')), parts along dimension 0
- enc_mask: int32 [512, 192], P(('dp', 'ws')), parts along dimension 0
- rel_bias: float32 [12, 384], replicated
- expert_idx: int32 [512], P(('dp', 'ws')), parts along dimension 0
- ln_self: float32 [768], replicated
- ln_cross: float32 [768], replicated
- ln_ffn: float32 [768], replicated
- wq_self: bfloat16 [768, 768], P(None, 'ws')
- wk_self: bfloat16 [768, 768], P(None, 'ws')
- wv_self: bfloat16 [768, 768], P(None, 'ws')
- wo_self: bfloat16 [768, 768], P(None, 'ws')
- wq_cross: bfloat16 [768, 768], P(None, 'ws')
- wo_cross: bfloat16 [768, 768], P(None, 'ws')
- w_router: float32 [768, 8], P(None, 'ws')
- w_in: bfloat16 [8, 768, 3072], P(None, None, 'ws')
- w_out: bfloat16 [8, 3072, 768], P(None, 'ws')
Outputs:
- output 1: bfloat16 [512, 768], P(('dp', 'ws')), parts along dimension 0
- output 2: bfloat16 [512, 12, 384, 64], P(('dp', 'ws')), parts along dimension 0
- output 3: bfloat16 [512, 12, 384, 64], P(('dp', 'ws')), parts along dimension 0
There are 4 independent parts. The reference program is written for one: setup_inputs(seed, part) draws one part's arguments, and reference() takes and returns one part's arrays. A program takes and returns all parts, laid end to end along the dimension named above; an argument that names none is the same for every part.
All inputs are finite; a program needn't handle non-finite values.
Results may differ from the reference program's by a relative error of at most 0.0115161.
Values are sent between devices in bfloat16 or wider.
A program may use at most 768 MiB of HBM per device.

```python
import jax
import jax.numpy as jnp
from jax import lax

D_MODEL = 768
NUM_HEADS = 12
HEAD_DIM = 64
D_FF = 3072
EXPERTS = 8
CACHE_LEN = 384
SRC_LEN = 192
GROUP_ROWS = 128

ATTN_WIDTH = NUM_HEADS * HEAD_DIM
CAPACITY = (2 * GROUP_ROWS + EXPERTS - 1) // EXPERTS
EPSILON = 1e-6
NEG_BIG = -1e30


def scaled_normal(key, shape, scale):
    return (jax.random.normal(key, shape, jnp.float32) * scale).astype(jnp.bfloat16)


def setup_inputs(seed: int = 0, part: int = 0) -> dict:
    base_key = jax.random.key(seed)
    shared = jax.random.split(base_key, 13)
    part_keys = jax.random.split(jax.random.fold_in(base_key, part), 12)
    row_ids = jnp.arange(GROUP_ROWS)
    cache_shape = (GROUP_ROWS, NUM_HEADS, CACHE_LEN, HEAD_DIM)
    src_shape = (GROUP_ROWS, NUM_HEADS, SRC_LEN, HEAD_DIM)
    hidden = scaled_normal(part_keys[0], (GROUP_ROWS, D_MODEL), 1.0)
    self_k = scaled_normal(part_keys[1], cache_shape, 1.0)
    self_v = scaled_normal(part_keys[2], cache_shape, 1.0)
    cross_k = scaled_normal(part_keys[3], src_shape, 1.0)
    cross_v = scaled_normal(part_keys[4], src_shape, 1.0)
    positions = jax.random.randint(part_keys[5], (GROUP_ROWS,), 0, CACHE_LEN)
    last_row = jax.random.randint(part_keys[6], (), 0, GROUP_ROWS)
    positions = jnp.where(row_ids == last_row, CACHE_LEN - 1, positions).astype(jnp.int32)
    src_lens = jax.random.randint(part_keys[7], (GROUP_ROWS,), 1, SRC_LEN + 1)
    full_row = jax.random.randint(part_keys[8], (), 0, GROUP_ROWS)
    src_lens = jnp.where(row_ids == full_row, SRC_LEN, src_lens)
    enc_mask = (jnp.arange(SRC_LEN)[None, :] < src_lens[:, None]).astype(jnp.int32)
    hot_expert = jax.random.randint(part_keys[9], (), 0, EXPERTS)
    free_pick = jax.random.randint(part_keys[10], (GROUP_ROWS,), 0, EXPERTS)
    row_order = jax.random.permutation(part_keys[11], GROUP_ROWS)
    hot_rows = jnp.zeros((GROUP_ROWS,), jnp.int32).at[row_order[:CAPACITY + 1]].set(1)
    expert_idx = jnp.where(hot_rows == 1, hot_expert, free_pick).astype(jnp.int32)
    return {
        'hidden': hidden,
        'self_k': self_k,
        'self_v': self_v,
        'cross_k': cross_k,
        'cross_v': cross_v,
        'positions': positions,
        'enc_mask': enc_mask,
        'rel_bias': jax.random.normal(shared[0], (NUM_HEADS, CACHE_LEN), jnp.float32),
        'expert_idx': expert_idx,
        'ln_self': jax.random.uniform(shared[1], (D_MODEL,), jnp.float32, 0.5, 1.5),
        'ln_cross': jax.random.uniform(shared[2], (D_MODEL,), jnp.float32, 0.5, 1.5),
        'ln_ffn': jax.random.uniform(shared[3], (D_MODEL,), jnp.float32, 0.5, 1.5),
        'wq_self': scaled_normal(shared[4], (D_MODEL, ATTN_WIDTH), 1.5 * (D_MODEL * HEAD_DIM) ** -0.5),
        'wk_self': scaled_normal(shared[5], (D_MODEL, ATTN_WIDTH), D_MODEL ** -0.5),
        'wv_self': scaled_normal(shared[6], (D_MODEL, ATTN_WIDTH), D_MODEL ** -0.5),
        'wo_self': scaled_normal(shared[7], (ATTN_WIDTH, D_MODEL), ATTN_WIDTH ** -0.5),
        'wq_cross': scaled_normal(shared[8], (D_MODEL, ATTN_WIDTH), 1.5 * (D_MODEL * HEAD_DIM) ** -0.5),
        'wo_cross': scaled_normal(shared[9], (ATTN_WIDTH, D_MODEL), ATTN_WIDTH ** -0.5),
        'w_router': jax.random.normal(shared[10], (D_MODEL, EXPERTS), jnp.float32) * D_MODEL ** -0.5,
        'w_in': scaled_normal(shared[11], (EXPERTS, D_MODEL, D_FF), D_MODEL ** -0.5),
        'w_out': scaled_normal(shared[12], (EXPERTS, D_FF, D_MODEL), (EXPERTS / D_FF) ** 0.5),
    }


def rms_norm(hidden, scale):
    hid_f32 = hidden.astype(jnp.float32)
    inv_rms = lax.rsqrt(jnp.mean(hid_f32 * hid_f32, axis=-1, keepdims=True) + EPSILON)
    return (hid_f32 * inv_rms * scale).astype(jnp.bfloat16)


def attend_row(row_args):
    queries, cache_keys, cache_vals, score_bias = row_args
    scores = jnp.einsum('hd,hld->hl', queries.astype(jnp.float32), cache_keys.astype(jnp.float32)) + score_bias
    attn_probs = jax.nn.softmax(scores, axis=-1).astype(jnp.bfloat16)
    context = jnp.einsum('hl,hld->hd', attn_probs.astype(jnp.float32), cache_vals.astype(jnp.float32))
    return context.astype(jnp.bfloat16)


def project(x_norm, weight):
    return jnp.dot(x_norm, weight, preferred_element_type=jnp.float32).astype(jnp.bfloat16)


def reference(hidden, self_k, self_v, cross_k, cross_v, positions, enc_mask, rel_bias, expert_idx,
              ln_self, ln_cross, ln_ffn, wq_self, wk_self, wv_self, wo_self, wq_cross, wo_cross,
              w_router, w_in, w_out):
    head_shape = (GROUP_ROWS, NUM_HEADS, HEAD_DIM)
    x_norm = rms_norm(hidden, ln_self)
    queries = project(x_norm, wq_self).reshape(head_shape)
    k_new = project(x_norm, wk_self).reshape(head_shape)
    v_new = project(x_norm, wv_self).reshape(head_shape)
    distance = positions[:, None] - jnp.arange(CACHE_LEN)[None, :]
    write_mask = (distance == 0)[:, None, :, None]
    new_self_k = jnp.where(write_mask, k_new[:, :, None, :], self_k)
    new_self_v = jnp.where(write_mask, v_new[:, :, None, :], self_v)
    pos_bias = jnp.take(rel_bias, jnp.clip(distance, 0, CACHE_LEN - 1), axis=1)
    pos_bias = jnp.where(distance[None] >= 0, pos_bias, NEG_BIG).transpose(1, 0, 2)
    context = lax.map(attend_row, (queries, new_self_k, new_self_v, pos_bias))
    attn_out = jnp.dot(context.reshape(GROUP_ROWS, ATTN_WIDTH), wo_self, preferred_element_type=jnp.float32)
    after_self = (hidden.astype(jnp.float32) + attn_out).astype(jnp.bfloat16)

    x_norm = rms_norm(after_self, ln_cross)
    queries = project(x_norm, wq_cross).reshape(head_shape)
    mask_bias = jnp.where(enc_mask == 1, 0.0, NEG_BIG)[:, None, :]
    context = lax.map(attend_row, (queries, cross_k, cross_v, mask_bias))
    attn_out = jnp.dot(context.reshape(GROUP_ROWS, ATTN_WIDTH), wo_cross, preferred_element_type=jnp.float32)
    after_cross = (after_self.astype(jnp.float32) + attn_out).astype(jnp.bfloat16)

    x_norm = rms_norm(after_cross, ln_ffn)
    logits = jnp.dot(x_norm.astype(jnp.float32), w_router, precision=lax.Precision.HIGHEST,
                     preferred_element_type=jnp.float32)
    router_probs = jax.nn.softmax(logits, axis=-1)
    chosen = jnp.arange(EXPERTS)[None, :] == expert_idx[:, None]
    gate_val = jnp.sum(jnp.where(chosen, router_probs, 0.0), axis=-1)
    row_ids = jnp.arange(GROUP_ROWS)
    earlier = (expert_idx[None, :] == expert_idx[:, None]) & (row_ids[None, :] < row_ids[:, None])
    slot_idx = jnp.sum(earlier.astype(jnp.int32), axis=1)
    keep_gate = jnp.where(slot_idx < CAPACITY, gate_val, 0.0)

    def expert_row(row_args):
        x_row, expert = row_args
        ffn_hidden = jnp.dot(x_row[None, :], w_in[expert], preferred_element_type=jnp.float32)
        ffn_hidden = jax.nn.relu(ffn_hidden).astype(jnp.bfloat16)
        ffn_out = jnp.dot(ffn_hidden, w_out[expert], preferred_element_type=jnp.float32)
        return ffn_out.astype(jnp.bfloat16)[0]

    expert_out = lax.map(expert_row, (x_norm, expert_idx))
    hidden_out = (after_cross.astype(jnp.float32) + expert_out.astype(jnp.float32) * keep_gate[:, None]).astype(jnp.bfloat16)
    return (hidden_out, new_self_k, new_self_v)
```

```python
import functools
import jax
import jax.numpy as jnp
from jax import lax
from jax.experimental import pallas as pl
from jax.experimental.pallas import tpu as pltpu
from jax.sharding import PartitionSpec as P

EPSILON = 1e-6
NEG_BIG = -1e30
F32, BF16 = jnp.float32, jnp.bfloat16
MESH = pl.DeviceIdType.MESH
ANY = pl.BlockSpec(memory_space=pl.ANY)
VM = pl.BlockSpec(memory_space=pltpu.VMEM)
HBM = pl.BlockSpec(memory_space=pltpu.HBM)
SM = pl.BlockSpec(memory_space=pltpu.SMEM)
NT = (((1,), (1,)), ((), ()))
PEERS = ((2, 0), (2, 1), (1, 0), (3, 0), (1, 1), (3, 1), (0, 1))
UNROLL = 4


def rms_norm(hid_f32, scale):
    inv_rms = lax.rsqrt(jnp.mean(hid_f32 * hid_f32, axis=-1, keepdims=True) + EPSILON)
    return (hid_f32 * inv_rms * scale).astype(BF16)


def dot_nt(a, b):
    return lax.dot_general(a, b, NT, preferred_element_type=F32)


def softmax_rows(scores):
    top = jnp.max(scores, axis=-1, keepdims=True)
    ex = jnp.exp(scores - top)
    return (ex / jnp.sum(ex, axis=-1, keepdims=True)).astype(BF16)


def make_dev(n):
    me = lax.axis_index('ws')
    chips = n // 2
    chip, core = me // 2, lax.rem(me, 2)

    def dev(step, other):
        return 2 * lax.rem(chip + step, chips) + ((1 - core) if other else core)
    return me, dev


def remote(src, dst, send_sem, recv_sem, dev):
    return pltpu.make_async_remote_copy(src_ref=src, dst_ref=dst, send_sem=send_sem, recv_sem=recv_sem,
                                        device_id={'ws': dev}, device_id_type=MESH)


def head_mask(heads_pad, width, head_dim):
    row = lax.broadcasted_iota(jnp.int32, (heads_pad, width), 0)
    col = lax.broadcasted_iota(jnp.int32, (heads_pad, width), 1)
    return (col // head_dim == row).astype(F32)


def proj_kernel(n, hid_hbm, ln_hbm, wq_hbm, wk_hbm, wv_hbm, wo_hbm, wqc_hbm, woc_hbm, k_hbm, v_hbm, ck_hbm, cv_hbm,
                qkv_ref, wall_ref, k_ref, v_ref, ck_ref, cv_ref,
                xall_ref, ln_ref, wqkv_ref, qsend_ref, qrecv_ref,
                in_sem, big_sem, x_send, x_recv, q_send, q_recv, w_send, w_recv):
    me, dev = make_dev(n)
    rows, width = hid_hbm.shape
    share = width // n
    half = share // 2
    piece = share + half

    barrier = pltpu.get_barrier_semaphore()
    for peer in PEERS:
        pl.semaphore_signal(barrier, inc=1, device_id={'ws': dev(*peer)}, device_id_type=MESH)

    mine = wall_ref.at[me]
    loads = [
        (hid_hbm, xall_ref.at[me]), (ln_hbm, ln_ref), (wq_hbm, wqkv_ref.at[0]), (wk_hbm, wqkv_ref.at[1]),
        (wv_hbm, wqkv_ref.at[2]),
        (wo_hbm, mine.at[pl.ds(0, share)]), (woc_hbm.at[pl.ds(0, half)], mine.at[pl.ds(share, half)]),
        (wqc_hbm, mine.at[pl.ds(piece, share)]),
        (woc_hbm.at[pl.ds(half, half)], mine.at[pl.ds(piece + share, half)]),
    ]
    loads = [pltpu.make_async_copy(src, dst, in_sem.at[i]) for i, (src, dst) in enumerate(loads)]
    for load in loads:
        load.start()
    big = [pltpu.make_async_copy(src, dst, big_sem.at[i]) for i, (src, dst) in
           enumerate([(k_hbm, k_ref), (v_hbm, v_ref), (ck_hbm, ck_ref), (cv_hbm, cv_ref)])]

    loads[0].wait()
    pl.semaphore_wait(barrier, n - 1)
    x_out = [remote(xall_ref.at[me], xall_ref.at[me], x_send.at[i], x_recv.at[me], dev(*peer))
             for i, peer in enumerate(PEERS)]
    for copy in x_out:
        copy.start()

    right, left, far, sib = dev(1, 0), dev(3, 0), dev(2, 0), dev(0, 1)
    w_out = []

    def send_piece(owner, part, target):
        block = wall_ref.at[owner, pl.ds(part * piece, piece)]
        copy = remote(block, block, w_send.at[len(w_out)], w_recv.at[owner, part], target)
        copy.start()
        w_out.append(copy)

    def wait_piece(owner, part):
        block = wall_ref.at[owner, pl.ds(part * piece, piece)]
        remote(block, block, w_send.at[0], w_recv.at[owner, part], sib).wait_recv()

    for load in loads[5:]:
        load.wait()
    send_piece(me, 0, right)
    send_piece(me, 1, left)
    for load in big:
        load.start()
    qsend_ref[...] = jnp.zeros_like(qsend_ref)

    for load in loads[1:5]:
        load.wait()
    for peer in PEERS:
        src = dev(*peer)
        remote(xall_ref.at[src], xall_ref.at[src], x_send.at[0], x_recv.at[src], src).wait_recv()
    x_norm = rms_norm(xall_ref[...].reshape(n * rows, width).astype(F32), ln_ref[...])
    for part in range(3):
        qsend_ref[:, part * 128:part * 128 + share] = dot_nt(x_norm, wqkv_ref[part]).astype(BF16)
    q_out = []
    for i, peer in enumerate(PEERS):
        dst = dev(*peer)
        q_out.append(remote(qsend_ref.at[pl.ds(dst * rows, rows)], qrecv_ref.at[me], q_send.at[i], q_recv.at[me], dst))
    for copy in q_out:
        copy.start()
    qrecv_ref[me] = qsend_ref[pl.ds(pl.multiple_of(me * rows, rows), rows), :]
    send_piece(me, 1, right)
    send_piece(me, 0, left)
    send_piece(me, 0, sib)
    send_piece(me, 1, sib)

    wait_piece(left, 0)
    send_piece(left, 0, right)
    wait_piece(right, 1)
    send_piece(right, 1, left)
    send_piece(left, 0, sib)
    send_piece(right, 1, sib)

    for peer in PEERS:
        src = dev(*peer)
        remote(qrecv_ref.at[src], qrecv_ref.at[src], q_send.at[0], q_recv.at[src], src).wait_recv()
    for part in range(3):
        qkv_ref[part] = jnp.concatenate([qrecv_ref[s][:, part * 128:part * 128 + share] for s in range(n)],
                                        axis=1).astype(F32)

    wait_piece(left, 1)
    send_piece(left, 1, sib)
    wait_piece(right, 0)
    send_piece(right, 0, sib)
    wait_piece(far, 0)
    send_piece(far, 0, sib)
    wait_piece(far, 1)
    send_piece(far, 1, sib)
    for step in range(n // 2):
        src = dev(step, 1)
        wait_piece(src, 0)
        wait_piece(src, 1)
    for load in big:
        load.wait()
    for copy in x_out + q_out + w_out:
        copy.wait_send()


def self_kernel(head_dim, pos_ref, qkv_ref, rel_ref, k_ref, v_ref, win_hbm, wout_hbm,
                newk_hbm, newv_hbm, ctx_ref, win_ref, wout_ref,
                kt_ref, vt_ref, kp_ref, vp_ref, s_ref, p_ref, ctx32_ref, rrev_ref, w_sem, k_sem, v_sem):
    rows, width, length = k_ref.shape
    heads_pad = s_ref.shape[1]
    steps = rows // UNROLL
    tiles = length // 128
    w_loads = [pltpu.make_async_copy(win_hbm, win_ref, w_sem.at[0]),
               pltpu.make_async_copy(wout_hbm, wout_ref, w_sem.at[1])]

    rel = jnp.concatenate([rel_ref[...], jnp.zeros((heads_pad - rel_ref.shape[0], length), F32)], axis=0)
    flip = (lax.broadcasted_iota(jnp.int32, (length, length), 0) + lax.broadcasted_iota(jnp.int32, (length, length), 1)
            == length - 1).astype(F32).astype(BF16)
    hi = rel.astype(BF16)
    rest = rel - hi.astype(F32)
    mid = rest.astype(BF16)
    low = (rest - mid.astype(F32)).astype(BF16)
    rrev_ref[...] = (jnp.dot(hi, flip, preferred_element_type=F32) + jnp.dot(mid, flip, preferred_element_type=F32)
                     + jnp.dot(low, flip, preferred_element_type=F32))
    pad = jnp.zeros((128 - rows, width), F32)
    kt_ref[...] = jnp.concatenate([qkv_ref[1], pad], axis=0).T
    vt_ref[...] = jnp.concatenate([qkv_ref[2], pad], axis=0).T

    h_mask = head_mask(heads_pad, width, head_dim)
    lane = lax.broadcasted_iota(jnp.int32, (1, length), 1)
    lane_tile = lax.broadcasted_iota(jnp.int32, (1, 128), 1)

    def out_copies(b, old_ref, patch_ref, new_hbm, sem):
        tile = pos_ref[b] // 128
        copies = []
        for k in range(tiles):
            cols = pl.ds(pl.multiple_of(lax.rem(tile + k, tiles) * 128, 128), 128)
            src = patch_ref.at[b] if k == 0 else old_ref.at[b, :, cols]
            copies.append(pltpu.make_async_copy(src, new_hbm.at[b, :, cols], sem.at[b, k]))
        return copies

    def put_row(b, column, old_ref, patch_ref, new_hbm, sem):
        pos = pos_ref[b]
        first = pl.multiple_of(pos // 128 * 128, 128)
        patch_ref[b] = jnp.where(lane_tile == pos - first, jnp.broadcast_to(column, (width, 128)).astype(BF16),
                                 old_ref[b, :, pl.ds(first, 128)])
        for copy in out_copies(b, old_ref, patch_ref, new_hbm, sem):
            copy.start()

    def score_step(i, carry):
        kt = kt_ref[...]
        for s in range(UNROLL):
            b = i * UNROLL + s
            put_row(b, kt[:, s:s + 1], k_ref, kp_ref, newk_hbm, k_sem)
            pos = pos_ref[b]
            q_diag = qkv_ref[0, pl.ds(b, 1), :] * h_mask
            scores = jnp.dot(q_diag.astype(BF16), k_ref[b], preferred_element_type=F32)
            new = jnp.sum(q_diag * qkv_ref[1, pl.ds(b, 1), :], axis=1, keepdims=True)
            bias = pltpu.roll(rrev_ref[...], pos + 1, axis=1)
            s_ref[b] = jnp.where(lane <= pos, jnp.where(lane == pos, new, scores) + bias, NEG_BIG)
        kt_ref[...] = pltpu.roll(kt, 128 - UNROLL, axis=1)
        return carry
    lax.fori_loop(0, steps, score_step, 0)
    for load in w_loads:
        load.start()

    p_ref[...] = softmax_rows(s_ref[...])

    def value_step(i, carry):
        vt = vt_ref[...]
        for s in range(UNROLL):
            b = i * UNROLL + s
            put_row(b, vt[:, s:s + 1], v_ref, vp_ref, newv_hbm, v_sem)
            here = lane == pos_ref[b]
            probs = p_ref[b].astype(F32)
            new = jnp.sum(jnp.where(here, probs, 0.0), axis=1, keepdims=True)
            spread = dot_nt(jnp.where(here, 0.0, probs).astype(BF16), v_ref[b])
            spread = spread + new * qkv_ref[2, pl.ds(b, 1), :]
            ctx32_ref[pl.ds(b, 1), :] = jnp.sum(spread * h_mask, axis=0, keepdims=True)
        vt_ref[...] = pltpu.roll(vt, 128 - UNROLL, axis=1)
        return carry
    lax.fori_loop(0, steps, value_step, 0)
    ctx_ref[...] = ctx32_ref[...].astype(BF16)

    def drain(b, carry):
        for copy in (out_copies(b, k_ref, kp_ref, newk_hbm, k_sem) + out_copies(b, v_ref, vp_ref, newv_hbm, v_sem)):
            copy.wait()
        return carry
    lax.fori_loop(0, rows, drain, 0)
    for load in w_loads:
        load.wait()


def cross_kernel(n, head_dim, capacity, eidx_ref, ctx_ref, wall_ref, hid_hbm, lnc_hbm, lnf_hbm, mask_hbm, wr_hbm,
                 k_ref, v_ref, win_ref, wout_ref,
                 out_ref,
                 hid_ref, lnc_ref, lnf_ref, mask_ref, wr_ref, eall_ref, q_ref, s_ref,
                 p_ref, ctx32_ref, xall_ref, u_ref, part_ref, rs_ref,
                 in_sem, r_send, r_recv, e_send, e_recv, x_send, x_recv, rs_send, rs_recv):
    me, dev = make_dev(n)
    rows, width, length = k_ref.shape
    heads_pad = s_ref.shape[1]
    share = width // n
    half = share // 2
    piece = share + half
    steps = rows // UNROLL
    experts = win_ref.shape[0]

    barrier = pltpu.get_barrier_semaphore()
    for peer in PEERS:
        pl.semaphore_signal(barrier, inc=1, device_id={'ws': dev(*peer)}, device_id_type=MESH)
    loads = [(hid_hbm, hid_ref), (lnc_hbm, lnc_ref), (lnf_hbm, lnf_ref), (mask_hbm, mask_ref), (wr_hbm, wr_ref.at[me])]
    loads = [pltpu.make_async_copy(src, dst, in_sem.at[i]) for i, (src, dst) in enumerate(loads)]
    for load in loads:
        load.start()

    row_id = lax.broadcasted_iota(jnp.int32, (rows, 128), 0)
    e_own = jnp.zeros((rows, 128), jnp.int32)
    for b in range(rows):
        e_own = jnp.where(row_id == b, eidx_ref[b], e_own)
    eall_ref[me] = e_own

    loads[0].wait()
    wo = wall_ref[:, 0:share, :].reshape(width, width)
    h1 = (hid_ref[...].astype(F32) + dot_nt(ctx_ref[...], wo)).astype(BF16).astype(F32)
    loads[1].wait()
    wqc = wall_ref[:, piece:piece + share, :].reshape(width, width)
    q_ref[...] = dot_nt(rms_norm(h1, lnc_ref[...]), wqc).astype(BF16).astype(F32)

    loads[4].wait()
    pl.semaphore_wait(barrier, n - 1)
    sends = []
    for i, peer in enumerate(PEERS):
        dst = dev(*peer)
        sends.append(remote(wr_ref.at[me], wr_ref.at[me], r_send.at[i], r_recv.at[me], dst))
        sends.append(remote(eall_ref.at[me], eall_ref.at[me], e_send.at[i], e_recv.at[me], dst))
    for copy in sends:
        copy.start()

    h_mask = head_mask(heads_pad, width, head_dim)
    loads[3].wait()

    def score_step(i, carry):
        for s in range(UNROLL):
            b = i * UNROLL + s
            q_diag = (q_ref[pl.ds(b, 1), :] * h_mask).astype(BF16)
            scores = jnp.dot(q_diag, k_ref[b], preferred_element_type=F32)
            s_ref[b] = jnp.where(mask_ref[pl.ds(b, 1), :] == 1, scores, NEG_BIG)
        return carry
    lax.fori_loop(0, steps, score_step, 0)
    p_ref[...] = softmax_rows(s_ref[...])

    def value_step(i, carry):
        for s in range(UNROLL):
            b = i * UNROLL + s
            spread = dot_nt(p_ref[b], v_ref[b])
            ctx32_ref[pl.ds(b, 1), :] = jnp.sum(spread * h_mask, axis=0, keepdims=True)
        return carry
    lax.fori_loop(0, steps, value_step, 0)

    woc = jnp.concatenate([wall_ref[:, share:piece, :], wall_ref[:, piece + share:2 * piece, :]], axis=1)
    woc = woc.reshape(width, width)
    h2 = (h1 + dot_nt(ctx32_ref[...].astype(BF16), woc)).astype(BF16).astype(F32)
    loads[2].wait()
    x_own = rms_norm(h2, lnf_ref[...])
    xall_ref[me] = x_own
    x_out = [remote(xall_ref.at[me], xall_ref.at[me], x_send.at[i], x_recv.at[me], dev(*peer))
             for i, peer in enumerate(PEERS)]
    for copy in x_out:
        copy.start()

    for peer in PEERS:
        src = dev(*peer)
        remote(wr_ref.at[src], wr_ref.at[src], r_send.at[0], r_recv.at[src], src).wait_recv()
        remote(eall_ref.at[src], eall_ref.at[src], e_send.at[0], e_recv.at[src], src).wait_recv()
    x_f32 = x_own.astype(F32)
    logits = [jnp.sum(x_f32 * wr_ref[e], axis=-1, keepdims=True) for e in range(experts)]
    top = functools.reduce(jnp.maximum, logits)
    ex = [jnp.exp(v - top) for v in logits]
    total = functools.reduce(jnp.add, ex)
    e_col = e_own[:, 0:1]
    gate = functools.reduce(jnp.add, [jnp.where(e_col == e, ex[e], 0.0) for e in range(experts)]) / total
    e_all = eall_ref[...].reshape(n * rows, 128)
    one_hot = (e_all == lax.broadcasted_iota(jnp.int32, (n * rows, 128), 1)).astype(F32).astype(BF16)
    earlier = (lax.broadcasted_iota(jnp.int32, (rows, n * rows), 1)
               < me * rows + lax.broadcasted_iota(jnp.int32, (rows, n * rows), 0)).astype(F32).astype(BF16)
    counts = jnp.dot(earlier, one_hot, preferred_element_type=F32)
    slot = jnp.sum(jnp.where(lax.broadcasted_iota(jnp.int32, (rows, 128), 1) == e_own, counts, 0.0), axis=-1,
                   keepdims=True)
    keep_gate = jnp.where(slot < capacity, gate, 0.0)

    for peer in PEERS:
        src = dev(*peer)
        remote(xall_ref.at[src], xall_ref.at[src], x_send.at[0], x_recv.at[src], src).wait_recv()
    x_all = xall_ref[...].reshape(n * rows, width)
    e_wide = jnp.concatenate([e_all] * (win_ref.shape[2] // 128), axis=1)

    def expert_step(e, carry):
        u = jnp.maximum(jnp.dot(x_all, win_ref[e], preferred_element_type=F32), 0.0)
        u_ref[e] = jnp.where(e_wide == e, u, 0.0).astype(BF16)
        return carry
    lax.fori_loop(0, experts, expert_step, 0)

    chunk = part_ref.shape[2]
    rs_out = []
    for c in range(width // chunk):
        acc = jnp.zeros((n * rows, chunk), F32)
        for e in range(experts):
            acc = acc + jnp.dot(u_ref[e], wout_ref[e, :, c * chunk:(c + 1) * chunk], preferred_element_type=F32)
        part_ref[c] = acc
        rs_ref[me, c] = part_ref[c, pl.ds(pl.multiple_of(me * rows, rows), rows), :]
        for i, peer in enumerate(PEERS):
            dst = dev(*peer)
            copy = remote(part_ref.at[c, pl.ds(dst * rows, rows)], rs_ref.at[me, c], rs_send.at[c, i],
                          rs_recv.at[c, me], dst)
            copy.start()
            rs_out.append(copy)
    for c in range(width // chunk):
        for peer in PEERS:
            src = dev(*peer)
            remote(rs_ref.at[src, c], rs_ref.at[src, c], rs_send.at[c, 0], rs_recv.at[c, src], src).wait_recv()
        y = jnp.sum(rs_ref[:, c], axis=0).astype(BF16).astype(F32)
        cols = slice(c * chunk, (c + 1) * chunk)
        out_ref[:, cols] = (h2[:, cols] + y * keep_gate).astype(BF16)
    for copy in sends + x_out + rs_out:
        copy.wait_send()


def solution(mesh):
    n = mesh.shape['ws']
    row_axes = ('dp', 'ws')
    row_vec = P(row_axes)
    row_mat = P(row_axes, None)
    cache_spec = P(row_axes, None, None, None)
    col_split = P(None, 'ws')
    in_specs = (row_mat, cache_spec, cache_spec, cache_spec, cache_spec, row_vec, row_mat, P(None, None), row_vec,
                P(None), P(None), P(None), col_split, col_split, col_split, col_split, col_split, col_split,
                col_split, P(None, None, 'ws'), P(None, 'ws', None))
    out_specs = (row_mat, cache_spec, cache_spec)

    def decoder_block(hidden, self_k, self_v, cross_k, cross_v, positions, enc_mask, rel_bias, expert_idx,
                      ln_self, ln_cross, ln_ffn, wq_self, wk_self, wv_self, wo_self, wq_cross, wo_cross,
                      w_router, w_in, w_out):
        rows, width = hidden.shape
        heads, length, head_dim = self_k.shape[1:]
        src_len = cross_k.shape[2]
        share = width // n
        heads_pad = -(-heads // 16) * 16
        experts, _, units = w_in.shape
        capacity = (2 * rows * n + experts - 1) // experts
        chunk = 256

        def flat(cache):
            return jnp.swapaxes(cache, 2, 3).reshape(rows, width, cache.shape[2])

        dma = pltpu.SemaphoreType.DMA
        qkv, wall, kv_k, kv_v, c_k, c_v = pl.pallas_call(
            functools.partial(proj_kernel, n),
            out_shape=(pltpu.VMEM((3, rows, width), F32), pltpu.VMEM((n, 3 * share, width), BF16),
                       pltpu.VMEM((rows, width, length), BF16), pltpu.VMEM((rows, width, length), BF16),
                       pltpu.VMEM((rows, width, src_len), BF16), pltpu.VMEM((rows, width, src_len), BF16)),
            in_specs=[HBM] * 12,
            out_specs=(VM,) * 6,
            scratch_shapes=[
                pltpu.VMEM((n, rows, width), BF16), pltpu.VMEM((1, width), F32), pltpu.VMEM((3, share, width), BF16),
                pltpu.VMEM((n * rows, 384), BF16), pltpu.VMEM((n, rows, 384), BF16),
                dma((9,)), dma((4,)), dma((7,)), dma((n,)), dma((7,)), dma((n,)), dma((14,)), dma((n, 2)),
            ],
            compiler_params=pltpu.CompilerParams(collective_id=0, has_side_effects=True,
                                                 vmem_limit_bytes=6 * 2 ** 20),
            name='proj_part',
        )(hidden, ln_self.reshape(1, width), wq_self.T, wk_self.T, wv_self.T, wo_self.T, wq_cross.T, wo_cross.T,
          flat(self_k), flat(self_v), flat(cross_k), flat(cross_v))

        newk, newv, ctx, win_v, wout_v = pl.pallas_call(
            functools.partial(self_kernel, head_dim),
            out_shape=(pltpu.HBM((rows, width, length), BF16), pltpu.HBM((rows, width, length), BF16),
                       pltpu.VMEM((rows, width), BF16), pltpu.VMEM(w_in.shape, BF16), pltpu.VMEM(w_out.shape, BF16)),
            in_specs=[SM, VM, VM, VM, VM, HBM, HBM],
            out_specs=(HBM, HBM, VM, VM, VM),
            scratch_shapes=[
                pltpu.VMEM((width, 128), F32), pltpu.VMEM((width, 128), F32), pltpu.VMEM((rows, width, 128), BF16),
                pltpu.VMEM((rows, width, 128), BF16), pltpu.VMEM((rows, heads_pad, length), F32),
                pltpu.VMEM((rows, heads_pad, length), BF16), pltpu.VMEM((rows, width), F32),
                pltpu.VMEM((heads_pad, length), F32),
                dma((2,)), dma((rows, length // 128)), dma((rows, length // 128)),
            ],
            compiler_params=pltpu.CompilerParams(has_side_effects=True, vmem_limit_bytes=12 * 2 ** 20),
            name='self_part',
        )(positions, qkv, rel_bias, kv_k, kv_v, w_in, w_out)

        out = pl.pallas_call(
            functools.partial(cross_kernel, n, head_dim, capacity),
            out_shape=jax.ShapeDtypeStruct((rows, width), BF16),
            in_specs=[SM, VM, VM] + [ANY] * 5 + [VM] * 4,
            out_specs=VM,
            scratch_shapes=[
                pltpu.VMEM((rows, width), BF16), pltpu.VMEM((1, width), F32), pltpu.VMEM((1, width), F32),
                pltpu.VMEM((rows, src_len), jnp.int32), pltpu.VMEM((n, 1, width), F32),
                pltpu.VMEM((n, rows, 128), jnp.int32), pltpu.VMEM((rows, width), F32),
                pltpu.VMEM((rows, heads_pad, src_len), F32), pltpu.VMEM((rows, heads_pad, src_len), BF16),
                pltpu.VMEM((rows, width), F32), pltpu.VMEM((n, rows, width), BF16),
                pltpu.VMEM((experts, n * rows, units), BF16), pltpu.VMEM((width // chunk, n * rows, chunk), F32),
                pltpu.VMEM((n, width // chunk, rows, chunk), F32),
                dma((5,)), dma((7,)), dma((n,)), dma((7,)), dma((n,)), dma((7,)),
                dma((n,)), dma((width // chunk, 7)), dma((width // chunk, n)),
            ],
            compiler_params=pltpu.CompilerParams(collective_id=1, has_side_effects=True,
                                                 vmem_limit_bytes=14 * 2 ** 20),
            name='cross_part',
        )(expert_idx, ctx, wall, hidden, ln_cross.reshape(1, width), ln_ffn.reshape(1, width), enc_mask, w_router.T,
          c_k, c_v, win_v, wout_v)

        def unflat(cache):
            return jnp.swapaxes(cache.reshape(rows, heads, head_dim, length), 2, 3)
        return out, unflat(newk), unflat(newv)

    return jax.shard_map(decoder_block, mesh=mesh, in_specs=in_specs, out_specs=out_specs, check_vma=False)
```

```python
import functools
import jax
import jax.numpy as jnp
from jax import lax
from jax.experimental import pallas as pl
from jax.experimental.pallas import tpu as pltpu
from jax.sharding import PartitionSpec as P

EPSILON = 1e-6
NEG_BIG = -1e30
F32, BF16 = jnp.float32, jnp.bfloat16
MESH = pl.DeviceIdType.MESH
VM = pl.BlockSpec(memory_space=pltpu.VMEM)
HBM = pl.BlockSpec(memory_space=pltpu.HBM)
SM = pl.BlockSpec(memory_space=pltpu.SMEM)
NT = (((1,), (1,)), ((), ()))
PEERS = ((2, 0), (2, 1), (1, 0), (3, 0), (1, 1), (3, 1), (0, 1))
UNROLL = 4


def in_hbm(*arrays):
    return [pltpu.with_memory_space_constraint(a, pltpu.HBM) for a in arrays]


def in_vmem(*arrays):
    return [pltpu.with_memory_space_constraint(a, pltpu.VMEM) for a in arrays]


def rms_norm(hid_f32, scale):
    inv_rms = lax.rsqrt(jnp.mean(hid_f32 * hid_f32, axis=-1, keepdims=True) + EPSILON)
    return (hid_f32 * inv_rms * scale).astype(BF16)


def dot_nt(a, b):
    return lax.dot_general(a, b, NT, preferred_element_type=F32)


def softmax_rows(scores):
    top = jnp.max(scores, axis=-1, keepdims=True)
    ex = jnp.exp(scores - top)
    return (ex / jnp.sum(ex, axis=-1, keepdims=True)).astype(BF16)


def make_dev(n):
    me = lax.axis_index('ws')
    chips = n // 2
    chip, core = me // 2, lax.rem(me, 2)

    def dev(step, other):
        return 2 * lax.rem(chip + step, chips) + ((1 - core) if other else core)
    return me, dev


def remote(src, dst, send_sem, recv_sem, dev):
    return pltpu.make_async_remote_copy(src_ref=src, dst_ref=dst, send_sem=send_sem, recv_sem=recv_sem,
                                        device_id={'ws': dev}, device_id_type=MESH)


def head_mask(heads_pad, width, head_dim):
    row = lax.broadcasted_iota(jnp.int32, (heads_pad, width), 0)
    col = lax.broadcasted_iota(jnp.int32, (heads_pad, width), 1)
    return (col // head_dim == row).astype(F32)


def proj_kernel(n, hid_hbm, ln_hbm, wq_hbm, wk_hbm, wv_hbm, wo_hbm, wqc_hbm, woc_hbm, k_hbm, v_hbm, ck_hbm, cv_hbm,
                qkv_ref, wall_ref, k_ref, v_ref, ck_ref, cv_ref,
                xall_ref, ln_ref, wqkv_ref, qsend_ref, qrecv_ref,
                in_sem, big_sem, x_send, x_recv, q_send, q_recv, w_send, w_recv):
    me, dev = make_dev(n)
    rows, width = hid_hbm.shape
    share = width // n
    half = share // 2
    piece = share + half

    barrier = pltpu.get_barrier_semaphore()
    for peer in PEERS:
        pl.semaphore_signal(barrier, inc=1, device_id={'ws': dev(*peer)}, device_id_type=MESH)

    mine = wall_ref.at[me]
    loads = [
        (hid_hbm, xall_ref.at[me]), (ln_hbm, ln_ref), (wq_hbm, wqkv_ref.at[0]), (wk_hbm, wqkv_ref.at[1]),
        (wv_hbm, wqkv_ref.at[2]),
        (wo_hbm, mine.at[pl.ds(0, share)]), (woc_hbm.at[pl.ds(0, half)], mine.at[pl.ds(share, half)]),
        (wqc_hbm, mine.at[pl.ds(piece, share)]),
        (woc_hbm.at[pl.ds(half, half)], mine.at[pl.ds(piece + share, half)]),
    ]
    loads = [pltpu.make_async_copy(src, dst, in_sem.at[i]) for i, (src, dst) in enumerate(loads)]
    for load in loads:
        load.start()
    big = [pltpu.make_async_copy(src, dst, big_sem.at[i]) for i, (src, dst) in
           enumerate([(k_hbm, k_ref), (v_hbm, v_ref), (ck_hbm, ck_ref), (cv_hbm, cv_ref)])]

    loads[0].wait()
    pl.semaphore_wait(barrier, n - 1)
    x_out = [remote(xall_ref.at[me], xall_ref.at[me], x_send.at[i], x_recv.at[me], dev(*peer))
             for i, peer in enumerate(PEERS)]
    for copy in x_out:
        copy.start()

    right, left, far, sib = dev(1, 0), dev(3, 0), dev(2, 0), dev(0, 1)
    w_out = []

    def send_piece(owner, part, target):
        block = wall_ref.at[owner, pl.ds(part * piece, piece)]
        copy = remote(block, block, w_send.at[len(w_out)], w_recv.at[owner, part], target)
        copy.start()
        w_out.append(copy)

    def wait_piece(owner, part):
        block = wall_ref.at[owner, pl.ds(part * piece, piece)]
        remote(block, block, w_send.at[0], w_recv.at[owner, part], sib).wait_recv()

    for load in loads[5:]:
        load.wait()
    send_piece(me, 0, right)
    send_piece(me, 1, left)
    for load in big:
        load.start()
    qsend_ref[...] = jnp.zeros_like(qsend_ref)

    for load in loads[1:5]:
        load.wait()
    for peer in PEERS:
        src = dev(*peer)
        remote(xall_ref.at[src], xall_ref.at[src], x_send.at[0], x_recv.at[src], src).wait_recv()
    x_norm = rms_norm(xall_ref[...].reshape(n * rows, width).astype(F32), ln_ref[...][None])
    for part in range(3):
        qsend_ref[:, part * 128:part * 128 + share] = dot_nt(x_norm, wqkv_ref[part]).astype(BF16)
    q_out = []
    for i, peer in enumerate(PEERS):
        dst = dev(*peer)
        q_out.append(remote(qsend_ref.at[pl.ds(dst * rows, rows)], qrecv_ref.at[me], q_send.at[i], q_recv.at[me], dst))
    for copy in q_out:
        copy.start()
    qrecv_ref[me] = qsend_ref[pl.ds(pl.multiple_of(me * rows, rows), rows), :]
    send_piece(me, 1, right)
    send_piece(me, 0, left)
    send_piece(me, 0, sib)
    send_piece(me, 1, sib)

    wait_piece(left, 0)
    send_piece(left, 0, right)
    wait_piece(right, 1)
    send_piece(right, 1, left)
    send_piece(left, 0, sib)
    send_piece(right, 1, sib)

    for peer in PEERS:
        src = dev(*peer)
        remote(qrecv_ref.at[src], qrecv_ref.at[src], q_send.at[0], q_recv.at[src], src).wait_recv()
    for part in range(3):
        qkv_ref[part] = jnp.concatenate([qrecv_ref[s][:, part * 128:part * 128 + share] for s in range(n)],
                                        axis=1).astype(F32)

    wait_piece(left, 1)
    send_piece(left, 1, sib)
    wait_piece(right, 0)
    send_piece(right, 0, sib)
    wait_piece(far, 0)
    send_piece(far, 0, sib)
    wait_piece(far, 1)
    send_piece(far, 1, sib)
    for step in range(n // 2):
        src = dev(step, 1)
        wait_piece(src, 0)
        wait_piece(src, 1)
    for load in big:
        load.wait()
    for copy in x_out + q_out + w_out:
        copy.wait_send()


def self_kernel(head_dim, pos_ref, qkv_ref, rel_hbm, k_ref, v_ref, win_hbm, wout_hbm,
                newk_hbm, newv_hbm, ctx_ref, win_ref, wout_ref,
                kt_ref, vt_ref, kp_ref, vp_ref, s_ref, p_ref, ctx32_ref, rrev_ref, rel_ref, w_sem, k_sem, v_sem):
    rows, width, length = k_ref.shape
    heads_pad = s_ref.shape[1]
    steps = rows // UNROLL
    tiles = length // 128
    w_loads = [pltpu.make_async_copy(win_hbm, win_ref, w_sem.at[0]),
               pltpu.make_async_copy(wout_hbm, wout_ref, w_sem.at[1])]
    rel_load = pltpu.make_async_copy(rel_hbm, rel_ref, w_sem.at[2])
    rel_load.start()
    pad = jnp.zeros((128 - rows, width), F32)
    kt_ref[...] = jnp.concatenate([qkv_ref[1], pad], axis=0).T
    vt_ref[...] = jnp.concatenate([qkv_ref[2], pad], axis=0).T
    rel_load.wait()

    rel = jnp.concatenate([rel_ref[...], jnp.zeros((heads_pad - rel_ref.shape[0], length), F32)], axis=0)
    flip = (lax.broadcasted_iota(jnp.int32, (length, length), 0) + lax.broadcasted_iota(jnp.int32, (length, length), 1)
            == length - 1).astype(F32).astype(BF16)
    hi = rel.astype(BF16)
    rest = rel - hi.astype(F32)
    mid = rest.astype(BF16)
    low = (rest - mid.astype(F32)).astype(BF16)
    rrev_ref[...] = (jnp.dot(hi, flip, preferred_element_type=F32) + jnp.dot(mid, flip, preferred_element_type=F32)
                     + jnp.dot(low, flip, preferred_element_type=F32))

    h_mask = head_mask(heads_pad, width, head_dim)
    lane = lax.broadcasted_iota(jnp.int32, (1, length), 1)
    lane_tile = lax.broadcasted_iota(jnp.int32, (1, 128), 1)

    def out_copies(b, old_ref, patch_ref, new_hbm, sem):
        tile = pos_ref[b] // 128
        copies = []
        for k in range(tiles):
            cols = pl.ds(pl.multiple_of(lax.rem(tile + k, tiles) * 128, 128), 128)
            src = patch_ref.at[b] if k == 0 else old_ref.at[b, :, cols]
            copies.append(pltpu.make_async_copy(src, new_hbm.at[b, :, cols], sem.at[b, k]))
        return copies

    def put_row(b, column, old_ref, patch_ref, new_hbm, sem):
        pos = pos_ref[b]
        first = pl.multiple_of(pos // 128 * 128, 128)
        patch_ref[b] = jnp.where(lane_tile == pos - first, jnp.broadcast_to(column, (width, 128)).astype(BF16),
                                 old_ref[b, :, pl.ds(first, 128)])
        for copy in out_copies(b, old_ref, patch_ref, new_hbm, sem):
            copy.start()

    def score_step(i, carry):
        kt = kt_ref[...]
        for s in range(UNROLL):
            b = i * UNROLL + s
            put_row(b, kt[:, s:s + 1], k_ref, kp_ref, newk_hbm, k_sem)
            pos = pos_ref[b]
            q_diag = qkv_ref[0, pl.ds(b, 1), :] * h_mask
            scores = jnp.dot(q_diag.astype(BF16), k_ref[b], preferred_element_type=F32)
            new = jnp.sum(q_diag * qkv_ref[1, pl.ds(b, 1), :], axis=1, keepdims=True)
            bias = pltpu.roll(rrev_ref[...], pos + 1, axis=1)
            s_ref[b] = jnp.where(lane <= pos, jnp.where(lane == pos, new, scores) + bias, NEG_BIG)
        kt_ref[...] = pltpu.roll(kt, 128 - UNROLL, axis=1)
        return carry
    lax.fori_loop(0, steps, score_step, 0)
    for load in w_loads:
        load.start()

    p_ref[...] = softmax_rows(s_ref[...])

    def value_step(i, carry):
        vt = vt_ref[...]
        for s in range(UNROLL):
            b = i * UNROLL + s
            put_row(b, vt[:, s:s + 1], v_ref, vp_ref, newv_hbm, v_sem)
            here = lane == pos_ref[b]
            probs = p_ref[b].astype(F32)
            new = jnp.sum(jnp.where(here, probs, 0.0), axis=1, keepdims=True)
            spread = dot_nt(jnp.where(here, 0.0, probs).astype(BF16), v_ref[b])
            spread = spread + new * qkv_ref[2, pl.ds(b, 1), :]
            ctx32_ref[pl.ds(b, 1), :] = jnp.sum(spread * h_mask, axis=0, keepdims=True)
        vt_ref[...] = pltpu.roll(vt, 128 - UNROLL, axis=1)
        return carry
    lax.fori_loop(0, steps, value_step, 0)
    ctx_ref[...] = ctx32_ref[...].astype(BF16)

    def drain(b, carry):
        for copy in (out_copies(b, k_ref, kp_ref, newk_hbm, k_sem) + out_copies(b, v_ref, vp_ref, newv_hbm, v_sem)):
            copy.wait()
        return carry
    lax.fori_loop(0, rows, drain, 0)
    for load in w_loads:
        load.wait()


def cross_kernel(n, head_dim, capacity, eidx_ref, ctx_ref, wall_ref, hid_hbm, lnc_hbm, lnf_hbm, mask_hbm, wr_hbm,
                 k_ref, v_ref, win_ref, wout_ref,
                 out_ref,
                 hid_ref, lnc_ref, lnf_ref, mask_ref, wr_ref, eall_ref, q_ref, s_ref,
                 p_ref, ctx32_ref, xall_ref, u_ref, part_ref, rs_ref,
                 in_sem, r_send, r_recv, e_send, e_recv, x_send, x_recv, rs_send, rs_recv):
    me, dev = make_dev(n)
    rows, width, length = k_ref.shape
    heads_pad = s_ref.shape[1]
    share = width // n
    half = share // 2
    piece = share + half
    steps = rows // UNROLL
    experts = win_ref.shape[0]

    barrier = pltpu.get_barrier_semaphore()
    for peer in PEERS:
        pl.semaphore_signal(barrier, inc=1, device_id={'ws': dev(*peer)}, device_id_type=MESH)
    loads = [(hid_hbm, hid_ref), (lnc_hbm, lnc_ref), (lnf_hbm, lnf_ref), (mask_hbm, mask_ref), (wr_hbm, wr_ref.at[me])]
    loads = [pltpu.make_async_copy(src, dst, in_sem.at[i]) for i, (src, dst) in enumerate(loads)]
    for load in loads:
        load.start()

    row_id = lax.broadcasted_iota(jnp.int32, (rows, 128), 0)
    e_own = jnp.zeros((rows, 128), jnp.int32)
    for b in range(rows):
        e_own = jnp.where(row_id == b, eidx_ref[b], e_own)
    eall_ref[me] = e_own

    loads[0].wait()
    wo = wall_ref[:, 0:share, :].reshape(width, width)
    h1 = (hid_ref[...].astype(F32) + dot_nt(ctx_ref[...], wo)).astype(BF16).astype(F32)
    loads[1].wait()
    wqc = wall_ref[:, piece:piece + share, :].reshape(width, width)
    q_ref[...] = dot_nt(rms_norm(h1, lnc_ref[...][None]), wqc).astype(BF16).astype(F32)

    loads[4].wait()
    pl.semaphore_wait(barrier, n - 1)
    sends = []
    for i, peer in enumerate(PEERS):
        dst = dev(*peer)
        sends.append(remote(wr_ref.at[me], wr_ref.at[me], r_send.at[i], r_recv.at[me], dst))
        sends.append(remote(eall_ref.at[me], eall_ref.at[me], e_send.at[i], e_recv.at[me], dst))
    for copy in sends:
        copy.start()

    h_mask = head_mask(heads_pad, width, head_dim)
    loads[3].wait()

    def score_step(i, carry):
        for s in range(UNROLL):
            b = i * UNROLL + s
            q_diag = (q_ref[pl.ds(b, 1), :] * h_mask).astype(BF16)
            scores = jnp.dot(q_diag, k_ref[b], preferred_element_type=F32)
            s_ref[b] = jnp.where(mask_ref[pl.ds(b, 1), :] == 1, scores, NEG_BIG)
        return carry
    lax.fori_loop(0, steps, score_step, 0)
    p_ref[...] = softmax_rows(s_ref[...])

    def value_step(i, carry):
        for s in range(UNROLL):
            b = i * UNROLL + s
            spread = dot_nt(p_ref[b], v_ref[b])
            ctx32_ref[pl.ds(b, 1), :] = jnp.sum(spread * h_mask, axis=0, keepdims=True)
        return carry
    lax.fori_loop(0, steps, value_step, 0)

    woc = jnp.concatenate([wall_ref[:, share:piece, :], wall_ref[:, piece + share:2 * piece, :]], axis=1)
    woc = woc.reshape(width, width)
    h2 = (h1 + dot_nt(ctx32_ref[...].astype(BF16), woc)).astype(BF16).astype(F32)
    loads[2].wait()
    x_own = rms_norm(h2, lnf_ref[...][None])
    xall_ref[me] = x_own
    x_out = [remote(xall_ref.at[me], xall_ref.at[me], x_send.at[i], x_recv.at[me], dev(*peer))
             for i, peer in enumerate(PEERS)]
    for copy in x_out:
        copy.start()

    for peer in PEERS:
        src = dev(*peer)
        remote(wr_ref.at[src], wr_ref.at[src], r_send.at[0], r_recv.at[src], src).wait_recv()
        remote(eall_ref.at[src], eall_ref.at[src], e_send.at[0], e_recv.at[src], src).wait_recv()
    x_f32 = x_own.astype(F32)
    logits = [jnp.sum(x_f32 * wr_ref[e], axis=-1, keepdims=True) for e in range(experts)]
    top = functools.reduce(jnp.maximum, logits)
    ex = [jnp.exp(v - top) for v in logits]
    total = functools.reduce(jnp.add, ex)
    e_col = e_own[:, 0:1]
    gate = functools.reduce(jnp.add, [jnp.where(e_col == e, ex[e], 0.0) for e in range(experts)]) / total
    e_all = eall_ref[...].reshape(n * rows, 128)
    one_hot = (e_all == lax.broadcasted_iota(jnp.int32, (n * rows, 128), 1)).astype(F32).astype(BF16)
    earlier = (lax.broadcasted_iota(jnp.int32, (rows, n * rows), 1)
               < me * rows + lax.broadcasted_iota(jnp.int32, (rows, n * rows), 0)).astype(F32).astype(BF16)
    counts = jnp.dot(earlier, one_hot, preferred_element_type=F32)
    slot = jnp.sum(jnp.where(lax.broadcasted_iota(jnp.int32, (rows, 128), 1) == e_own, counts, 0.0), axis=-1,
                   keepdims=True)
    keep_gate = jnp.where(slot < capacity, gate, 0.0)

    for peer in PEERS:
        src = dev(*peer)
        remote(xall_ref.at[src], xall_ref.at[src], x_send.at[0], x_recv.at[src], src).wait_recv()
    x_all = xall_ref[...].reshape(n * rows, width)
    e_wide = jnp.concatenate([e_all] * (win_ref.shape[2] // 128), axis=1)

    def expert_step(e, carry):
        u = jnp.maximum(jnp.dot(x_all, win_ref[e], preferred_element_type=F32), 0.0)
        u_ref[e] = jnp.where(e_wide == e, u, 0.0).astype(BF16)
        return carry
    lax.fori_loop(0, experts, expert_step, 0)

    chunk = part_ref.shape[2]
    rs_out = []
    for c in range(width // chunk):
        acc = jnp.zeros((n * rows, chunk), F32)
        for e in range(experts):
            acc = acc + jnp.dot(u_ref[e], wout_ref[e, :, c * chunk:(c + 1) * chunk], preferred_element_type=F32)
        part_ref[c] = acc
        rs_ref[me, c] = part_ref[c, pl.ds(pl.multiple_of(me * rows, rows), rows), :]
        for i, peer in enumerate(PEERS):
            dst = dev(*peer)
            copy = remote(part_ref.at[c, pl.ds(dst * rows, rows)], rs_ref.at[me, c], rs_send.at[c, i],
                          rs_recv.at[c, me], dst)
            copy.start()
            rs_out.append(copy)
    for c in range(width // chunk):
        for peer in PEERS:
            src = dev(*peer)
            remote(rs_ref.at[src, c], rs_ref.at[src, c], rs_send.at[c, 0], rs_recv.at[c, src], src).wait_recv()
        y = jnp.sum(rs_ref[:, c], axis=0).astype(BF16).astype(F32)
        cols = slice(c * chunk, (c + 1) * chunk)
        out_ref[:, cols] = (h2[:, cols] + y * keep_gate).astype(BF16)
    for copy in sends + x_out + rs_out:
        copy.wait_send()


def solution(mesh):
    n = mesh.shape['ws']
    row_axes = ('dp', 'ws')
    row_vec = P(row_axes)
    row_mat = P(row_axes, None)
    cache_spec = P(row_axes, None, None, None)
    col_split = P(None, 'ws')
    in_specs = (row_mat, cache_spec, cache_spec, cache_spec, cache_spec, row_vec, row_mat, P(None, None), row_vec,
                P(None), P(None), P(None), col_split, col_split, col_split, col_split, col_split, col_split,
                col_split, P(None, None, 'ws'), P(None, 'ws', None))
    out_specs = (row_mat, cache_spec, cache_spec)

    def decoder_block(hidden, self_k, self_v, cross_k, cross_v, positions, enc_mask, rel_bias, expert_idx,
                      ln_self, ln_cross, ln_ffn, wq_self, wk_self, wv_self, wo_self, wq_cross, wo_cross,
                      w_router, w_in, w_out):
        rows, width = hidden.shape
        heads, length, head_dim = self_k.shape[1:]
        src_len = cross_k.shape[2]
        share = width // n
        heads_pad = -(-heads // 16) * 16
        experts, _, units = w_in.shape
        capacity = (2 * rows * n + experts - 1) // experts
        chunk = 256

        def flat(cache):
            return jnp.swapaxes(cache, 2, 3).reshape(rows, width, cache.shape[2])

        dma = pltpu.SemaphoreType.DMA
        qkv, wall, kv_k, kv_v, c_k, c_v = pl.pallas_call(
            functools.partial(proj_kernel, n),
            out_shape=(pltpu.VMEM((3, rows, width), F32), pltpu.VMEM((n, 3 * share, width), BF16),
                       pltpu.VMEM((rows, width, length), BF16), pltpu.VMEM((rows, width, length), BF16),
                       pltpu.VMEM((rows, width, src_len), BF16), pltpu.VMEM((rows, width, src_len), BF16)),
            in_specs=[HBM] * 12,
            out_specs=(VM,) * 6,
            scratch_shapes=[
                pltpu.VMEM((n, rows, width), BF16), pltpu.VMEM((width,), F32), pltpu.VMEM((3, share, width), BF16),
                pltpu.VMEM((n * rows, 384), BF16), pltpu.VMEM((n, rows, 384), BF16),
                dma((9,)), dma((4,)), dma((7,)), dma((n,)), dma((7,)), dma((n,)), dma((14,)), dma((n, 2)),
            ],
            compiler_params=pltpu.CompilerParams(collective_id=0, has_side_effects=True,
                                                 vmem_limit_bytes=6 * 2 ** 20),
            name='proj_part',
        )(*in_hbm(hidden, ln_self, wq_self.T, wk_self.T, wv_self.T, wo_self.T, wq_cross.T, wo_cross.T,
                  flat(self_k), flat(self_v), flat(cross_k), flat(cross_v)))

        newk, newv, ctx, win_v, wout_v = pl.pallas_call(
            functools.partial(self_kernel, head_dim),
            out_shape=(pltpu.HBM((rows, width, length), BF16), pltpu.HBM((rows, width, length), BF16),
                       pltpu.VMEM((rows, width), BF16), pltpu.VMEM(w_in.shape, BF16), pltpu.VMEM(w_out.shape, BF16)),
            in_specs=[SM, VM, HBM, VM, VM, HBM, HBM],
            out_specs=(HBM, HBM, VM, VM, VM),
            scratch_shapes=[
                pltpu.VMEM((width, 128), F32), pltpu.VMEM((width, 128), F32), pltpu.VMEM((rows, width, 128), BF16),
                pltpu.VMEM((rows, width, 128), BF16), pltpu.VMEM((rows, heads_pad, length), F32),
                pltpu.VMEM((rows, heads_pad, length), BF16), pltpu.VMEM((rows, width), F32),
                pltpu.VMEM((heads_pad, length), F32), pltpu.VMEM((heads, length), F32),
                dma((3,)), dma((rows, length // 128)), dma((rows, length // 128)),
            ],
            compiler_params=pltpu.CompilerParams(has_side_effects=True, vmem_limit_bytes=12 * 2 ** 20),
            name='self_part',
        )(positions, *in_vmem(qkv), *in_hbm(rel_bias), *in_vmem(kv_k, kv_v), *in_hbm(w_in, w_out))

        out = pl.pallas_call(
            functools.partial(cross_kernel, n, head_dim, capacity),
            out_shape=jax.ShapeDtypeStruct((rows, width), BF16),
            in_specs=[SM, VM, VM] + [HBM] * 5 + [VM] * 4,
            out_specs=VM,
            scratch_shapes=[
                pltpu.VMEM((rows, width), BF16), pltpu.VMEM((width,), F32), pltpu.VMEM((width,), F32),
                pltpu.VMEM((rows, src_len), jnp.int32), pltpu.VMEM((n, 1, width), F32),
                pltpu.VMEM((n, rows, 128), jnp.int32), pltpu.VMEM((rows, width), F32),
                pltpu.VMEM((rows, heads_pad, src_len), F32), pltpu.VMEM((rows, heads_pad, src_len), BF16),
                pltpu.VMEM((rows, width), F32), pltpu.VMEM((n, rows, width), BF16),
                pltpu.VMEM((experts, n * rows, units), BF16), pltpu.VMEM((width // chunk, n * rows, chunk), F32),
                pltpu.VMEM((n, width // chunk, rows, chunk), F32),
                dma((5,)), dma((7,)), dma((n,)), dma((7,)), dma((n,)), dma((7,)),
                dma((n,)), dma((width // chunk, 7)), dma((width // chunk, n)),
            ],
            compiler_params=pltpu.CompilerParams(collective_id=1, has_side_effects=True,
                                                 vmem_limit_bytes=14 * 2 ** 20),
            name='cross_part',
        )(expert_idx, *in_vmem(ctx, wall), *in_hbm(hidden, ln_cross, ln_ffn, enc_mask, w_router.T),
          *in_vmem(c_k, c_v, win_v, wout_v))

        def unflat(cache):
            return jnp.swapaxes(cache.reshape(rows, heads, head_dim, length), 2, 3)
        return out, unflat(newk), unflat(newv)

    return jax.shard_map(decoder_block, mesh=mesh, in_specs=in_specs, out_specs=out_specs, check_vma=False)
```

```python
import functools
import jax
import jax.numpy as jnp
from jax import lax
from jax.experimental import pallas as pl
from jax.experimental.pallas import tpu as pltpu
from jax.sharding import PartitionSpec as P

EPSILON = 1e-6
NEG_BIG = -1e30
F32, BF16 = jnp.float32, jnp.bfloat16
MESH = pl.DeviceIdType.MESH
VM = pl.BlockSpec(memory_space=pltpu.VMEM)
HBM = pl.BlockSpec(memory_space=pltpu.HBM)
SM = pl.BlockSpec(memory_space=pltpu.SMEM)
NT = (((1,), (1,)), ((), ()))
PEERS = ((2, 0), (2, 1), (1, 0), (3, 0), (1, 1), (3, 1), (0, 1))
UNROLL = 4


def in_hbm(*arrays):
    return [pltpu.with_memory_space_constraint(a, pltpu.HBM) for a in arrays]


def in_vmem(*arrays):
    return [pltpu.with_memory_space_constraint(a, pltpu.VMEM) for a in arrays]


def rms_norm(hid_f32, scale):
    inv_rms = lax.rsqrt(jnp.mean(hid_f32 * hid_f32, axis=-1, keepdims=True) + EPSILON)
    return (hid_f32 * inv_rms * scale).astype(BF16)


def dot_nt(a, b):
    return lax.dot_general(a, b, NT, preferred_element_type=F32)


def softmax_rows(scores):
    top = jnp.max(scores, axis=-1, keepdims=True)
    ex = jnp.exp(scores - top)
    return (ex / jnp.sum(ex, axis=-1, keepdims=True)).astype(BF16)


def make_dev(n):
    me = lax.axis_index('ws')
    chips = n // 2
    chip, core = me // 2, lax.rem(me, 2)

    def dev(step, other):
        return 2 * lax.rem(chip + step, chips) + ((1 - core) if other else core)
    return me, dev


def remote(src, dst, send_sem, recv_sem, dev):
    return pltpu.make_async_remote_copy(src_ref=src, dst_ref=dst, send_sem=send_sem, recv_sem=recv_sem,
                                        device_id={'ws': dev}, device_id_type=MESH)


def head_mask(heads_pad, width, head_dim):
    row = lax.broadcasted_iota(jnp.int32, (heads_pad, width), 0)
    col = lax.broadcasted_iota(jnp.int32, (heads_pad, width), 1)
    return (col // head_dim == row).astype(F32)


def self_kernel(n, head_dim, pos_ref, eidx_ref, hid_hbm, ln_hbm, rel_hbm, wr_hbm, wq_hbm, wk_hbm, wv_hbm, wo_hbm,
                wqc_hbm, woc_hbm, k_hbm, v_hbm, ck_hbm, cv_hbm, win_hbm, wout_hbm,
                ctx_ref, kv_ref, wall_ref, wr_ref, eall_ref, k_ref, v_ref, ck_ref, cv_ref, win_ref, wout_ref,
                xall_ref, ln_ref, rel_ref, wqkv_ref, qsend_ref, qrecv_ref, q_ref, s_ref, p_ref, ctx32_ref, rrev_ref,
                in_sem, k_sem, v_sem, big_sem, x_send, x_recv, r_send, r_recv, e_send, e_recv, q_send, q_recv,
                w_send, w_recv):
    me, dev = make_dev(n)
    rows, width, length = k_ref.shape
    heads_pad = s_ref.shape[1]
    share = width // n
    half = share // 2
    steps = rows // UNROLL
    pieces = ((0, share), (share, share), (2 * share, half), (2 * share + half, half))

    barrier = pltpu.get_barrier_semaphore()
    for peer in PEERS:
        pl.semaphore_signal(barrier, inc=1, device_id={'ws': dev(*peer)}, device_id_type=MESH)

    mine = wall_ref.at[me]
    loads = [
        (hid_hbm, xall_ref.at[me]), (wr_hbm, wr_ref.at[me]), (ln_hbm, ln_ref), (wq_hbm, wqkv_ref.at[0]),
        (wk_hbm, wqkv_ref.at[1]), (wv_hbm, wqkv_ref.at[2]), (rel_hbm, rel_ref),
        (wo_hbm, mine.at[pl.ds(0, share)]), (wqc_hbm, mine.at[pl.ds(share, share)]),
        (woc_hbm, mine.at[pl.ds(2 * share, share)]),
    ]
    loads = [pltpu.make_async_copy(src, dst, in_sem.at[i]) for i, (src, dst) in enumerate(loads)]
    for load in loads:
        load.start()
    lane_id = lax.broadcasted_iota(jnp.int32, (1, 128), 1)
    e_row = jnp.zeros((1, 128), jnp.int32)
    for b in range(rows):
        e_row = jnp.where(lane_id == b, eidx_ref[b], e_row)
    eall_ref[me] = e_row

    loads[0].wait()
    pl.semaphore_wait(barrier, n - 1)
    x_out = [remote(xall_ref.at[me], xall_ref.at[me], x_send.at[i], x_recv.at[me], dev(*peer))
             for i, peer in enumerate(PEERS)]
    for copy in x_out:
        copy.start()
    for load in loads[7:]:
        load.wait()

    right, left, far, sib = dev(1, 0), dev(3, 0), dev(2, 0), dev(0, 1)
    w_out = []

    def send_piece(owner, part, target):
        start, size = pieces[part]
        block = wall_ref.at[owner, pl.ds(start, size)]
        copy = remote(block, block, w_send.at[len(w_out)], w_recv.at[owner, part], target)
        copy.start()
        w_out.append(copy)

    def wait_piece(owner, part):
        start, size = pieces[part]
        block = wall_ref.at[owner, pl.ds(start, size)]
        remote(block, block, w_send.at[0], w_recv.at[owner, part], sib).wait_recv()

    send_piece(me, 0, right)
    send_piece(me, 1, left)
    loads[1].wait()
    small = []
    for i, peer in enumerate(PEERS):
        dst = dev(*peer)
        small.append(remote(wr_ref.at[me], wr_ref.at[me], r_send.at[i], r_recv.at[me], dst))
        small.append(remote(eall_ref.at[me], eall_ref.at[me], e_send.at[i], e_recv.at[me], dst))
    k_loads = [pltpu.make_async_copy(k_hbm.at[pl.ds(i * UNROLL, UNROLL)], k_ref.at[pl.ds(i * UNROLL, UNROLL)],
                                     k_sem.at[i]) for i in range(steps)]
    v_loads = [pltpu.make_async_copy(v_hbm.at[pl.ds(i * UNROLL, UNROLL)], v_ref.at[pl.ds(i * UNROLL, UNROLL)],
                                     v_sem.at[i]) for i in range(steps)]
    big = [pltpu.make_async_copy(src, dst, big_sem.at[i]) for i, (src, dst) in
           enumerate([(ck_hbm, ck_ref), (cv_hbm, cv_ref), (win_hbm, win_ref), (wout_hbm, wout_ref)])]
    for load in k_loads + v_loads + big:
        load.start()

    loads[6].wait()
    rel = jnp.concatenate([rel_ref[...], jnp.zeros((heads_pad - rel_ref.shape[0], length), F32)], axis=0)
    flip = (lax.broadcasted_iota(jnp.int32, (length, length), 0) + lax.broadcasted_iota(jnp.int32, (length, length), 1)
            == length - 1).astype(F32).astype(BF16)
    hi = rel.astype(BF16)
    rest = rel - hi.astype(F32)
    mid = rest.astype(BF16)
    low = (rest - mid.astype(F32)).astype(BF16)
    rrev_ref[...] = (jnp.dot(hi, flip, preferred_element_type=F32) + jnp.dot(mid, flip, preferred_element_type=F32)
                     + jnp.dot(low, flip, preferred_element_type=F32))
    qsend_ref[...] = jnp.zeros_like(qsend_ref)

    for load in loads[2:6]:
        load.wait()
    for peer in PEERS:
        src = dev(*peer)
        remote(xall_ref.at[src], xall_ref.at[src], x_send.at[0], x_recv.at[src], src).wait_recv()
    x_norm = rms_norm(xall_ref[...].reshape(n * rows, width).astype(F32), ln_ref[...][None])
    for part in range(3):
        qsend_ref[:, part * 128:part * 128 + share] = dot_nt(x_norm, wqkv_ref[part]).astype(BF16)
    q_out = []
    for i, peer in enumerate(PEERS):
        dst = dev(*peer)
        q_out.append(remote(qsend_ref.at[pl.ds(dst * rows, rows)], qrecv_ref.at[me], q_send.at[i], q_recv.at[me], dst))
    for copy in q_out:
        copy.start()
    qrecv_ref[me] = qsend_ref[pl.ds(pl.multiple_of(me * rows, rows), rows), :]
    for target, order in ((right, (2, 1, 3)), (left, (3, 0, 2))):
        for part in order:
            send_piece(me, part, target)
    for part in range(len(pieces)):
        send_piece(me, part, sib)
    for copy in small:
        copy.start()

    for peer in PEERS:
        src = dev(*peer)
        remote(qrecv_ref.at[src], qrecv_ref.at[src], q_send.at[0], q_recv.at[src], src).wait_recv()
    wait_piece(left, 0)
    send_piece(left, 0, right)
    wait_piece(right, 1)
    send_piece(right, 1, left)
    send_piece(left, 0, sib)
    send_piece(right, 1, sib)

    def columns(part):
        return jnp.concatenate([qrecv_ref[s][:, part * 128:part * 128 + share] for s in range(n)], axis=1).astype(F32)
    q_ref[...] = columns(0)
    kv_ref[0] = columns(1)
    kv_ref[1] = columns(2)

    h_mask = head_mask(heads_pad, width, head_dim)
    lane = lax.broadcasted_iota(jnp.int32, (1, length), 1)

    def score_step(i, carry):
        pltpu.make_async_copy(k_hbm.at[pl.ds(i * UNROLL, UNROLL)], k_ref.at[pl.ds(i * UNROLL, UNROLL)],
                              k_sem.at[i]).wait()
        for s in range(UNROLL):
            b = i * UNROLL + s
            pos = pos_ref[b]
            q_diag = q_ref[pl.ds(b, 1), :] * h_mask
            scores = jnp.dot(q_diag.astype(BF16), k_ref[b], preferred_element_type=F32)
            new = jnp.sum(q_diag * kv_ref[0, pl.ds(b, 1), :], axis=1, keepdims=True)
            bias = pltpu.roll(rrev_ref[...], pos + 1, axis=1)
            s_ref[b] = jnp.where(lane <= pos, jnp.where(lane == pos, new, scores) + bias, NEG_BIG)
        return carry
    lax.fori_loop(0, steps, score_step, 0)

    wait_piece(left, 2)
    send_piece(left, 2, right)
    wait_piece(right, 3)
    send_piece(right, 3, left)
    send_piece(left, 2, sib)
    send_piece(right, 3, sib)

    p_ref[...] = softmax_rows(s_ref[...])

    def value_step(i, carry):
        pltpu.make_async_copy(v_hbm.at[pl.ds(i * UNROLL, UNROLL)], v_ref.at[pl.ds(i * UNROLL, UNROLL)],
                              v_sem.at[i]).wait()
        for s in range(UNROLL):
            b = i * UNROLL + s
            here = lane == pos_ref[b]
            probs = p_ref[b].astype(F32)
            new = jnp.sum(jnp.where(here, probs, 0.0), axis=1, keepdims=True)
            spread = dot_nt(jnp.where(here, 0.0, probs).astype(BF16), v_ref[b])
            spread = spread + new * kv_ref[1, pl.ds(b, 1), :]
            ctx32_ref[pl.ds(b, 1), :] = jnp.sum(spread * h_mask, axis=0, keepdims=True)
        return carry
    lax.fori_loop(0, steps, value_step, 0)
    ctx_ref[...] = ctx32_ref[...].astype(BF16)

    for owner, part in ((left, 1), (right, 0), (left, 3), (right, 2)):
        wait_piece(owner, part)
        send_piece(owner, part, sib)
    for part in range(len(pieces)):
        wait_piece(far, part)
        send_piece(far, part, sib)
    for step in range(n // 2):
        for part in range(len(pieces)):
            wait_piece(dev(step, 1), part)
    for peer in PEERS:
        src = dev(*peer)
        remote(wr_ref.at[src], wr_ref.at[src], r_send.at[0], r_recv.at[src], src).wait_recv()
        remote(eall_ref.at[src], eall_ref.at[src], e_send.at[0], e_recv.at[src], src).wait_recv()
    for load in big:
        load.wait()
    for copy in x_out + q_out + w_out + small:
        copy.wait_send()


def cross_kernel(head_dim, pos_ref, kv_ref, ctx_ref, wall_ref, hid_hbm, lnc_hbm, mask_hbm, k_ref, v_ref, ck_ref, cv_ref,
                 newk_hbm, newv_hbm, h1_ref, ctx2_ref,
                 hid_ref, lnc_ref, mask_ref, kt_ref, vt_ref, kp_ref, vp_ref, q_ref, s_ref, p_ref, ctx32_ref,
                 in_sem, k_sem, v_sem):
    rows, width, length = k_ref.shape
    heads_pad = s_ref.shape[1]
    share = width // wall_ref.shape[0]
    steps = rows // UNROLL
    tiles = length // 128
    loads = [(hid_hbm, hid_ref), (lnc_hbm, lnc_ref), (mask_hbm, mask_ref)]
    loads = [pltpu.make_async_copy(src, dst, in_sem.at[i]) for i, (src, dst) in enumerate(loads)]
    for load in loads:
        load.start()
    pad = jnp.zeros((128 - rows, width), F32)
    kt_ref[...] = jnp.concatenate([kv_ref[0], pad], axis=0).T
    vt_ref[...] = jnp.concatenate([kv_ref[1], pad], axis=0).T
    lane_tile = lax.broadcasted_iota(jnp.int32, (1, 128), 1)

    def out_copies(b, old_ref, patch_ref, new_hbm, sem):
        tile = pos_ref[b] // 128
        copies = []
        for k in range(tiles):
            cols = pl.ds(pl.multiple_of(lax.rem(tile + k, tiles) * 128, 128), 128)
            src = patch_ref.at[b] if k == 0 else old_ref.at[b, :, cols]
            copies.append(pltpu.make_async_copy(src, new_hbm.at[b, :, cols], sem.at[b, k]))
        return copies

    def put_row(b, column, old_ref, patch_ref, new_hbm, sem):
        pos = pos_ref[b]
        first = pl.multiple_of(pos // 128 * 128, 128)
        patch_ref[b] = jnp.where(lane_tile == pos - first, jnp.broadcast_to(column, (width, 128)).astype(BF16),
                                 old_ref[b, :, pl.ds(first, 128)])
        for copy in out_copies(b, old_ref, patch_ref, new_hbm, sem):
            copy.start()

    def patch_step(i, carry):
        kt = kt_ref[...]
        vt = vt_ref[...]
        for s in range(UNROLL):
            b = i * UNROLL + s
            put_row(b, kt[:, s:s + 1], k_ref, kp_ref, newk_hbm, k_sem)
            put_row(b, vt[:, s:s + 1], v_ref, vp_ref, newv_hbm, v_sem)
        kt_ref[...] = pltpu.roll(kt, 128 - UNROLL, axis=1)
        vt_ref[...] = pltpu.roll(vt, 128 - UNROLL, axis=1)
        return carry
    lax.fori_loop(0, steps, patch_step, 0)

    loads[0].wait()
    loads[1].wait()
    wo = wall_ref[:, 0:share, :].reshape(width, width)
    h1 = (hid_ref[...].astype(F32) + dot_nt(ctx_ref[...], wo)).astype(BF16).astype(F32)
    h1_ref[...] = h1
    wqc = wall_ref[:, share:2 * share, :].reshape(width, width)
    q_ref[...] = dot_nt(rms_norm(h1, lnc_ref[...][None]), wqc).astype(BF16).astype(F32)

    h_mask = head_mask(heads_pad, width, head_dim)
    loads[2].wait()

    def score_step(i, carry):
        for s in range(UNROLL):
            b = i * UNROLL + s
            q_diag = (q_ref[pl.ds(b, 1), :] * h_mask).astype(BF16)
            scores = jnp.dot(q_diag, ck_ref[b], preferred_element_type=F32)
            s_ref[b] = jnp.where(mask_ref[pl.ds(b, 1), :] == 1, scores, NEG_BIG)
        return carry
    lax.fori_loop(0, steps, score_step, 0)
    p_ref[...] = softmax_rows(s_ref[...])

    def value_step(i, carry):
        for s in range(UNROLL):
            b = i * UNROLL + s
            spread = dot_nt(p_ref[b], cv_ref[b])
            ctx32_ref[pl.ds(b, 1), :] = jnp.sum(spread * h_mask, axis=0, keepdims=True)
        return carry
    lax.fori_loop(0, steps, value_step, 0)
    ctx2_ref[...] = ctx32_ref[...].astype(BF16)

    def drain(b, carry):
        for copy in (out_copies(b, k_ref, kp_ref, newk_hbm, k_sem) + out_copies(b, v_ref, vp_ref, newv_hbm, v_sem)):
            copy.wait()
        return carry
    lax.fori_loop(0, rows, drain, 0)


def ffn_kernel(n, capacity, h1_ref, ctx2_ref, wall_ref, wr_ref, eall_ref, lnf_hbm, win_ref, wout_ref,
               out_ref,
               lnf_ref, xall_ref, u_ref, part_ref, rs_ref,
               in_sem, x_send, x_recv, rs_send, rs_recv):
    me, dev = make_dev(n)
    rows, width = h1_ref.shape
    share = width // n
    experts = win_ref.shape[0]
    barrier = pltpu.get_barrier_semaphore()
    for peer in PEERS:
        pl.semaphore_signal(barrier, inc=1, device_id={'ws': dev(*peer)}, device_id_type=MESH)
    load = pltpu.make_async_copy(lnf_hbm, lnf_ref, in_sem.at[0])
    load.start()
    woc = wall_ref[:, 2 * share:3 * share, :].reshape(width, width)
    h2 = (h1_ref[...] + dot_nt(ctx2_ref[...], woc)).astype(BF16).astype(F32)
    load.wait()
    x_own = rms_norm(h2, lnf_ref[...][None])
    xall_ref[me] = x_own
    pl.semaphore_wait(barrier, n - 1)
    x_out = [remote(xall_ref.at[me], xall_ref.at[me], x_send.at[i], x_recv.at[me], dev(*peer))
             for i, peer in enumerate(PEERS)]
    for copy in x_out:
        copy.start()

    x_f32 = x_own.astype(F32)
    logits = [jnp.sum(x_f32 * wr_ref[e], axis=-1, keepdims=True) for e in range(experts)]
    top = functools.reduce(jnp.maximum, logits)
    ex = [jnp.exp(v - top) for v in logits]
    total = functools.reduce(jnp.add, ex)
    e_pad = jnp.concatenate([eall_ref[...].reshape(n, 128), jnp.zeros((128 - n, 128), jnp.int32)], axis=0)
    e_cols = e_pad.astype(F32).T.astype(jnp.int32)
    e_all = jnp.concatenate([jnp.broadcast_to(e_cols[0:rows, s:s + 1], (rows, 128)) for s in range(n)], axis=0)
    row_id = lax.broadcasted_iota(jnp.int32, (rows, 128), 1)
    source = lax.broadcasted_iota(jnp.int32, (rows, 128), 1)
    e_own = jnp.sum(jnp.where(source == me, e_cols[0:rows, :], 0).astype(F32), axis=1, keepdims=True).astype(jnp.int32)
    gate = functools.reduce(jnp.add, [jnp.where(e_own == e, ex[e], 0.0) for e in range(experts)]) / total
    one_hot = (e_all == lax.broadcasted_iota(jnp.int32, (n * rows, 128), 1)).astype(F32).astype(BF16)
    earlier = (lax.broadcasted_iota(jnp.int32, (rows, n * rows), 1)
               < me * rows + lax.broadcasted_iota(jnp.int32, (rows, n * rows), 0)).astype(F32).astype(BF16)
    counts = jnp.dot(earlier, one_hot, preferred_element_type=F32)
    slot = jnp.sum(jnp.where(row_id == e_own, counts, 0.0), axis=-1, keepdims=True)
    keep_gate = jnp.where(slot < capacity, gate, 0.0)

    for peer in PEERS:
        src = dev(*peer)
        remote(xall_ref.at[src], xall_ref.at[src], x_send.at[0], x_recv.at[src], src).wait_recv()
    x_all = xall_ref[...].reshape(n * rows, width)
    e_wide = jnp.concatenate([e_all] * (win_ref.shape[2] // 128), axis=1)

    def expert_step(e, carry):
        u = jnp.maximum(jnp.dot(x_all, win_ref[e], preferred_element_type=F32), 0.0)
        u_ref[e] = jnp.where(e_wide == e, u, 0.0).astype(BF16)
        return carry
    lax.fori_loop(0, experts, expert_step, 0)

    chunk = part_ref.shape[2]
    rs_out = []
    for c in range(width // chunk):
        acc = jnp.zeros((n * rows, chunk), F32)
        for e in range(experts):
            acc = acc + jnp.dot(u_ref[e], wout_ref[e, :, c * chunk:(c + 1) * chunk], preferred_element_type=F32)
        part_ref[c] = acc
        rs_ref[me, c] = part_ref[c, pl.ds(pl.multiple_of(me * rows, rows), rows), :]
        for i, peer in enumerate(PEERS):
            dst = dev(*peer)
            copy = remote(part_ref.at[c, pl.ds(dst * rows, rows)], rs_ref.at[me, c], rs_send.at[c, i],
                          rs_recv.at[c, me], dst)
            copy.start()
            rs_out.append(copy)
    for c in range(width // chunk):
        for peer in PEERS:
            src = dev(*peer)
            remote(rs_ref.at[src, c], rs_ref.at[src, c], rs_send.at[c, 0], rs_recv.at[c, src], src).wait_recv()
        y = jnp.sum(rs_ref[:, c], axis=0).astype(BF16).astype(F32)
        cols = slice(c * chunk, (c + 1) * chunk)
        out_ref[:, cols] = (h2[:, cols] + y * keep_gate).astype(BF16)
    for copy in x_out + rs_out:
        copy.wait_send()


def solution(mesh):
    n = mesh.shape['ws']
    row_axes = ('dp', 'ws')
    row_vec = P(row_axes)
    row_mat = P(row_axes, None)
    cache_spec = P(row_axes, None, None, None)
    col_split = P(None, 'ws')
    in_specs = (row_mat, cache_spec, cache_spec, cache_spec, cache_spec, row_vec, row_mat, P(None, None), row_vec,
                P(None), P(None), P(None), col_split, col_split, col_split, col_split, col_split, col_split,
                col_split, P(None, None, 'ws'), P(None, 'ws', None))
    out_specs = (row_mat, cache_spec, cache_spec)

    def decoder_block(hidden, self_k, self_v, cross_k, cross_v, positions, enc_mask, rel_bias, expert_idx,
                      ln_self, ln_cross, ln_ffn, wq_self, wk_self, wv_self, wo_self, wq_cross, wo_cross,
                      w_router, w_in, w_out):
        rows, width = hidden.shape
        heads, length, head_dim = self_k.shape[1:]
        src_len = cross_k.shape[2]
        share = width // n
        heads_pad = -(-heads // 16) * 16
        experts, _, units = w_in.shape
        capacity = (2 * rows * n + experts - 1) // experts
        steps = rows // UNROLL
        chunk = 256

        def flat(cache):
            return jnp.swapaxes(cache, 2, 3).reshape(rows, width, cache.shape[2])

        dma = pltpu.SemaphoreType.DMA
        vmem, big_cache, big_src = pltpu.VMEM, (rows, width, length), (rows, width, src_len)
        ctx, kv, wall, router, e_all, k_v, v_v, ck_v, cv_v, win_v, wout_v = pl.pallas_call(
            functools.partial(self_kernel, n, head_dim),
            out_shape=(vmem((rows, width), BF16), vmem((2, rows, width), F32), vmem((n, 3 * share, width), BF16),
                       vmem((n, 1, width), F32), vmem((n, 1, 128), jnp.int32), vmem(big_cache, BF16),
                       vmem(big_cache, BF16), vmem(big_src, BF16), vmem(big_src, BF16), vmem(w_in.shape, BF16),
                       vmem(w_out.shape, BF16)),
            in_specs=[SM, SM] + [HBM] * 16,
            out_specs=(VM,) * 11,
            scratch_shapes=[
                vmem((n, rows, width), BF16), vmem((width,), F32), vmem((heads, length), F32),
                vmem((3, share, width), BF16), vmem((n * rows, 384), BF16), vmem((n, rows, 384), BF16),
                vmem((rows, width), F32), vmem((rows, heads_pad, length), F32), vmem((rows, heads_pad, length), BF16),
                vmem((rows, width), F32), vmem((heads_pad, length), F32),
                dma((10,)), dma((steps,)), dma((steps,)), dma((4,)), dma((7,)), dma((n,)), dma((7,)), dma((n,)),
                dma((7,)), dma((n,)), dma((7,)), dma((n,)), dma((28,)), dma((n, 4)),
            ],
            compiler_params=pltpu.CompilerParams(collective_id=0, has_side_effects=True,
                                                 vmem_limit_bytes=8 * 2 ** 20),
            name='self_part',
        )(positions, expert_idx,
          *in_hbm(hidden, ln_self, rel_bias, w_router.T, wq_self.T, wk_self.T, wv_self.T, wo_self.T, wq_cross.T,
                  wo_cross.T, flat(self_k), flat(self_v), flat(cross_k), flat(cross_v), w_in, w_out))

        newk, newv, h1, ctx2 = pl.pallas_call(
            functools.partial(cross_kernel, head_dim),
            out_shape=(pltpu.HBM(big_cache, BF16), pltpu.HBM(big_cache, BF16), vmem((rows, width), F32),
                       vmem((rows, width), BF16)),
            in_specs=[SM, VM, VM, VM, HBM, HBM, HBM, VM, VM, VM, VM],
            out_specs=(HBM, HBM, VM, VM),
            scratch_shapes=[
                vmem((rows, width), BF16), vmem((width,), F32), vmem((rows, src_len), jnp.int32), vmem((width, 128), F32),
                vmem((width, 128), F32), vmem((rows, width, 128), BF16), vmem((rows, width, 128), BF16),
                vmem((rows, width), F32), vmem((rows, heads_pad, src_len), F32), vmem((rows, heads_pad, src_len), BF16),
                vmem((rows, width), F32),
                dma((3,)), dma((rows, length // 128)), dma((rows, length // 128)),
            ],
            compiler_params=pltpu.CompilerParams(has_side_effects=True, vmem_limit_bytes=12 * 2 ** 20),
            name='cross_part',
        )(positions, *in_vmem(kv, ctx, wall), *in_hbm(hidden, ln_cross, enc_mask), *in_vmem(k_v, v_v, ck_v, cv_v))

        out = pl.pallas_call(
            functools.partial(ffn_kernel, n, capacity),
            out_shape=jax.ShapeDtypeStruct((rows, width), BF16),
            in_specs=[VM] * 5 + [HBM] + [VM] * 2,
            out_specs=VM,
            scratch_shapes=[
                vmem((width,), F32), vmem((n, rows, width), BF16), vmem((experts, n * rows, units), BF16),
                vmem((width // chunk, n * rows, chunk), F32), vmem((n, width // chunk, rows, chunk), F32),
                dma((1,)), dma((7,)), dma((n,)), dma((width // chunk, 7)), dma((width // chunk, n)),
            ],
            compiler_params=pltpu.CompilerParams(collective_id=1, has_side_effects=True,
                                                 vmem_limit_bytes=12 * 2 ** 20),
            name='ffn_part',
        )(*in_vmem(h1, ctx2, wall, router, e_all), *in_hbm(ln_ffn), *in_vmem(win_v, wout_v))

        def unflat(cache):
            return jnp.swapaxes(cache.reshape(rows, heads, head_dim, length), 2, 3)
        return out, unflat(newk), unflat(newv)

    return jax.shard_map(decoder_block, mesh=mesh, in_specs=in_specs, out_specs=out_specs, check_vma=False)
```

```python
import functools
import jax
import jax.numpy as jnp
from jax import lax
from jax.experimental import pallas as pl
from jax.experimental.pallas import tpu as pltpu
from jax.sharding import PartitionSpec as P

EPSILON = 1e-6
NEG_BIG = -1e30
F32, BF16 = jnp.float32, jnp.bfloat16
MESH = pl.DeviceIdType.MESH
VM = pl.BlockSpec(memory_space=pltpu.VMEM)
HBM = pl.BlockSpec(memory_space=pltpu.HBM)
NT = (((1,), (1,)), ((), ()))
FROM_LEFT, FROM_RIGHT, FROM_FAR = 0, 1, 2
PEERS = ((2, 0), (2, 1), (1, 0), (3, 0), (1, 1), (3, 1), (0, 1))
UNROLL = 4


def in_hbm(*arrays):
    return [pltpu.with_memory_space_constraint(a, pltpu.HBM) for a in arrays]


def in_vmem(*arrays):
    return [pltpu.with_memory_space_constraint(a, pltpu.VMEM) for a in arrays]


def rms_norm(hid_f32, scale):
    inv_rms = lax.rsqrt(jnp.mean(hid_f32 * hid_f32, axis=-1, keepdims=True) + EPSILON)
    return (hid_f32 * inv_rms * scale).astype(BF16)


def dot_nt(a, b):
    return lax.dot_general(a, b, NT, preferred_element_type=F32)


def softmax_rows(scores):
    top = jnp.max(scores, axis=-1, keepdims=True)
    ex = jnp.exp(scores - top)
    return (ex / jnp.sum(ex, axis=-1, keepdims=True)).astype(BF16)


def make_dev(n):
    me = lax.axis_index('ws')
    chips = n // 2
    chip, core = me // 2, lax.rem(me, 2)

    def dev(step, other):
        return 2 * lax.rem(chip + step, chips) + ((1 - core) if other else core)
    return me, dev


def remote(src, dst, send_sem, recv_sem, dev):
    return pltpu.make_async_remote_copy(src_ref=src, dst_ref=dst, send_sem=send_sem, recv_sem=recv_sem,
                                        device_id={'ws': dev}, device_id_type=MESH)


def to_peers(dev, me, ref, send_sem, recv_sem):
    return [remote(ref.at[me], ref.at[me], send_sem, recv_sem, dev(*peer)) for peer in PEERS]


def all_of(ref, count, send_sem, recv_sem, dev):
    block = ref.at[pl.ds(0, count)]
    return remote(block, block, send_sem, recv_sem, dev)


def head_mask(heads_pad, width, head_dim):
    row = lax.broadcasted_iota(jnp.int32, (heads_pad, width), 0)
    col = lax.broadcasted_iota(jnp.int32, (heads_pad, width), 1)
    return (col // head_dim == row).astype(F32)


def main_kernel(n, head_dim, capacity, pos_hbm, eidx_hbm, hid_hbm, ln_hbm, lnc_hbm, lnf_hbm, rel_hbm, mask_hbm, wr_hbm,
                wq_hbm, wk_hbm, wv_hbm, wo_hbm, wqc_hbm, woc_hbm, k_hbm, v_hbm, ck_hbm, cv_hbm, win_hbm, wout_hbm,
                out_ref, k_ref, v_ref,
                ck_ref, cv_ref, win_ref, wout_ref, wall_ref, pos_ref, eidx_ref, ln_ref, lnc_ref, lnf_ref, rel_ref, mask_ref, wr_ref, eall_ref, xall_ref, yall_ref, hid_ref,
                wqkv_ref, qsend_ref, qrecv_ref, q_ref, kv_ref, kt_ref, vt_ref, s_ref, p_ref, s2_ref, p2_ref, ctx32_ref,
                rrev_ref, u_ref, part_ref, rs_ref,
                in_sem, big_sem, x_sem, r_sem, e_sem, q_sem, y_sem, w_send, w_recv, pair_recv, rs_send, rs_recv):
    me, dev = make_dev(n)
    rows, width, length = k_ref.shape
    heads_pad = s_ref.shape[1]
    share = width // n
    half = share // 2
    steps = rows // UNROLL
    peers = len(PEERS)
    pieces = ((0, share), (share, share), (2 * share, half), (2 * share + half, half))

    barrier = pltpu.get_barrier_semaphore()
    for peer in PEERS:
        pl.semaphore_signal(barrier, inc=1, device_id={'ws': dev(*peer)}, device_id_type=MESH)

    mine = wall_ref.at[me]
    loads = [
        (hid_hbm, xall_ref.at[me], 0), (wr_hbm, wr_ref.at[me], 1), (ln_hbm, ln_ref, 2), (wq_hbm, wqkv_ref.at[0], 3),
        (wk_hbm, wqkv_ref.at[1], 3), (wv_hbm, wqkv_ref.at[2], 3), (rel_hbm, rel_ref, 4),
        (wo_hbm, mine.at[pl.ds(0, share)], 5), (wqc_hbm, mine.at[pl.ds(share, share)], 5),
        (woc_hbm, mine.at[pl.ds(2 * share, share)], 5), (eidx_hbm, eidx_ref, 6), (pos_hbm, pos_ref, 7),
        (lnc_hbm, lnc_ref, 8), (lnf_hbm, lnf_ref, 9), (mask_hbm, mask_ref, 10), (hid_hbm, hid_ref, 11),
    ]
    loads = [pltpu.make_async_copy(src, dst, in_sem.at[i]) for src, dst, i in loads]
    for load in loads:
        load.start()
    experts = win_ref.shape[0]
    lane_id = lax.broadcasted_iota(jnp.int32, (1, 128), 1)
    loads[0].wait()
    pl.semaphore_wait(barrier, n - 1)
    for copy in to_peers(dev, me, xall_ref, x_sem.at[0], x_sem.at[1]):
        copy.start()
    pltpu.make_async_copy(mine, mine, in_sem.at[5]).wait()

    right, left, far, sib = dev(1, 0), dev(3, 0), dev(2, 0), dev(0, 1)

    def send_piece(owner, role, part, target):
        start, size = pieces[part]
        block = wall_ref.at[owner, pl.ds(start, size)]
        sem = pair_recv.at[part // 2] if role is None else w_recv.at[role, part]
        remote(block, block, w_send.at[0], sem, target).start()

    def wait_piece(owner, role, part):
        start, size = pieces[part]
        block = wall_ref.at[owner, pl.ds(start, size)]
        remote(block, block, w_send.at[0], w_recv.at[role, part], sib).wait_recv()

    def wait_pair(stage):
        size = 2 * share if stage == 0 else share
        block = wall_ref.at[pl.ds(0, n // 2), pl.ds(0, size)]
        remote(block, block, w_send.at[0], pair_recv.at[stage], sib).wait_recv()

    send_piece(me, FROM_LEFT, 0, right)
    send_piece(me, FROM_RIGHT, 1, left)
    loads[1].wait()
    loads[10].wait()
    e_row = jnp.zeros((1, 128), jnp.int32)
    for b in range(rows):
        e_row = jnp.where(lane_id == b, eidx_ref[b], e_row)
    eall_ref[me] = e_row
    big = [pltpu.make_async_copy(src, dst, big_sem.at[i]) for i, (src, dst) in
           enumerate([(k_hbm, k_ref), (v_hbm, v_ref), (ck_hbm, ck_ref), (cv_hbm, cv_ref), (win_hbm, win_ref), (wout_hbm, wout_ref)])]
    for load in big:
        load.start()

    loads[6].wait()
    rel = jnp.concatenate([rel_ref[...], jnp.zeros((heads_pad - rel_ref.shape[0], length), F32)], axis=0)
    flip = (lax.broadcasted_iota(jnp.int32, (length, length), 0) + lax.broadcasted_iota(jnp.int32, (length, length), 1)
            == length - 1).astype(F32).astype(BF16)
    hi = rel.astype(BF16)
    rest = rel - hi.astype(F32)
    mid = rest.astype(BF16)
    low = (rest - mid.astype(F32)).astype(BF16)
    rrev_ref[...] = (jnp.dot(hi, flip, preferred_element_type=F32) + jnp.dot(mid, flip, preferred_element_type=F32)
                     + jnp.dot(low, flip, preferred_element_type=F32))
    qsend_ref[...] = jnp.zeros_like(qsend_ref)

    for load in loads[2:3] + loads[11:]:
        load.wait()
    pltpu.make_async_copy(wqkv_ref, wqkv_ref, in_sem.at[3]).wait()
    all_of(xall_ref, peers, x_sem.at[0], x_sem.at[1], sib).wait_recv()
    x_norm = rms_norm(xall_ref[...].reshape(n * rows, width).astype(F32), ln_ref[...][None])
    for part in range(3):
        qsend_ref[:, part * 128:part * 128 + share] = dot_nt(x_norm, wqkv_ref[part]).astype(BF16)
    for peer in PEERS:
        dst = dev(*peer)
        remote(qsend_ref.at[pl.ds(dst * rows, rows)], qrecv_ref.at[me], q_sem.at[0], q_sem.at[1], dst).start()
    qrecv_ref[me] = qsend_ref[pl.ds(pl.multiple_of(me * rows, rows), rows), :]
    send_piece(me, FROM_LEFT, 1, right)
    send_piece(me, FROM_RIGHT, 0, left)
    for part in range(len(pieces)):
        send_piece(me, None, part, sib)
    for copy in (to_peers(dev, me, wr_ref, r_sem.at[0], r_sem.at[1])
                 + to_peers(dev, me, eall_ref, e_sem.at[0], e_sem.at[1])):
        copy.start()

    all_of(qrecv_ref, peers, q_sem.at[0], q_sem.at[1], sib).wait_recv()
    wait_piece(left, FROM_LEFT, 0)
    send_piece(left, FROM_FAR, 0, right)
    wait_piece(right, FROM_RIGHT, 1)
    send_piece(right, FROM_FAR, 1, left)
    for part in (2, 3):
        send_piece(me, FROM_LEFT, part, right)
        send_piece(me, FROM_RIGHT, 5 - part, left)
    send_piece(left, None, 0, sib)
    send_piece(right, None, 1, sib)

    def columns(part):
        return jnp.concatenate([qrecv_ref[s][:, part * 128:part * 128 + share] for s in range(n)], axis=1).astype(F32)
    q_ref[...] = columns(0)
    kv_ref[0] = columns(1)
    kv_ref[1] = columns(2)

    h_mask = head_mask(heads_pad, width, head_dim)
    lane = lax.broadcasted_iota(jnp.int32, (1, length), 1)

    big[0].wait()

    def score_step(i, carry):
        for s in range(UNROLL):
            b = i * UNROLL + s
            pos = pos_ref[b]
            q_diag = q_ref[pl.ds(b, 1), :] * h_mask
            scores = jnp.dot(q_diag.astype(BF16), k_ref[b], preferred_element_type=F32)
            new = jnp.sum(q_diag * kv_ref[0, pl.ds(b, 1), :], axis=1, keepdims=True)
            bias = pltpu.roll(rrev_ref[...], pos + 1, axis=1)
            s_ref[b] = jnp.where(lane <= pos, jnp.where(lane == pos, new, scores) + bias, NEG_BIG)
        return carry
    lax.fori_loop(0, steps, score_step, 0)

    p_ref[...] = softmax_rows(s_ref[...])

    big[1].wait()

    def value_step(i, carry):
        for s in range(UNROLL):
            b = i * UNROLL + s
            here = lane == pos_ref[b]
            probs = p_ref[b].astype(F32)
            new = jnp.sum(jnp.where(here, probs, 0.0), axis=1, keepdims=True)
            spread = dot_nt(jnp.where(here, 0.0, probs).astype(BF16), v_ref[b])
            spread = spread + new * kv_ref[1, pl.ds(b, 1), :]
            ctx32_ref[pl.ds(b, 1), :] = jnp.sum(spread * h_mask, axis=0, keepdims=True)
        return carry
    lax.fori_loop(0, steps // 2, value_step, 0)
    for owner, role, part in ((left, FROM_LEFT, 1), (right, FROM_RIGHT, 0)):
        wait_piece(owner, role, part)
        send_piece(owner, None, part, sib)
    lax.fori_loop(steps // 2, steps, value_step, 0)

    for part in (0, 1):
        wait_piece(far, FROM_FAR, part)
        send_piece(far, None, part, sib)
    wait_pair(0)

    wo = wall_ref[:, 0:share, :].reshape(width, width)
    h1 = (hid_ref[...].astype(F32) + dot_nt(ctx32_ref[...].astype(BF16), wo)).astype(BF16).astype(F32)
    wqc = wall_ref[:, share:2 * share, :].reshape(width, width)
    q_ref[...] = dot_nt(rms_norm(h1, lnc_ref[...][None]), wqc).astype(BF16).astype(F32)
    wait_piece(left, FROM_LEFT, 2)
    send_piece(left, FROM_FAR, 2, right)
    wait_piece(right, FROM_RIGHT, 3)
    send_piece(right, FROM_FAR, 3, left)
    send_piece(left, None, 2, sib)
    send_piece(right, None, 3, sib)
    for load in big[2:]:
        load.wait()

    def cross_score(i, carry):
        for s in range(UNROLL):
            b = i * UNROLL + s
            q_diag = (q_ref[pl.ds(b, 1), :] * h_mask).astype(BF16)
            scores = jnp.dot(q_diag, ck_ref[b], preferred_element_type=F32)
            s2_ref[b] = jnp.where(mask_ref[pl.ds(b, 1), :] == 1, scores, NEG_BIG)
        return carry
    lax.fori_loop(0, steps, cross_score, 0)
    for owner, role, part in ((left, FROM_LEFT, 3), (right, FROM_RIGHT, 2)):
        wait_piece(owner, role, part)
        send_piece(owner, None, part, sib)
    p2_ref[...] = softmax_rows(s2_ref[...])

    def cross_value(i, carry):
        for s in range(UNROLL):
            b = i * UNROLL + s
            spread = dot_nt(p2_ref[b], cv_ref[b])
            ctx32_ref[pl.ds(b, 1), :] = jnp.sum(spread * h_mask, axis=0, keepdims=True)
        return carry
    lax.fori_loop(0, steps, cross_value, 0)

    for part in (2, 3):
        wait_piece(far, FROM_FAR, part)
        send_piece(far, None, part, sib)
    wait_pair(1)
    woc = wall_ref[:, 2 * share:3 * share, :].reshape(width, width)
    h2 = (h1 + dot_nt(ctx32_ref[...].astype(BF16), woc)).astype(BF16).astype(F32)
    x_own = rms_norm(h2, lnf_ref[...][None])
    yall_ref[me] = x_own
    for copy in to_peers(dev, me, yall_ref, y_sem.at[0], y_sem.at[1]):
        copy.start()

    all_of(wr_ref, peers, r_sem.at[0], r_sem.at[1], sib).wait_recv()
    all_of(eall_ref, peers, e_sem.at[0], e_sem.at[1], sib).wait_recv()
    x_f32 = x_own.astype(F32)
    logits = [jnp.sum(x_f32 * wr_ref[e], axis=-1, keepdims=True) for e in range(experts)]
    top = functools.reduce(jnp.maximum, logits)
    ex = [jnp.exp(v - top) for v in logits]
    total = functools.reduce(jnp.add, ex)
    e_pad = jnp.concatenate([eall_ref[...].reshape(n, 128), jnp.zeros((128 - n, 128), jnp.int32)], axis=0)
    e_cols = e_pad.astype(F32).T.astype(jnp.int32)
    e_all = jnp.concatenate([jnp.broadcast_to(e_cols[0:rows, s:s + 1], (rows, 128)) for s in range(n)], axis=0)
    row_id = lax.broadcasted_iota(jnp.int32, (rows, 128), 1)
    source = lax.broadcasted_iota(jnp.int32, (rows, 128), 1)
    e_own = jnp.sum(jnp.where(source == me, e_cols[0:rows, :], 0).astype(F32), axis=1, keepdims=True).astype(jnp.int32)
    gate = functools.reduce(jnp.add, [jnp.where(e_own == e, ex[e], 0.0) for e in range(experts)]) / total
    one_hot = (e_all == lax.broadcasted_iota(jnp.int32, (n * rows, 128), 1)).astype(F32).astype(BF16)
    earlier = (lax.broadcasted_iota(jnp.int32, (rows, n * rows), 1)
               < me * rows + lax.broadcasted_iota(jnp.int32, (rows, n * rows), 0)).astype(F32).astype(BF16)
    counts = jnp.dot(earlier, one_hot, preferred_element_type=F32)
    slot = jnp.sum(jnp.where(row_id == e_own, counts, 0.0), axis=-1, keepdims=True)
    keep_gate = jnp.where(slot < capacity, gate, 0.0)

    pad = jnp.zeros((128 - rows, width), F32)
    kt_ref[...] = jnp.concatenate([kv_ref[0], pad], axis=0).T
    vt_ref[...] = jnp.concatenate([kv_ref[1], pad], axis=0).T

    def patch_row(b, column, cache_ref):
        cache_ref[b] = jnp.where(lane == pos_ref[b], jnp.broadcast_to(column, (width, length)).astype(BF16), cache_ref[b])

    def patch_step(i, carry):
        kt = kt_ref[...]
        vt = vt_ref[...]
        for s in range(UNROLL):
            patch_row(i * UNROLL + s, kt[:, s:s + 1], k_ref)
            patch_row(i * UNROLL + s, vt[:, s:s + 1], v_ref)
        kt_ref[...] = pltpu.roll(kt, 128 - UNROLL, axis=1)
        vt_ref[...] = pltpu.roll(vt, 128 - UNROLL, axis=1)
        return carry
    lax.fori_loop(0, steps, patch_step, 0)

    all_of(yall_ref, peers, y_sem.at[0], y_sem.at[1], sib).wait_recv()
    x_all = yall_ref[...].reshape(n * rows, width)
    e_wide = jnp.concatenate([e_all] * (win_ref.shape[2] // 128), axis=1)

    def expert_step(e, carry):
        u = jnp.maximum(jnp.dot(x_all, win_ref[e], preferred_element_type=F32), 0.0)
        u_ref[e] = jnp.where(e_wide == e, u, 0.0).astype(BF16)
        return carry
    lax.fori_loop(0, experts, expert_step, 0)

    chunk = part_ref.shape[2]
    for c in range(width // chunk):
        acc = jnp.zeros((n * rows, chunk), F32)
        for e in range(experts):
            acc = acc + jnp.dot(u_ref[e], wout_ref[e, :, c * chunk:(c + 1) * chunk], preferred_element_type=F32)
        part_ref[c] = acc
        rs_ref[c, me] = part_ref[c, pl.ds(pl.multiple_of(me * rows, rows), rows), :]
        for peer in PEERS:
            dst = dev(*peer)
            remote(part_ref.at[c, pl.ds(dst * rows, rows)], rs_ref.at[c, me], rs_send.at[0], rs_recv.at[c], dst).start()
    for c in range(width // chunk):
        all_of(rs_ref.at[c], peers, rs_send.at[0], rs_recv.at[c], sib).wait_recv()
        y = jnp.sum(rs_ref[c], axis=0).astype(BF16).astype(F32)
        cols = slice(c * chunk, (c + 1) * chunk)
        out_ref[:, cols] = (h2[:, cols] + y * keep_gate).astype(BF16)
    for ref, sem in ((xall_ref, x_sem), (qrecv_ref, q_sem), (yall_ref, y_sem), (wr_ref, r_sem), (eall_ref, e_sem),
                     (wall_ref, w_send)):
        all_of(ref, peers, sem.at[0], sem.at[0], sib).wait_send()
    sent = rs_ref.at[:, pl.ds(0, peers)]
    remote(sent, sent, rs_send.at[0], rs_send.at[0], sib).wait_send()


def write_kernel(hid_ref, k_ref, v_ref, out_hbm, newk_hbm, newv_hbm, sem):
    span = k_ref.shape[0] // 4
    copies = [pltpu.make_async_copy(hid_ref, out_hbm, sem.at[8])]
    for i in range(4):
        rows = pl.ds(i * span, span)
        copies.append(pltpu.make_async_copy(k_ref.at[rows], newk_hbm.at[rows], sem.at[2 * i]))
        copies.append(pltpu.make_async_copy(v_ref.at[rows], newv_hbm.at[rows], sem.at[2 * i + 1]))
    for copy in copies:
        copy.start()
    for copy in copies:
        copy.wait()


def solution(mesh):
    n = mesh.shape['ws']
    row_axes = ('dp', 'ws')
    row_vec = P(row_axes)
    row_mat = P(row_axes, None)
    cache_spec = P(row_axes, None, None, None)
    col_split = P(None, 'ws')
    in_specs = (row_mat, cache_spec, cache_spec, cache_spec, cache_spec, row_vec, row_mat, P(None, None), row_vec,
                P(None), P(None), P(None), col_split, col_split, col_split, col_split, col_split, col_split,
                col_split, P(None, None, 'ws'), P(None, 'ws', None))
    out_specs = (row_mat, cache_spec, cache_spec)

    def decoder_block(hidden, self_k, self_v, cross_k, cross_v, positions, enc_mask, rel_bias, expert_idx,
                      ln_self, ln_cross, ln_ffn, wq_self, wk_self, wv_self, wo_self, wq_cross, wo_cross,
                      w_router, w_in, w_out):
        rows, width = hidden.shape
        heads, length, head_dim = self_k.shape[1:]
        src_len = cross_k.shape[2]
        share = width // n
        heads_pad = -(-heads // 16) * 16
        experts, _, units = w_in.shape
        capacity = (2 * rows * n + experts - 1) // experts
        chunk = 256

        def flat(cache):
            return jnp.swapaxes(cache, 2, 3).reshape(rows, width, cache.shape[2])

        dma = pltpu.SemaphoreType.DMA
        vmem, big_cache, big_src = pltpu.VMEM, (rows, width, length), (rows, width, src_len)
        parts, smem = width // chunk, pltpu.SMEM
        hid_out, k_v, v_v = pl.pallas_call(
            functools.partial(main_kernel, n, head_dim, capacity),
            out_shape=(vmem((rows, width), BF16), vmem(big_cache, BF16), vmem(big_cache, BF16)),
            in_specs=[HBM] * 21,
            out_specs=(VM,) * 3,
            scratch_shapes=[
                vmem(big_src, BF16), vmem(big_src, BF16), vmem(w_in.shape, BF16), vmem(w_out.shape, BF16),
                vmem((n, 3 * share, width), BF16),
                smem((rows,), jnp.int32), smem((rows,), jnp.int32), vmem((width,), F32), vmem((width,), F32),
                vmem((width,), F32), vmem((heads, length), F32), vmem((rows, src_len), jnp.int32),
                vmem((n, 1, width), F32), vmem((n, 1, 128), jnp.int32), vmem((n, rows, width), BF16),
                vmem((n, rows, width), BF16), vmem((rows, width), BF16), vmem((3, share, width), BF16),
                vmem((n * rows, 384), BF16), vmem((n, rows, 384), BF16), vmem((rows, width), F32),
                vmem((2, rows, width), F32), vmem((width, 128), F32), vmem((width, 128), F32),
                vmem((rows, heads_pad, length), F32), vmem((rows, heads_pad, length), BF16),
                vmem((rows, heads_pad, src_len), F32), vmem((rows, heads_pad, src_len), BF16), vmem((rows, width), F32),
                vmem((heads_pad, length), F32), vmem((experts, n * rows, units), BF16),
                vmem((parts, n * rows, chunk), F32), vmem((parts, n, rows, chunk), F32),
                dma((12,)), dma((6,)), dma((2,)), dma((2,)), dma((2,)), dma((2,)), dma((2,)), dma((1,)), dma((3, 4)),
                dma((2,)), dma((1,)), dma((parts,)),
            ],
            compiler_params=pltpu.CompilerParams(collective_id=0, has_side_effects=True,
                                                 vmem_limit_bytes=34 * 2 ** 20),
            name='main_part',
        )(*in_hbm(positions, expert_idx, hidden, ln_self, ln_cross, ln_ffn, rel_bias, enc_mask, w_router.T, wq_self.T,
                  wk_self.T, wv_self.T, wo_self.T, wq_cross.T, wo_cross.T, flat(self_k), flat(self_v), flat(cross_k),
                  flat(cross_v), w_in, w_out))

        out, newk, newv = pl.pallas_call(
            write_kernel,
            out_shape=(pltpu.HBM((rows, width), BF16), pltpu.HBM(big_cache, BF16), pltpu.HBM(big_cache, BF16)),
            in_specs=[VM] * 3,
            out_specs=(HBM,) * 3,
            scratch_shapes=[dma((9,))],
            compiler_params=pltpu.CompilerParams(has_side_effects=True, vmem_limit_bytes=2 ** 20),
            name='write_part',
        )(*in_vmem(hid_out, k_v, v_v))

        def unflat(cache):
            return jnp.swapaxes(cache.reshape(rows, heads, head_dim, length), 2, 3)
        return out, unflat(newk), unflat(newv)

    return jax.shard_map(decoder_block, mesh=mesh, in_specs=in_specs, out_specs=out_specs, check_vma=False)
```

```python
import functools
import jax
import jax.numpy as jnp
from jax import lax
from jax.experimental import pallas as pl
from jax.experimental.pallas import tpu as pltpu
from jax.sharding import PartitionSpec as P

EPSILON = 1e-6
NEG_BIG = -1e30
F32, BF16 = jnp.float32, jnp.bfloat16
MESH = pl.DeviceIdType.MESH
VM = pl.BlockSpec(memory_space=pltpu.VMEM)
HBM = pl.BlockSpec(memory_space=pltpu.HBM)
NT = (((1,), (1,)), ((), ()))
FROM_LEFT, FROM_RIGHT, FROM_FAR = 0, 1, 2
PEERS = ((2, 0), (2, 1), (1, 0), (3, 0), (1, 1), (3, 1), (0, 1))
UNROLL = 4


def in_hbm(*arrays):
    return [pltpu.with_memory_space_constraint(a, pltpu.HBM) for a in arrays]


def in_vmem(*arrays):
    return [pltpu.with_memory_space_constraint(a, pltpu.VMEM) for a in arrays]


def rms_norm(hid_f32, scale):
    inv_rms = lax.rsqrt(jnp.mean(hid_f32 * hid_f32, axis=-1, keepdims=True) + EPSILON)
    return (hid_f32 * inv_rms * scale).astype(BF16)


def dot_nt(a, b):
    return lax.dot_general(a, b, NT, preferred_element_type=F32)


def softmax_rows(scores):
    top = jnp.max(scores, axis=-1, keepdims=True)
    ex = jnp.exp(scores - top)
    return (ex / jnp.sum(ex, axis=-1, keepdims=True)).astype(BF16)


def make_dev(n):
    me = lax.axis_index('ws')
    chips = n // 2
    chip, core = me // 2, lax.rem(me, 2)

    def dev(step, other):
        return 2 * lax.rem(chip + step, chips) + ((1 - core) if other else core)
    return me, dev


def remote(src, dst, send_sem, recv_sem, dev):
    return pltpu.make_async_remote_copy(src_ref=src, dst_ref=dst, send_sem=send_sem, recv_sem=recv_sem,
                                        device_id={'ws': dev}, device_id_type=MESH)


def to_peers(dev, me, ref, send_sem, recv_sem):
    return [remote(ref.at[me], ref.at[me], send_sem, recv_sem, dev(*peer)) for peer in PEERS]


def all_of(ref, count, send_sem, recv_sem, dev):
    block = ref.at[pl.ds(0, count)]
    return remote(block, block, send_sem, recv_sem, dev)


def head_mask(heads_pad, width, head_dim):
    row = lax.broadcasted_iota(jnp.int32, (heads_pad, width), 0)
    col = lax.broadcasted_iota(jnp.int32, (heads_pad, width), 1)
    return (col // head_dim == row).astype(F32)


def main_kernel(n, head_dim, capacity, pos_hbm, eidx_hbm, hid_hbm, ln_hbm, lnc_hbm, lnf_hbm, rel_hbm, mask_hbm, wr_hbm,
                wq_hbm, wk_hbm, wv_hbm, wo_hbm, wqc_hbm, woc_hbm, k_hbm, v_hbm, ck_hbm, cv_hbm, win_hbm, wout_hbm,
                out_ref, k_ref, v_ref,
                ck_ref, cv_ref, win_ref, wout_ref, wall_ref, pos_ref, eidx_ref, ln_ref, lnc_ref, lnf_ref, rel_ref, mask_ref, wr_ref, eall_ref, xall_ref, yall_ref, hid_ref,
                wqkv_ref, qsend_ref, qrecv_ref, q_ref, kv_ref, kt_ref, vt_ref, s_ref, p_ref, s2_ref, p2_ref, ctx32_ref,
                rrev_ref, u_ref, part_ref, pair_ref, pair_sum_ref, rs_ref,
                in_sem, big_sem, x_sem, r_sem, e_sem, q_sem, y_sem, w_send, w_recv, pair_recv, d_send, d_recv, rs_send, rs_recv):
    me, dev = make_dev(n)
    rows, width, length = k_ref.shape
    heads_pad = s_ref.shape[1]
    share = width // n
    half = share // 2
    steps = rows // UNROLL
    peers = len(PEERS)
    pieces = ((0, share), (share, share), (2 * share, half), (2 * share + half, half))

    barrier = pltpu.get_barrier_semaphore()
    for peer in PEERS:
        pl.semaphore_signal(barrier, inc=1, device_id={'ws': dev(*peer)}, device_id_type=MESH)

    mine = wall_ref.at[me]
    loads = [
        (hid_hbm, xall_ref.at[me], 0), (wr_hbm, wr_ref.at[me], 1), (ln_hbm, ln_ref, 2), (wq_hbm, wqkv_ref.at[0], 3),
        (wk_hbm, wqkv_ref.at[1], 3), (wv_hbm, wqkv_ref.at[2], 3), (rel_hbm, rel_ref, 4),
        (wo_hbm, mine.at[pl.ds(0, share)], 5), (wqc_hbm, mine.at[pl.ds(share, share)], 5),
        (woc_hbm, mine.at[pl.ds(2 * share, share)], 5), (eidx_hbm, eidx_ref, 6), (pos_hbm, pos_ref, 7),
        (lnc_hbm, lnc_ref, 8), (lnf_hbm, lnf_ref, 9), (mask_hbm, mask_ref, 10), (hid_hbm, hid_ref, 11),
    ]
    loads = [pltpu.make_async_copy(src, dst, in_sem.at[i]) for src, dst, i in loads]
    for load in loads:
        load.start()
    experts = win_ref.shape[0]
    lane_id = lax.broadcasted_iota(jnp.int32, (1, 128), 1)
    loads[0].wait()
    pl.semaphore_wait(barrier, n - 1)
    for copy in to_peers(dev, me, xall_ref, x_sem.at[0], x_sem.at[1]):
        copy.start()
    pltpu.make_async_copy(mine, mine, in_sem.at[5]).wait()

    right, left, far, sib = dev(1, 0), dev(3, 0), dev(2, 0), dev(0, 1)

    def send_piece(owner, role, part, target):
        start, size = pieces[part]
        block = wall_ref.at[owner, pl.ds(start, size)]
        sem = pair_recv.at[part // 2] if role is None else w_recv.at[role, part]
        remote(block, block, w_send.at[0], sem, target).start()

    def wait_piece(owner, role, part):
        start, size = pieces[part]
        block = wall_ref.at[owner, pl.ds(start, size)]
        remote(block, block, w_send.at[0], w_recv.at[role, part], sib).wait_recv()

    def wait_pair(stage):
        size = 2 * share if stage == 0 else share
        block = wall_ref.at[pl.ds(0, n // 2), pl.ds(0, size)]
        remote(block, block, w_send.at[0], pair_recv.at[stage], sib).wait_recv()

    send_piece(me, FROM_LEFT, 0, right)
    send_piece(me, FROM_RIGHT, 1, left)
    loads[1].wait()
    loads[10].wait()
    e_row = jnp.zeros((1, 128), jnp.int32)
    for b in range(rows):
        e_row = jnp.where(lane_id == b, eidx_ref[b], e_row)
    eall_ref[me] = e_row
    big = [pltpu.make_async_copy(src, dst, big_sem.at[i]) for i, (src, dst) in
           enumerate([(k_hbm, k_ref), (v_hbm, v_ref), (ck_hbm, ck_ref), (cv_hbm, cv_ref), (win_hbm, win_ref), (wout_hbm, wout_ref)])]
    for load in big:
        load.start()

    loads[6].wait()
    rel = jnp.concatenate([rel_ref[...], jnp.zeros((heads_pad - rel_ref.shape[0], length), F32)], axis=0)
    flip = (lax.broadcasted_iota(jnp.int32, (length, length), 0) + lax.broadcasted_iota(jnp.int32, (length, length), 1)
            == length - 1).astype(F32).astype(BF16)
    hi = rel.astype(BF16)
    rest = rel - hi.astype(F32)
    mid = rest.astype(BF16)
    low = (rest - mid.astype(F32)).astype(BF16)
    rrev_ref[...] = (jnp.dot(hi, flip, preferred_element_type=F32) + jnp.dot(mid, flip, preferred_element_type=F32)
                     + jnp.dot(low, flip, preferred_element_type=F32))
    qsend_ref[...] = jnp.zeros_like(qsend_ref)

    for load in loads[2:3] + loads[11:]:
        load.wait()
    pltpu.make_async_copy(wqkv_ref, wqkv_ref, in_sem.at[3]).wait()
    all_of(xall_ref, peers, x_sem.at[0], x_sem.at[1], sib).wait_recv()
    x_norm = rms_norm(xall_ref[...].reshape(n * rows, width).astype(F32), ln_ref[...][None])
    for part in range(3):
        qsend_ref[:, part * 128:part * 128 + share] = dot_nt(x_norm, wqkv_ref[part]).astype(BF16)
    for peer in PEERS:
        dst = dev(*peer)
        remote(qsend_ref.at[pl.ds(dst * rows, rows)], qrecv_ref.at[me], q_sem.at[0], q_sem.at[1], dst).start()
    qrecv_ref[me] = qsend_ref[pl.ds(pl.multiple_of(me * rows, rows), rows), :]
    send_piece(me, FROM_LEFT, 1, right)
    send_piece(me, FROM_RIGHT, 0, left)
    for part in range(len(pieces)):
        send_piece(me, None, part, sib)
    for copy in (to_peers(dev, me, wr_ref, r_sem.at[0], r_sem.at[1])
                 + to_peers(dev, me, eall_ref, e_sem.at[0], e_sem.at[1])):
        copy.start()

    all_of(qrecv_ref, peers, q_sem.at[0], q_sem.at[1], sib).wait_recv()
    wait_piece(left, FROM_LEFT, 0)
    send_piece(left, FROM_FAR, 0, right)
    wait_piece(right, FROM_RIGHT, 1)
    send_piece(right, FROM_FAR, 1, left)
    for part in (2, 3):
        send_piece(me, FROM_LEFT, part, right)
        send_piece(me, FROM_RIGHT, 5 - part, left)
    send_piece(left, None, 0, sib)
    send_piece(right, None, 1, sib)

    def columns(part):
        return jnp.concatenate([qrecv_ref[s][:, part * 128:part * 128 + share] for s in range(n)], axis=1).astype(F32)
    q_ref[...] = columns(0)
    kv_ref[0] = columns(1)
    kv_ref[1] = columns(2)

    h_mask = head_mask(heads_pad, width, head_dim)
    lane = lax.broadcasted_iota(jnp.int32, (1, length), 1)

    big[0].wait()

    def score_step(i, carry):
        for s in range(UNROLL):
            b = i * UNROLL + s
            pos = pos_ref[b]
            q_diag = q_ref[pl.ds(b, 1), :] * h_mask
            scores = jnp.dot(q_diag.astype(BF16), k_ref[b], preferred_element_type=F32)
            new = jnp.sum(q_diag * kv_ref[0, pl.ds(b, 1), :], axis=1, keepdims=True)
            bias = pltpu.roll(rrev_ref[...], pos + 1, axis=1)
            s_ref[b] = jnp.where(lane <= pos, jnp.where(lane == pos, new, scores) + bias, NEG_BIG)
        return carry
    lax.fori_loop(0, steps, score_step, 0)

    p_ref[...] = softmax_rows(s_ref[...])

    big[1].wait()

    def value_step(i, carry):
        for s in range(UNROLL):
            b = i * UNROLL + s
            here = lane == pos_ref[b]
            probs = p_ref[b].astype(F32)
            new = jnp.sum(jnp.where(here, probs, 0.0), axis=1, keepdims=True)
            spread = dot_nt(jnp.where(here, 0.0, probs).astype(BF16), v_ref[b])
            spread = spread + new * kv_ref[1, pl.ds(b, 1), :]
            ctx32_ref[pl.ds(b, 1), :] = jnp.sum(spread * h_mask, axis=0, keepdims=True)
        return carry
    lax.fori_loop(0, steps // 2, value_step, 0)
    for owner, role, part in ((left, FROM_LEFT, 1), (right, FROM_RIGHT, 0)):
        wait_piece(owner, role, part)
        send_piece(owner, None, part, sib)
    lax.fori_loop(steps // 2, steps, value_step, 0)

    for part in (0, 1):
        wait_piece(far, FROM_FAR, part)
        send_piece(far, None, part, sib)
    wait_pair(0)

    wait_piece(left, FROM_LEFT, 2)
    send_piece(left, FROM_FAR, 2, right)
    wait_piece(right, FROM_RIGHT, 3)
    send_piece(right, FROM_FAR, 3, left)
    send_piece(left, None, 2, sib)
    send_piece(right, None, 3, sib)
    wo = wall_ref[:, 0:share, :].reshape(width, width)
    h1 = (hid_ref[...].astype(F32) + dot_nt(ctx32_ref[...].astype(BF16), wo)).astype(BF16).astype(F32)
    wqc = wall_ref[:, share:2 * share, :].reshape(width, width)
    q_ref[...] = dot_nt(rms_norm(h1, lnc_ref[...][None]), wqc).astype(BF16).astype(F32)
    for load in big[2:]:
        load.wait()

    def cross_score(i, carry):
        for s in range(UNROLL):
            b = i * UNROLL + s
            q_diag = (q_ref[pl.ds(b, 1), :] * h_mask).astype(BF16)
            scores = jnp.dot(q_diag, ck_ref[b], preferred_element_type=F32)
            s2_ref[b] = jnp.where(mask_ref[pl.ds(b, 1), :] == 1, scores, NEG_BIG)
        return carry
    lax.fori_loop(0, steps, cross_score, 0)
    for owner, role, part in ((left, FROM_LEFT, 3), (right, FROM_RIGHT, 2)):
        wait_piece(owner, role, part)
        send_piece(owner, None, part, sib)
    p2_ref[...] = softmax_rows(s2_ref[...])

    def cross_value(i, carry):
        for s in range(UNROLL):
            b = i * UNROLL + s
            spread = dot_nt(p2_ref[b], cv_ref[b])
            ctx32_ref[pl.ds(b, 1), :] = jnp.sum(spread * h_mask, axis=0, keepdims=True)
        return carry
    lax.fori_loop(0, steps, cross_value, 0)

    for part in (2, 3):
        wait_piece(far, FROM_FAR, part)
        send_piece(far, None, part, sib)
    wait_pair(1)
    woc = wall_ref[:, 2 * share:3 * share, :].reshape(width, width)
    h2 = (h1 + dot_nt(ctx32_ref[...].astype(BF16), woc)).astype(BF16).astype(F32)
    x_own = rms_norm(h2, lnf_ref[...][None])
    yall_ref[me] = x_own
    for copy in to_peers(dev, me, yall_ref, y_sem.at[0], y_sem.at[1]):
        copy.start()

    all_of(wr_ref, peers, r_sem.at[0], r_sem.at[1], sib).wait_recv()
    all_of(eall_ref, peers, e_sem.at[0], e_sem.at[1], sib).wait_recv()
    x_f32 = x_own.astype(F32)
    logits = [jnp.sum(x_f32 * wr_ref[e], axis=-1, keepdims=True) for e in range(experts)]
    top = functools.reduce(jnp.maximum, logits)
    ex = [jnp.exp(v - top) for v in logits]
    total = functools.reduce(jnp.add, ex)
    e_pad = jnp.concatenate([eall_ref[...].reshape(n, 128), jnp.zeros((128 - n, 128), jnp.int32)], axis=0)
    e_cols = e_pad.astype(F32).T.astype(jnp.int32)
    e_all = jnp.concatenate([jnp.broadcast_to(e_cols[0:rows, s:s + 1], (rows, 128)) for s in range(n)], axis=0)
    row_id = lax.broadcasted_iota(jnp.int32, (rows, 128), 1)
    source = lax.broadcasted_iota(jnp.int32, (rows, 128), 1)
    e_own = jnp.sum(jnp.where(source == me, e_cols[0:rows, :], 0).astype(F32), axis=1, keepdims=True).astype(jnp.int32)
    gate = functools.reduce(jnp.add, [jnp.where(e_own == e, ex[e], 0.0) for e in range(experts)]) / total
    one_hot = (e_all == lax.broadcasted_iota(jnp.int32, (n * rows, 128), 1)).astype(F32).astype(BF16)
    earlier = (lax.broadcasted_iota(jnp.int32, (rows, n * rows), 1)
               < me * rows + lax.broadcasted_iota(jnp.int32, (rows, n * rows), 0)).astype(F32).astype(BF16)
    counts = jnp.dot(earlier, one_hot, preferred_element_type=F32)
    slot = jnp.sum(jnp.where(row_id == e_own, counts, 0.0), axis=-1, keepdims=True)
    keep_gate = jnp.where(slot < capacity, gate, 0.0)

    pad = jnp.zeros((128 - rows, width), F32)
    kt_ref[...] = jnp.concatenate([kv_ref[0], pad], axis=0).T
    vt_ref[...] = jnp.concatenate([kv_ref[1], pad], axis=0).T

    def patch_row(b, column, cache_ref):
        cache_ref[b] = jnp.where(lane == pos_ref[b], jnp.broadcast_to(column, (width, length)).astype(BF16), cache_ref[b])

    def patch_step(i, carry):
        kt = kt_ref[...]
        vt = vt_ref[...]
        for s in range(UNROLL):
            patch_row(i * UNROLL + s, kt[:, s:s + 1], k_ref)
            patch_row(i * UNROLL + s, vt[:, s:s + 1], v_ref)
        kt_ref[...] = pltpu.roll(kt, 128 - UNROLL, axis=1)
        vt_ref[...] = pltpu.roll(vt, 128 - UNROLL, axis=1)
        return carry
    lax.fori_loop(0, steps, patch_step, 0)

    all_of(yall_ref, peers, y_sem.at[0], y_sem.at[1], sib).wait_recv()
    x_all = yall_ref[...].reshape(n * rows, width)
    units = win_ref.shape[2]
    e_wide = jnp.concatenate([e_all] * (2 * units // 128), axis=1)
    second = (lax.broadcasted_iota(jnp.int32, (1, 2 * units), 1) >= units).astype(jnp.int32)
    for e in range(0, experts, 2):
        w_pair = jnp.concatenate([win_ref[e], win_ref[e + 1]], axis=1)
        u = jnp.maximum(jnp.dot(x_all, w_pair, preferred_element_type=F32), 0.0)
        u_ref[:, e * units:(e + 2) * units] = jnp.where(e_wide == e + second, u, 0.0).astype(BF16)

    chunk = part_ref.shape[4]
    parts = width // chunk
    chip, core = me // 2, lax.rem(me, 2)
    w_all = wout_ref.reshape(experts * units, width)
    for c in range(parts):
        acc = jnp.dot(u_ref[...], w_all[:, c * chunk:(c + 1) * chunk], preferred_element_type=F32)
        part_ref[c] = acc.reshape(n // 2, 2, rows, chunk)
        remote(part_ref.at[c, :, 1 - core], pair_ref.at[c], d_send.at[0], d_recv.at[c], sib).start()
    for c in range(parts):
        remote(pair_ref.at[c], pair_ref.at[c], d_send.at[0], d_recv.at[c], sib).wait_recv()
        pair_sum_ref[c] = part_ref[c, :, core] + pair_ref[c]
        rs_ref[c, chip] = pair_sum_ref[c, chip]
        for step in (2, 1, 3):
            target = lax.rem(chip + step, n // 2)
            remote(pair_sum_ref.at[c, target], rs_ref.at[c, chip], rs_send.at[0], rs_recv.at[c],
                   2 * target + core).start()
    others = n // 2 - 1
    for c in range(parts):
        all_of(rs_ref.at[c], others, rs_send.at[0], rs_recv.at[c], sib).wait_recv()
        y = jnp.sum(rs_ref[c], axis=0).astype(BF16).astype(F32)
        cols = slice(c * chunk, (c + 1) * chunk)
        out_ref[:, cols] = (h2[:, cols] + y * keep_gate).astype(BF16)
    for ref, sem in ((xall_ref, x_sem), (qrecv_ref, q_sem), (yall_ref, y_sem), (wr_ref, r_sem), (eall_ref, e_sem),
                     (wall_ref, w_send)):
        all_of(ref, peers, sem.at[0], sem.at[0], sib).wait_send()
    sent = rs_ref.at[:, pl.ds(0, others)]
    remote(sent, sent, rs_send.at[0], rs_send.at[0], sib).wait_send()
    remote(pair_ref, pair_ref, d_send.at[0], d_send.at[0], sib).wait_send()


def write_kernel(hid_ref, k_ref, v_ref, out_hbm, newk_hbm, newv_hbm, sem):
    span = k_ref.shape[0] // 4
    copies = [pltpu.make_async_copy(hid_ref, out_hbm, sem.at[8])]
    for i in range(4):
        rows = pl.ds(i * span, span)
        copies.append(pltpu.make_async_copy(k_ref.at[rows], newk_hbm.at[rows], sem.at[2 * i]))
        copies.append(pltpu.make_async_copy(v_ref.at[rows], newv_hbm.at[rows], sem.at[2 * i + 1]))
    for copy in copies:
        copy.start()
    for copy in copies:
        copy.wait()


def solution(mesh):
    n = mesh.shape['ws']
    row_axes = ('dp', 'ws')
    row_vec = P(row_axes)
    row_mat = P(row_axes, None)
    cache_spec = P(row_axes, None, None, None)
    col_split = P(None, 'ws')
    in_specs = (row_mat, cache_spec, cache_spec, cache_spec, cache_spec, row_vec, row_mat, P(None, None), row_vec,
                P(None), P(None), P(None), col_split, col_split, col_split, col_split, col_split, col_split,
                col_split, P(None, None, 'ws'), P(None, 'ws', None))
    out_specs = (row_mat, cache_spec, cache_spec)

    def decoder_block(hidden, self_k, self_v, cross_k, cross_v, positions, enc_mask, rel_bias, expert_idx,
                      ln_self, ln_cross, ln_ffn, wq_self, wk_self, wv_self, wo_self, wq_cross, wo_cross,
                      w_router, w_in, w_out):
        rows, width = hidden.shape
        heads, length, head_dim = self_k.shape[1:]
        src_len = cross_k.shape[2]
        share = width // n
        heads_pad = -(-heads // 16) * 16
        experts, _, units = w_in.shape
        capacity = (2 * rows * n + experts - 1) // experts
        chunk = 256

        def flat(cache):
            return jnp.swapaxes(cache, 2, 3).reshape(rows, width, cache.shape[2])

        dma = pltpu.SemaphoreType.DMA
        vmem, big_cache, big_src = pltpu.VMEM, (rows, width, length), (rows, width, src_len)
        parts, smem = width // chunk, pltpu.SMEM
        hid_out, k_v, v_v = pl.pallas_call(
            functools.partial(main_kernel, n, head_dim, capacity),
            out_shape=(vmem((rows, width), BF16), vmem(big_cache, BF16), vmem(big_cache, BF16)),
            in_specs=[HBM] * 21,
            out_specs=(VM,) * 3,
            scratch_shapes=[
                vmem(big_src, BF16), vmem(big_src, BF16), vmem(w_in.shape, BF16), vmem(w_out.shape, BF16),
                vmem((n, 3 * share, width), BF16),
                smem((rows,), jnp.int32), smem((rows,), jnp.int32), vmem((width,), F32), vmem((width,), F32),
                vmem((width,), F32), vmem((heads, length), F32), vmem((rows, src_len), jnp.int32),
                vmem((n, 1, width), F32), vmem((n, 1, 128), jnp.int32), vmem((n, rows, width), BF16),
                vmem((n, rows, width), BF16), vmem((rows, width), BF16), vmem((3, share, width), BF16),
                vmem((n * rows, 384), BF16), vmem((n, rows, 384), BF16), vmem((rows, width), F32),
                vmem((2, rows, width), F32), vmem((width, 128), F32), vmem((width, 128), F32),
                vmem((rows, heads_pad, length), F32), vmem((rows, heads_pad, length), BF16),
                vmem((rows, heads_pad, src_len), F32), vmem((rows, heads_pad, src_len), BF16), vmem((rows, width), F32),
                vmem((heads_pad, length), F32), vmem((n * rows, experts * units), BF16),
                vmem((parts, n // 2, 2, rows, chunk), F32), vmem((parts, n // 2, rows, chunk), F32),
                vmem((parts, n // 2, rows, chunk), F32), vmem((parts, n // 2, rows, chunk), F32),
                dma((12,)), dma((6,)), dma((2,)), dma((2,)), dma((2,)), dma((2,)), dma((2,)), dma((1,)), dma((3, 4)),
                dma((2,)), dma((1,)), dma((parts,)), dma((1,)), dma((parts,)),
            ],
            compiler_params=pltpu.CompilerParams(collective_id=0, has_side_effects=True,
                                                 vmem_limit_bytes=34 * 2 ** 20),
            name='main_part',
        )(*in_hbm(positions, expert_idx, hidden, ln_self, ln_cross, ln_ffn, rel_bias, enc_mask, w_router.T, wq_self.T,
                  wk_self.T, wv_self.T, wo_self.T, wq_cross.T, wo_cross.T, flat(self_k), flat(self_v), flat(cross_k),
                  flat(cross_v), w_in, w_out))

        out, newk, newv = pl.pallas_call(
            write_kernel,
            out_shape=(pltpu.HBM((rows, width), BF16), pltpu.HBM(big_cache, BF16), pltpu.HBM(big_cache, BF16)),
            in_specs=[VM] * 3,
            out_specs=(HBM,) * 3,
            scratch_shapes=[dma((9,))],
            compiler_params=pltpu.CompilerParams(has_side_effects=True, vmem_limit_bytes=2 ** 20),
            name='write_part',
        )(*in_vmem(hid_out, k_v, v_v))

        def unflat(cache):
            return jnp.swapaxes(cache.reshape(rows, heads, head_dim, length), 2, 3)
        return out, unflat(newk), unflat(newv)

    return jax.shard_map(decoder_block, mesh=mesh, in_specs=in_specs, out_specs=out_specs, check_vma=False)
```

```python
import functools
import jax
import jax.numpy as jnp
from jax import lax
from jax.experimental import pallas as pl
from jax.experimental.pallas import tpu as pltpu
from jax.sharding import PartitionSpec as P

EPSILON = 1e-6
NEG_BIG = -1e30
F32, BF16 = jnp.float32, jnp.bfloat16
MESH = pl.DeviceIdType.MESH
VM = pl.BlockSpec(memory_space=pltpu.VMEM)
HBM = pl.BlockSpec(memory_space=pltpu.HBM)
NT = (((1,), (1,)), ((), ()))
FROM_LEFT, FROM_RIGHT, FROM_FAR = 0, 1, 2
PEERS = ((2, 0), (2, 1), (1, 0), (3, 0), (1, 1), (3, 1), (0, 1))
UNROLL = 4


def in_hbm(*arrays):
    return [pltpu.with_memory_space_constraint(a, pltpu.HBM) for a in arrays]


def in_vmem(*arrays):
    return [pltpu.with_memory_space_constraint(a, pltpu.VMEM) for a in arrays]


def rms_norm(hid_f32, scale):
    inv_rms = lax.rsqrt(jnp.mean(hid_f32 * hid_f32, axis=-1, keepdims=True) + EPSILON)
    return (hid_f32 * inv_rms * scale).astype(BF16)


def dot_nt(a, b):
    return lax.dot_general(a, b, NT, preferred_element_type=F32)


def softmax_rows(scores):
    top = jnp.max(scores, axis=-1, keepdims=True)
    ex = jnp.exp(scores - top)
    return (ex / jnp.sum(ex, axis=-1, keepdims=True)).astype(BF16)


def make_dev(n):
    me = lax.axis_index('ws')
    chips = n // 2
    chip, core = me // 2, lax.rem(me, 2)

    def dev(step, other):
        return 2 * lax.rem(chip + step, chips) + ((1 - core) if other else core)
    return me, dev


def remote(src, dst, send_sem, recv_sem, dev):
    return pltpu.make_async_remote_copy(src_ref=src, dst_ref=dst, send_sem=send_sem, recv_sem=recv_sem,
                                        device_id={'ws': dev}, device_id_type=MESH)


def to_peers(dev, me, ref, send_sem, recv_sem):
    return [remote(ref.at[me], ref.at[me], send_sem, recv_sem, dev(*peer)) for peer in PEERS]


def all_of(ref, count, send_sem, recv_sem, dev):
    block = ref.at[pl.ds(0, count)]
    return remote(block, block, send_sem, recv_sem, dev)


def head_mask(heads_pad, width, head_dim):
    row = lax.broadcasted_iota(jnp.int32, (heads_pad, width), 0)
    col = lax.broadcasted_iota(jnp.int32, (heads_pad, width), 1)
    return (col // head_dim == row).astype(F32)


def main_kernel(n, head_dim, capacity, pos_hbm, eidx_hbm, hid_hbm, ln_hbm, lnc_hbm, lnf_hbm, rel_hbm, mask_hbm, wr_hbm,
                wq_hbm, wk_hbm, wv_hbm, wo_hbm, wqc_hbm, woc_hbm, k_hbm, v_hbm, ck_hbm, cv_hbm, win_hbm, wout_hbm,
                out_ref, k_ref, v_ref,
                ck_ref, cv_ref, win_ref, wout_ref, wall_ref, pos_ref, eidx_ref, ln_ref, lnc_ref, lnf_ref, rel_ref, mask_ref, wr_ref, eall_ref, xall_ref, yall_ref, hid_ref,
                wqkv_ref, qsend_ref, qrecv_ref, q_ref, kv_ref, kt_ref, vt_ref, s_ref, p_ref, s2_ref, p2_ref, ctx32_ref,
                rrev_ref, u_ref, part_ref, pair_ref, pair_sum_ref, rs_ref,
                in_sem, big_sem, x_sem, r_sem, e_sem, q_sem, y_sem, w_send, w_recv, pair_recv, d_send, d_recv, rs_send, rs_recv):
    me, dev = make_dev(n)
    rows, width, length = k_ref.shape
    heads_pad = s_ref.shape[1]
    share = width // n
    half = share // 2
    steps = rows // UNROLL
    peers = len(PEERS)

    barrier = pltpu.get_barrier_semaphore()
    for peer in PEERS:
        pl.semaphore_signal(barrier, inc=1, device_id={'ws': dev(*peer)}, device_id_type=MESH)

    mine = wall_ref.at[me]
    loads = [
        (hid_hbm, xall_ref.at[me], 0), (wr_hbm, wr_ref.at[me], 1), (ln_hbm, ln_ref, 2), (wq_hbm, wqkv_ref.at[0], 3),
        (wk_hbm, wqkv_ref.at[1], 3), (wv_hbm, wqkv_ref.at[2], 3), (rel_hbm, rel_ref, 4),
        (wo_hbm, mine.at[pl.ds(0, share)], 5), (wqc_hbm, mine.at[pl.ds(share, share)], 5),
        (woc_hbm, mine.at[pl.ds(2 * share, share)], 5), (eidx_hbm, eidx_ref, 6), (pos_hbm, pos_ref, 7),
        (lnc_hbm, lnc_ref, 8), (lnf_hbm, lnf_ref, 9), (mask_hbm, mask_ref, 10), (hid_hbm, hid_ref, 11),
    ]
    loads = [pltpu.make_async_copy(src, dst, in_sem.at[i]) for src, dst, i in loads]
    for load in loads:
        load.start()
    experts = win_ref.shape[0]
    lane_id = lax.broadcasted_iota(jnp.int32, (1, 128), 1)
    loads[0].wait()
    pl.semaphore_wait(barrier, n - 1)
    right, left, far, sib = dev(1, 0), dev(3, 0), dev(2, 0), dev(0, 1)

    def send_rows(owner, sem, target):
        remote(xall_ref.at[owner], xall_ref.at[owner], x_sem.at[0], x_sem.at[sem], target).start()

    def rows_over(owner, sem):
        remote(xall_ref.at[owner], xall_ref.at[owner], x_sem.at[0], x_sem.at[sem], sib).wait_recv()
        send_rows(owner, 4, sib)

    send_rows(me, 3, far)
    send_rows(me, 1, right)
    send_rows(me, 2, left)
    send_rows(me, 4, sib)
    pltpu.make_async_copy(mine, mine, in_sem.at[5]).wait()

    def half_of(owner, part):
        return wall_ref.at[owner, pl.ds(part * half, half)]

    def send_piece(owner, role, part, target):
        sem = pair_recv.at[part // 2] if role is None else w_recv.at[role, part]
        remote(half_of(owner, part), half_of(owner, part), w_send.at[0], sem, target).start()

    def wait_piece(owner, role, part):
        remote(half_of(owner, part), half_of(owner, part), w_send.at[0], w_recv.at[role, part], sib).wait_recv()

    def wait_pair(stage):
        block = wall_ref.at[pl.ds(0, n // 2), pl.ds(stage * share, share)]
        remote(block, block, w_send.at[0], pair_recv.at[stage], sib).wait_recv()

    def pass_on(first):
        wait_piece(left, FROM_LEFT, first)
        send_piece(left, FROM_FAR, first, right)
        wait_piece(right, FROM_RIGHT, first + 1)
        send_piece(right, FROM_FAR, first + 1, left)

    def send_own(*parts):
        for part in parts:
            send_piece(me, FROM_LEFT, part, right)
            send_piece(me, FROM_RIGHT, part + 1 if part % 2 == 0 else part - 1, left)

    send_own(0, 1, 2)
    loads[1].wait()
    loads[10].wait()
    e_row = jnp.zeros((1, 128), jnp.int32)
    for b in range(rows):
        e_row = jnp.where(lane_id == b, eidx_ref[b], e_row)
    eall_ref[me] = e_row
    big = [pltpu.make_async_copy(src, dst, big_sem.at[i]) for i, (src, dst) in
           enumerate([(k_hbm, k_ref), (v_hbm, v_ref), (ck_hbm, ck_ref), (cv_hbm, cv_ref), (win_hbm, win_ref), (wout_hbm, wout_ref)])]
    for load in big:
        load.start()

    loads[6].wait()
    rel = jnp.concatenate([rel_ref[...], jnp.zeros((heads_pad - rel_ref.shape[0], length), F32)], axis=0)
    flip = (lax.broadcasted_iota(jnp.int32, (length, length), 0) + lax.broadcasted_iota(jnp.int32, (length, length), 1)
            == length - 1).astype(F32).astype(BF16)
    hi = rel.astype(BF16)
    rest = rel - hi.astype(F32)
    mid = rest.astype(BF16)
    low = (rest - mid.astype(F32)).astype(BF16)
    rrev_ref[...] = (jnp.dot(hi, flip, preferred_element_type=F32) + jnp.dot(mid, flip, preferred_element_type=F32)
                     + jnp.dot(low, flip, preferred_element_type=F32))
    qsend_ref[...] = jnp.zeros_like(qsend_ref)

    rows_over(left, 1)
    rows_over(right, 2)
    for load in loads[2:3] + loads[11:]:
        load.wait()
    pltpu.make_async_copy(wqkv_ref, wqkv_ref, in_sem.at[3]).wait()
    rows_over(far, 3)
    all_of(xall_ref, n // 2, x_sem.at[0], x_sem.at[4], sib).wait_recv()
    x_norm = rms_norm(xall_ref[...].reshape(n * rows, width).astype(F32), ln_ref[...][None])
    for part in range(3):
        qsend_ref[:, part * 128:part * 128 + share] = dot_nt(x_norm, wqkv_ref[part]).astype(BF16)
    for peer in PEERS:
        dst = dev(*peer)
        remote(qsend_ref.at[pl.ds(dst * rows, rows)], qrecv_ref.at[me], q_sem.at[0], q_sem.at[1], dst).start()
    qrecv_ref[me] = qsend_ref[pl.ds(pl.multiple_of(me * rows, rows), rows), :]
    pass_on(0)
    send_own(3)
    for part in range(6):
        send_piece(me, None, part, sib)

    all_of(qrecv_ref, peers, q_sem.at[0], q_sem.at[1], sib).wait_recv()
    def far_over(first):
        for part in (first, first + 1):
            wait_piece(far, FROM_FAR, part)
            send_piece(far, None, part, sib)

    pass_on(2)
    send_own(4, 5)
    for copy in (to_peers(dev, me, wr_ref, r_sem.at[0], r_sem.at[1])
                 + to_peers(dev, me, eall_ref, e_sem.at[0], e_sem.at[1])):
        copy.start()
    wait_piece(left, FROM_LEFT, 1)
    wait_piece(right, FROM_RIGHT, 0)
    for part in (0, 1):
        send_piece(left, None, part, sib)
        send_piece(right, None, part, sib)
    send_piece(left, None, 2, sib)
    send_piece(right, None, 3, sib)

    def columns(part):
        return jnp.concatenate([qrecv_ref[s][:, part * 128:part * 128 + share] for s in range(n)], axis=1).astype(F32)
    q_ref[...] = columns(0)
    kv_ref[0] = columns(1)
    kv_ref[1] = columns(2)

    h_mask = head_mask(heads_pad, width, head_dim)
    lane = lax.broadcasted_iota(jnp.int32, (1, length), 1)

    big[0].wait()

    def score_step(i, carry):
        for s in range(UNROLL):
            b = i * UNROLL + s
            pos = pos_ref[b]
            q_diag = q_ref[pl.ds(b, 1), :] * h_mask
            scores = jnp.dot(q_diag.astype(BF16), k_ref[b], preferred_element_type=F32)
            new = jnp.sum(q_diag * kv_ref[0, pl.ds(b, 1), :], axis=1, keepdims=True)
            bias = pltpu.roll(rrev_ref[...], pos + 1, axis=1)
            s_ref[b] = jnp.where(lane <= pos, jnp.where(lane == pos, new, scores) + bias, NEG_BIG)
        return carry
    lax.fori_loop(0, steps, score_step, 0)

    p_ref[...] = softmax_rows(s_ref[...])

    big[1].wait()

    def value_step(i, carry):
        for s in range(UNROLL):
            b = i * UNROLL + s
            here = lane == pos_ref[b]
            probs = p_ref[b].astype(F32)
            new = jnp.sum(jnp.where(here, probs, 0.0), axis=1, keepdims=True)
            spread = dot_nt(jnp.where(here, 0.0, probs).astype(BF16), v_ref[b])
            spread = spread + new * kv_ref[1, pl.ds(b, 1), :]
            ctx32_ref[pl.ds(b, 1), :] = jnp.sum(spread * h_mask, axis=0, keepdims=True)
        return carry
    lax.fori_loop(0, steps // 2, value_step, 0)
    far_over(0)
    wait_piece(left, FROM_LEFT, 3)
    send_piece(left, None, 3, sib)
    wait_piece(right, FROM_RIGHT, 2)
    send_piece(right, None, 2, sib)
    lax.fori_loop(steps // 2, steps, value_step, 0)

    far_over(2)
    wait_pair(0)
    wo = wall_ref[:, 0:share, :].reshape(width, width)
    h1 = (hid_ref[...].astype(F32) + dot_nt(ctx32_ref[...].astype(BF16), wo)).astype(BF16).astype(F32)
    wait_pair(1)
    wqc = wall_ref[:, share:2 * share, :].reshape(width, width)
    q_ref[...] = dot_nt(rms_norm(h1, lnc_ref[...][None]), wqc).astype(BF16).astype(F32)
    pass_on(4)
    send_piece(left, None, 4, sib)
    send_piece(right, None, 5, sib)
    for load in big[2:]:
        load.wait()

    def cross_score(i, carry):
        for s in range(UNROLL):
            b = i * UNROLL + s
            q_diag = (q_ref[pl.ds(b, 1), :] * h_mask).astype(BF16)
            scores = jnp.dot(q_diag, ck_ref[b], preferred_element_type=F32)
            s2_ref[b] = jnp.where(mask_ref[pl.ds(b, 1), :] == 1, scores, NEG_BIG)
        return carry
    lax.fori_loop(0, steps, cross_score, 0)
    wait_piece(left, FROM_LEFT, 5)
    send_piece(left, None, 5, sib)
    wait_piece(right, FROM_RIGHT, 4)
    send_piece(right, None, 4, sib)
    p2_ref[...] = softmax_rows(s2_ref[...])

    def cross_value(i, carry):
        for s in range(UNROLL):
            b = i * UNROLL + s
            spread = dot_nt(p2_ref[b], cv_ref[b])
            ctx32_ref[pl.ds(b, 1), :] = jnp.sum(spread * h_mask, axis=0, keepdims=True)
        return carry
    lax.fori_loop(0, steps, cross_value, 0)

    far_over(4)
    wait_pair(2)
    woc = wall_ref[:, 2 * share:3 * share, :].reshape(width, width)
    h2 = (h1 + dot_nt(ctx32_ref[...].astype(BF16), woc)).astype(BF16).astype(F32)
    x_own = rms_norm(h2, lnf_ref[...][None])
    yall_ref[me] = x_own
    for copy in to_peers(dev, me, yall_ref, y_sem.at[0], y_sem.at[1]):
        copy.start()

    all_of(wr_ref, peers, r_sem.at[0], r_sem.at[1], sib).wait_recv()
    all_of(eall_ref, peers, e_sem.at[0], e_sem.at[1], sib).wait_recv()
    x_f32 = x_own.astype(F32)
    logits = [jnp.sum(x_f32 * wr_ref[e], axis=-1, keepdims=True) for e in range(experts)]
    top = functools.reduce(jnp.maximum, logits)
    ex = [jnp.exp(v - top) for v in logits]
    total = functools.reduce(jnp.add, ex)
    e_pad = jnp.concatenate([eall_ref[...].reshape(n, 128), jnp.zeros((128 - n, 128), jnp.int32)], axis=0)
    e_cols = e_pad.astype(F32).T.astype(jnp.int32)
    e_all = jnp.concatenate([jnp.broadcast_to(e_cols[0:rows, s:s + 1], (rows, 128)) for s in range(n)], axis=0)
    row_id = lax.broadcasted_iota(jnp.int32, (rows, 128), 1)
    source = lax.broadcasted_iota(jnp.int32, (rows, 128), 1)
    e_own = jnp.sum(jnp.where(source == me, e_cols[0:rows, :], 0).astype(F32), axis=1, keepdims=True).astype(jnp.int32)
    gate = functools.reduce(jnp.add, [jnp.where(e_own == e, ex[e], 0.0) for e in range(experts)]) / total
    one_hot = (e_all == lax.broadcasted_iota(jnp.int32, (n * rows, 128), 1)).astype(F32).astype(BF16)
    earlier = (lax.broadcasted_iota(jnp.int32, (rows, n * rows), 1)
               < me * rows + lax.broadcasted_iota(jnp.int32, (rows, n * rows), 0)).astype(F32).astype(BF16)
    counts = jnp.dot(earlier, one_hot, preferred_element_type=F32)
    slot = jnp.sum(jnp.where(row_id == e_own, counts, 0.0), axis=-1, keepdims=True)
    keep_gate = jnp.where(slot < capacity, gate, 0.0)

    pad = jnp.zeros((128 - rows, width), F32)
    kt_ref[...] = jnp.concatenate([kv_ref[0], pad], axis=0).T
    vt_ref[...] = jnp.concatenate([kv_ref[1], pad], axis=0).T

    def patch_row(b, column, cache_ref):
        cache_ref[b] = jnp.where(lane == pos_ref[b], jnp.broadcast_to(column, (width, length)).astype(BF16), cache_ref[b])

    def patch_step(i, carry):
        kt = kt_ref[...]
        vt = vt_ref[...]
        for s in range(UNROLL):
            patch_row(i * UNROLL + s, kt[:, s:s + 1], k_ref)
            patch_row(i * UNROLL + s, vt[:, s:s + 1], v_ref)
        kt_ref[...] = pltpu.roll(kt, 128 - UNROLL, axis=1)
        vt_ref[...] = pltpu.roll(vt, 128 - UNROLL, axis=1)
        return carry
    lax.fori_loop(0, steps, patch_step, 0)

    all_of(yall_ref, peers, y_sem.at[0], y_sem.at[1], sib).wait_recv()
    x_all = yall_ref[...].reshape(n * rows, width)
    units = win_ref.shape[2]
    e_wide = jnp.concatenate([e_all] * (2 * units // 128), axis=1)
    second = (lax.broadcasted_iota(jnp.int32, (1, 2 * units), 1) >= units).astype(jnp.int32)
    for e in range(0, experts, 2):
        w_pair = jnp.concatenate([win_ref[e], win_ref[e + 1]], axis=1)
        u = jnp.maximum(jnp.dot(x_all, w_pair, preferred_element_type=F32), 0.0)
        u_ref[:, e * units:(e + 2) * units] = jnp.where(e_wide == e + second, u, 0.0).astype(BF16)

    chunk = part_ref.shape[4]
    parts = width // chunk
    chip, core = me // 2, lax.rem(me, 2)
    w_all = wout_ref.reshape(experts * units, width)
    for c in range(parts):
        acc = jnp.dot(u_ref[...], w_all[:, c * chunk:(c + 1) * chunk], preferred_element_type=F32)
        part_ref[c] = acc.reshape(n // 2, 2, rows, chunk)
        remote(part_ref.at[c, :, 1 - core], pair_ref.at[c], d_send.at[0], d_recv.at[c], sib).start()
    for c in range(parts):
        remote(pair_ref.at[c], pair_ref.at[c], d_send.at[0], d_recv.at[c], sib).wait_recv()
        pair_sum_ref[c] = part_ref[c, :, core] + pair_ref[c]
        rs_ref[c, chip] = pair_sum_ref[c, chip]
        for step in (2, 1, 3):
            target = lax.rem(chip + step, n // 2)
            remote(pair_sum_ref.at[c, target], rs_ref.at[c, chip], rs_send.at[0], rs_recv.at[c],
                   2 * target + core).start()
    others = n // 2 - 1
    for c in range(parts):
        all_of(rs_ref.at[c], others, rs_send.at[0], rs_recv.at[c], sib).wait_recv()
        y = jnp.sum(rs_ref[c], axis=0).astype(BF16).astype(F32)
        cols = slice(c * chunk, (c + 1) * chunk)
        out_ref[:, cols] = (h2[:, cols] + y * keep_gate).astype(BF16)
    for ref, sem in ((xall_ref, x_sem), (qrecv_ref, q_sem), (yall_ref, y_sem), (wr_ref, r_sem), (eall_ref, e_sem),
                     (wall_ref, w_send)):
        all_of(ref, peers, sem.at[0], sem.at[0], sib).wait_send()
    sent = rs_ref.at[:, pl.ds(0, others)]
    remote(sent, sent, rs_send.at[0], rs_send.at[0], sib).wait_send()
    remote(pair_ref, pair_ref, d_send.at[0], d_send.at[0], sib).wait_send()


def write_kernel(hid_ref, k_ref, v_ref, out_hbm, newk_hbm, newv_hbm, sem):
    span = k_ref.shape[0] // 4
    copies = [pltpu.make_async_copy(hid_ref, out_hbm, sem.at[8])]
    for i in range(4):
        rows = pl.ds(i * span, span)
        copies.append(pltpu.make_async_copy(k_ref.at[rows], newk_hbm.at[rows], sem.at[2 * i]))
        copies.append(pltpu.make_async_copy(v_ref.at[rows], newv_hbm.at[rows], sem.at[2 * i + 1]))
    for copy in copies:
        copy.start()
    for copy in copies:
        copy.wait()


def solution(mesh):
    n = mesh.shape['ws']
    row_axes = ('dp', 'ws')
    row_vec = P(row_axes)
    row_mat = P(row_axes, None)
    cache_spec = P(row_axes, None, None, None)
    col_split = P(None, 'ws')
    in_specs = (row_mat, cache_spec, cache_spec, cache_spec, cache_spec, row_vec, row_mat, P(None, None), row_vec,
                P(None), P(None), P(None), col_split, col_split, col_split, col_split, col_split, col_split,
                col_split, P(None, None, 'ws'), P(None, 'ws', None))
    out_specs = (row_mat, cache_spec, cache_spec)

    def decoder_block(hidden, self_k, self_v, cross_k, cross_v, positions, enc_mask, rel_bias, expert_idx,
                      ln_self, ln_cross, ln_ffn, wq_self, wk_self, wv_self, wo_self, wq_cross, wo_cross,
                      w_router, w_in, w_out):
        rows, width = hidden.shape
        heads, length, head_dim = self_k.shape[1:]
        src_len = cross_k.shape[2]
        share = width // n
        heads_pad = -(-heads // 16) * 16
        experts, _, units = w_in.shape
        capacity = (2 * rows * n + experts - 1) // experts
        chunk = 256

        def flat(cache):
            return jnp.swapaxes(cache, 2, 3).reshape(rows, width, cache.shape[2])

        dma = pltpu.SemaphoreType.DMA
        vmem, big_cache, big_src = pltpu.VMEM, (rows, width, length), (rows, width, src_len)
        parts, smem = width // chunk, pltpu.SMEM
        hid_out, k_v, v_v = pl.pallas_call(
            functools.partial(main_kernel, n, head_dim, capacity),
            out_shape=(vmem((rows, width), BF16), vmem(big_cache, BF16), vmem(big_cache, BF16)),
            in_specs=[HBM] * 21,
            out_specs=(VM,) * 3,
            scratch_shapes=[
                vmem(big_src, BF16), vmem(big_src, BF16), vmem(w_in.shape, BF16), vmem(w_out.shape, BF16),
                vmem((n, 3 * share, width), BF16),
                smem((rows,), jnp.int32), smem((rows,), jnp.int32), vmem((width,), F32), vmem((width,), F32),
                vmem((width,), F32), vmem((heads, length), F32), vmem((rows, src_len), jnp.int32),
                vmem((n, 1, width), F32), vmem((n, 1, 128), jnp.int32), vmem((n, rows, width), BF16),
                vmem((n, rows, width), BF16), vmem((rows, width), BF16), vmem((3, share, width), BF16),
                vmem((n * rows, 384), BF16), vmem((n, rows, 384), BF16), vmem((rows, width), F32),
                vmem((2, rows, width), F32), vmem((width, 128), F32), vmem((width, 128), F32),
                vmem((rows, heads_pad, length), F32), vmem((rows, heads_pad, length), BF16),
                vmem((rows, heads_pad, src_len), F32), vmem((rows, heads_pad, src_len), BF16), vmem((rows, width), F32),
                vmem((heads_pad, length), F32), vmem((n * rows, experts * units), BF16),
                vmem((parts, n // 2, 2, rows, chunk), F32), vmem((parts, n // 2, rows, chunk), F32),
                vmem((parts, n // 2, rows, chunk), F32), vmem((parts, n // 2, rows, chunk), F32),
                dma((12,)), dma((6,)), dma((5,)), dma((2,)), dma((2,)), dma((2,)), dma((2,)), dma((1,)), dma((3, 6)),
                dma((3,)), dma((1,)), dma((parts,)), dma((1,)), dma((parts,)),
            ],
            compiler_params=pltpu.CompilerParams(collective_id=0, has_side_effects=True,
                                                 vmem_limit_bytes=34 * 2 ** 20),
            name='main_part',
        )(*in_hbm(positions, expert_idx, hidden, ln_self, ln_cross, ln_ffn, rel_bias, enc_mask, w_router.T, wq_self.T,
                  wk_self.T, wv_self.T, wo_self.T, wq_cross.T, wo_cross.T, flat(self_k), flat(self_v), flat(cross_k),
                  flat(cross_v), w_in, w_out))

        out, newk, newv = pl.pallas_call(
            write_kernel,
            out_shape=(pltpu.HBM((rows, width), BF16), pltpu.HBM(big_cache, BF16), pltpu.HBM(big_cache, BF16)),
            in_specs=[VM] * 3,
            out_specs=(HBM,) * 3,
            scratch_shapes=[dma((9,))],
            compiler_params=pltpu.CompilerParams(has_side_effects=True, vmem_limit_bytes=2 ** 20),
            name='write_part',
        )(*in_vmem(hid_out, k_v, v_v))

        def unflat(cache):
            return jnp.swapaxes(cache.reshape(rows, heads, head_dim, length), 2, 3)
        return out, unflat(newk), unflat(newv)

    return jax.shard_map(decoder_block, mesh=mesh, in_specs=in_specs, out_specs=out_specs, check_vma=False)
```

```python
import functools
import jax
import jax.numpy as jnp
from jax import lax
from jax.experimental import pallas as pl
from jax.experimental.pallas import tpu as pltpu
from jax.sharding import PartitionSpec as P

EPSILON = 1e-6
NEG_BIG = -1e30
F32, BF16 = jnp.float32, jnp.bfloat16
MESH = pl.DeviceIdType.MESH
VM = pl.BlockSpec(memory_space=pltpu.VMEM)
HBM = pl.BlockSpec(memory_space=pltpu.HBM)
NT = (((1,), (1,)), ((), ()))
FROM_LEFT, FROM_RIGHT, FROM_FAR = 0, 1, 2
PEERS = ((2, 0), (2, 1), (1, 0), (3, 0), (1, 1), (3, 1), (0, 1))
UNROLL = 8


def in_hbm(*arrays):
    return [pltpu.with_memory_space_constraint(a, pltpu.HBM) for a in arrays]


def in_vmem(*arrays):
    return [pltpu.with_memory_space_constraint(a, pltpu.VMEM) for a in arrays]


def rms_norm(hid_f32, scale):
    inv_rms = lax.rsqrt(jnp.mean(hid_f32 * hid_f32, axis=-1, keepdims=True) + EPSILON)
    return (hid_f32 * inv_rms * scale).astype(BF16)


def dot_nt(a, b):
    return lax.dot_general(a, b, NT, preferred_element_type=F32)


def softmax_rows(scores):
    top = jnp.max(scores, axis=-1, keepdims=True)
    ex = jnp.exp(scores - top)
    return (ex / jnp.sum(ex, axis=-1, keepdims=True)).astype(BF16)


def make_dev(n):
    me = lax.axis_index('ws')
    chips = n // 2
    chip, core = me // 2, lax.rem(me, 2)

    def dev(step, other):
        return 2 * lax.rem(chip + step, chips) + ((1 - core) if other else core)
    return me, dev


def remote(src, dst, send_sem, recv_sem, dev):
    return pltpu.make_async_remote_copy(src_ref=src, dst_ref=dst, send_sem=send_sem, recv_sem=recv_sem,
                                        device_id={'ws': dev}, device_id_type=MESH)


def to_peers(dev, me, ref, send_sem, recv_sem):
    return [remote(ref.at[me], ref.at[me], send_sem, recv_sem, dev(*peer)) for peer in PEERS]


def all_of(ref, count, send_sem, recv_sem, dev):
    block = ref.at[pl.ds(0, count)]
    return remote(block, block, send_sem, recv_sem, dev)


def head_mask(heads_pad, width, head_dim):
    row = lax.broadcasted_iota(jnp.int32, (heads_pad, width), 0)
    col = lax.broadcasted_iota(jnp.int32, (heads_pad, width), 1)
    return (col // head_dim == row).astype(F32)


def main_kernel(n, head_dim, capacity, pos_hbm, eidx_hbm, hid_hbm, ln_hbm, lnc_hbm, lnf_hbm, rel_hbm, mask_hbm, wr_hbm,
                wq_hbm, wk_hbm, wv_hbm, wo_hbm, wqc_hbm, woc_hbm, k_hbm, v_hbm, ck_hbm, cv_hbm, win_hbm, wout_hbm,
                out_ref, k_ref, v_ref,
                ck_ref, cv_ref, win_ref, wout_ref, wall_ref, pos_ref, eidx_ref, ln_ref, lnc_ref, lnf_ref, rel_ref, mask_ref, wr_ref, eall_ref, xall_ref, yall_ref, hid_ref,
                wqkv_ref, qsend_ref, qrecv_ref, q_ref, kv_ref, kt_ref, vt_ref, s_ref, p_ref, s2_ref, p2_ref, ctx32_ref,
                rrev_ref, u_ref, part_ref, pair_ref, pair_sum_ref, rs_ref,
                in_sem, big_sem, x_sem, r_sem, e_sem, q_sem, y_sem, w_send, w_recv, pair_recv, d_send, d_recv, rs_send, rs_recv):
    me, dev = make_dev(n)
    rows, width, length = k_ref.shape
    heads_pad = s_ref.shape[1]
    share = width // n
    half = share // 2
    steps = rows // UNROLL
    peers = len(PEERS)

    barrier = pltpu.get_barrier_semaphore()
    for peer in PEERS:
        pl.semaphore_signal(barrier, inc=1, device_id={'ws': dev(*peer)}, device_id_type=MESH)

    mine = wall_ref.at[me]
    loads = [
        (hid_hbm, xall_ref.at[me], 0), (wr_hbm, wr_ref.at[me], 1), (ln_hbm, ln_ref, 2), (wq_hbm, wqkv_ref.at[0], 3),
        (wk_hbm, wqkv_ref.at[1], 3), (wv_hbm, wqkv_ref.at[2], 3), (rel_hbm, rel_ref, 4),
        (wo_hbm, mine.at[pl.ds(0, share)], 5), (wqc_hbm, mine.at[pl.ds(share, share)], 5),
        (woc_hbm, mine.at[pl.ds(2 * share, share)], 5), (eidx_hbm, eidx_ref, 6), (pos_hbm, pos_ref, 7),
        (lnc_hbm, lnc_ref, 8), (lnf_hbm, lnf_ref, 9), (mask_hbm, mask_ref, 10), (hid_hbm, hid_ref, 11),
    ]
    loads = [pltpu.make_async_copy(src, dst, in_sem.at[i]) for src, dst, i in loads]
    for load in loads:
        load.start()
    experts = win_ref.shape[0]
    lane_id = lax.broadcasted_iota(jnp.int32, (1, 128), 1)
    loads[0].wait()
    pl.semaphore_wait(barrier, n - 1)
    right, left, far, sib = dev(1, 0), dev(3, 0), dev(2, 0), dev(0, 1)

    def send_rows(owner, sem, target):
        remote(xall_ref.at[owner], xall_ref.at[owner], x_sem.at[0], x_sem.at[sem], target).start()

    def rows_over(owner, sem):
        remote(xall_ref.at[owner], xall_ref.at[owner], x_sem.at[0], x_sem.at[sem], sib).wait_recv()
        send_rows(owner, 4, sib)

    send_rows(me, 3, far)
    send_rows(me, 1, right)
    send_rows(me, 2, left)
    send_rows(me, 4, sib)
    pltpu.make_async_copy(mine, mine, in_sem.at[5]).wait()

    def half_of(owner, part):
        return wall_ref.at[owner, pl.ds(part * half, half)]

    def send_piece(owner, role, part, target):
        sem = pair_recv.at[part // 2] if role is None else w_recv.at[role, part]
        remote(half_of(owner, part), half_of(owner, part), w_send.at[0], sem, target).start()

    def wait_piece(owner, role, part):
        remote(half_of(owner, part), half_of(owner, part), w_send.at[0], w_recv.at[role, part], sib).wait_recv()

    def wait_pair(stage):
        block = wall_ref.at[pl.ds(0, n // 2), pl.ds(stage * share, share)]
        remote(block, block, w_send.at[0], pair_recv.at[stage], sib).wait_recv()

    def pass_on(first):
        wait_piece(left, FROM_LEFT, first)
        send_piece(left, FROM_FAR, first, right)
        wait_piece(right, FROM_RIGHT, first + 1)
        send_piece(right, FROM_FAR, first + 1, left)

    def send_own(*parts):
        for part in parts:
            send_piece(me, FROM_LEFT, part, right)
            send_piece(me, FROM_RIGHT, part + 1 if part % 2 == 0 else part - 1, left)

    send_own(0, 1, 2)
    loads[1].wait()
    loads[10].wait()
    e_row = jnp.zeros((1, 128), jnp.int32)
    for b in range(rows):
        e_row = jnp.where(lane_id == b, eidx_ref[b], e_row)
    eall_ref[me] = e_row
    big = [pltpu.make_async_copy(src, dst, big_sem.at[i]) for i, (src, dst) in
           enumerate([(k_hbm, k_ref), (v_hbm, v_ref), (ck_hbm, ck_ref), (cv_hbm, cv_ref), (win_hbm, win_ref), (wout_hbm, wout_ref)])]
    for load in big:
        load.start()

    loads[6].wait()
    rel = jnp.concatenate([rel_ref[...], jnp.zeros((heads_pad - rel_ref.shape[0], length), F32)], axis=0)
    flip = (lax.broadcasted_iota(jnp.int32, (length, length), 0) + lax.broadcasted_iota(jnp.int32, (length, length), 1)
            == length - 1).astype(F32).astype(BF16)
    hi = rel.astype(BF16)
    rest = rel - hi.astype(F32)
    mid = rest.astype(BF16)
    low = (rest - mid.astype(F32)).astype(BF16)
    rrev_ref[...] = (jnp.dot(hi, flip, preferred_element_type=F32) + jnp.dot(mid, flip, preferred_element_type=F32)
                     + jnp.dot(low, flip, preferred_element_type=F32))
    qsend_ref[...] = jnp.zeros_like(qsend_ref)

    rows_over(left, 1)
    rows_over(right, 2)
    for load in loads[2:3] + loads[11:]:
        load.wait()
    pltpu.make_async_copy(wqkv_ref, wqkv_ref, in_sem.at[3]).wait()
    rows_over(far, 3)
    all_of(xall_ref, n // 2, x_sem.at[0], x_sem.at[4], sib).wait_recv()
    x_norm = rms_norm(xall_ref[...].reshape(n * rows, width).astype(F32), ln_ref[...][None])
    for part in range(3):
        qsend_ref[:, part * 128:part * 128 + share] = dot_nt(x_norm, wqkv_ref[part]).astype(BF16)
    for peer in PEERS:
        dst = dev(*peer)
        remote(qsend_ref.at[pl.ds(dst * rows, rows)], qrecv_ref.at[me], q_sem.at[0], q_sem.at[1], dst).start()
    qrecv_ref[me] = qsend_ref[pl.ds(pl.multiple_of(me * rows, rows), rows), :]
    pass_on(0)
    send_own(3)
    for part in range(6):
        send_piece(me, None, part, sib)

    all_of(qrecv_ref, peers, q_sem.at[0], q_sem.at[1], sib).wait_recv()
    def far_over(first):
        for part in (first, first + 1):
            wait_piece(far, FROM_FAR, part)
            send_piece(far, None, part, sib)

    pass_on(2)
    send_own(4, 5)
    for copy in (to_peers(dev, me, wr_ref, r_sem.at[0], r_sem.at[1])
                 + to_peers(dev, me, eall_ref, e_sem.at[0], e_sem.at[1])):
        copy.start()
    wait_piece(left, FROM_LEFT, 1)
    wait_piece(right, FROM_RIGHT, 0)
    for part in (0, 1):
        send_piece(left, None, part, sib)
        send_piece(right, None, part, sib)
    send_piece(left, None, 2, sib)
    send_piece(right, None, 3, sib)

    def columns(part):
        return jnp.concatenate([qrecv_ref[s][:, part * 128:part * 128 + share] for s in range(n)], axis=1).astype(F32)
    q_ref[...] = columns(0)
    kv_ref[0] = columns(1)
    kv_ref[1] = columns(2)

    h_mask = head_mask(heads_pad, width, head_dim)
    lane = lax.broadcasted_iota(jnp.int32, (1, length), 1)

    big[0].wait()

    def score_step(i, carry):
        for s in range(UNROLL):
            b = i * UNROLL + s
            pos = pos_ref[b]
            q_diag = q_ref[pl.ds(b, 1), :] * h_mask
            scores = jnp.dot(q_diag.astype(BF16), k_ref[b], preferred_element_type=F32)
            new = jnp.sum(q_diag * kv_ref[0, pl.ds(b, 1), :], axis=1, keepdims=True)
            bias = pltpu.roll(rrev_ref[...], pos + 1, axis=1)
            s_ref[b] = jnp.where(lane <= pos, jnp.where(lane == pos, new, scores) + bias, NEG_BIG)
        return carry
    lax.fori_loop(0, steps, score_step, 0)

    p_ref[...] = softmax_rows(s_ref[...])

    big[1].wait()

    def value_step(i, carry):
        for s in range(UNROLL):
            b = i * UNROLL + s
            here = lane == pos_ref[b]
            probs = p_ref[b].astype(F32)
            new = jnp.sum(jnp.where(here, probs, 0.0), axis=1, keepdims=True)
            spread = dot_nt(jnp.where(here, 0.0, probs).astype(BF16), v_ref[b])
            spread = spread + new * kv_ref[1, pl.ds(b, 1), :]
            ctx32_ref[pl.ds(b, 1), :] = jnp.sum(spread * h_mask, axis=0, keepdims=True)
        return carry
    lax.fori_loop(0, steps // 2, value_step, 0)
    far_over(0)
    wait_piece(left, FROM_LEFT, 3)
    send_piece(left, None, 3, sib)
    wait_piece(right, FROM_RIGHT, 2)
    send_piece(right, None, 2, sib)
    lax.fori_loop(steps // 2, steps, value_step, 0)

    far_over(2)
    wait_pair(0)
    wo = wall_ref[:, 0:share, :].reshape(width, width)
    h1 = (hid_ref[...].astype(F32) + dot_nt(ctx32_ref[...].astype(BF16), wo)).astype(BF16).astype(F32)
    pass_on(4)
    send_piece(left, None, 4, sib)
    send_piece(right, None, 5, sib)
    wait_pair(1)
    wqc = wall_ref[:, share:2 * share, :].reshape(width, width)
    q_ref[...] = dot_nt(rms_norm(h1, lnc_ref[...][None]), wqc).astype(BF16).astype(F32)
    for load in big[2:]:
        load.wait()

    def cross_score(i, carry):
        for s in range(UNROLL):
            b = i * UNROLL + s
            q_diag = (q_ref[pl.ds(b, 1), :] * h_mask).astype(BF16)
            scores = jnp.dot(q_diag, ck_ref[b], preferred_element_type=F32)
            s2_ref[b] = jnp.where(mask_ref[pl.ds(b, 1), :] == 1, scores, NEG_BIG)
        return carry
    lax.fori_loop(0, steps, cross_score, 0)
    wait_piece(left, FROM_LEFT, 5)
    send_piece(left, None, 5, sib)
    wait_piece(right, FROM_RIGHT, 4)
    send_piece(right, None, 4, sib)
    p2_ref[...] = softmax_rows(s2_ref[...])

    def cross_value(i, carry):
        for s in range(UNROLL):
            b = i * UNROLL + s
            spread = dot_nt(p2_ref[b], cv_ref[b])
            ctx32_ref[pl.ds(b, 1), :] = jnp.sum(spread * h_mask, axis=0, keepdims=True)
        return carry
    lax.fori_loop(0, steps // 2, cross_value, 0)
    far_over(4)
    lax.fori_loop(steps // 2, steps, cross_value, 0)

    wait_pair(2)
    woc = wall_ref[:, 2 * share:3 * share, :].reshape(width, width)
    h2 = (h1 + dot_nt(ctx32_ref[...].astype(BF16), woc)).astype(BF16).astype(F32)
    x_own = rms_norm(h2, lnf_ref[...][None])
    yall_ref[me] = x_own
    for copy in to_peers(dev, me, yall_ref, y_sem.at[0], y_sem.at[1]):
        copy.start()

    all_of(wr_ref, peers, r_sem.at[0], r_sem.at[1], sib).wait_recv()
    all_of(eall_ref, peers, e_sem.at[0], e_sem.at[1], sib).wait_recv()
    x_f32 = x_own.astype(F32)
    logits = [jnp.sum(x_f32 * wr_ref[e], axis=-1, keepdims=True) for e in range(experts)]
    top = functools.reduce(jnp.maximum, logits)
    ex = [jnp.exp(v - top) for v in logits]
    total = functools.reduce(jnp.add, ex)
    e_pad = jnp.concatenate([eall_ref[...].reshape(n, 128), jnp.zeros((128 - n, 128), jnp.int32)], axis=0)
    e_cols = e_pad.astype(F32).T.astype(jnp.int32)
    e_all = jnp.concatenate([jnp.broadcast_to(e_cols[0:rows, s:s + 1], (rows, 128)) for s in range(n)], axis=0)
    row_id = lax.broadcasted_iota(jnp.int32, (rows, 128), 1)
    source = lax.broadcasted_iota(jnp.int32, (rows, 128), 1)
    e_own = jnp.sum(jnp.where(source == me, e_cols[0:rows, :], 0).astype(F32), axis=1, keepdims=True).astype(jnp.int32)
    gate = functools.reduce(jnp.add, [jnp.where(e_own == e, ex[e], 0.0) for e in range(experts)]) / total
    one_hot = (e_all == lax.broadcasted_iota(jnp.int32, (n * rows, 128), 1)).astype(F32).astype(BF16)
    earlier = (lax.broadcasted_iota(jnp.int32, (rows, n * rows), 1)
               < me * rows + lax.broadcasted_iota(jnp.int32, (rows, n * rows), 0)).astype(F32).astype(BF16)
    counts = jnp.dot(earlier, one_hot, preferred_element_type=F32)
    slot = jnp.sum(jnp.where(row_id == e_own, counts, 0.0), axis=-1, keepdims=True)
    keep_gate = jnp.where(slot < capacity, gate, 0.0)

    pad = jnp.zeros((128 - rows, width), F32)
    kt_ref[...] = jnp.concatenate([kv_ref[0], pad], axis=0).T
    vt_ref[...] = jnp.concatenate([kv_ref[1], pad], axis=0).T

    def patch_row(b, column, cache_ref):
        cache_ref[b] = jnp.where(lane == pos_ref[b], jnp.broadcast_to(column, (width, length)).astype(BF16), cache_ref[b])

    def patch_step(i, carry):
        kt = kt_ref[...]
        vt = vt_ref[...]
        for s in range(UNROLL):
            patch_row(i * UNROLL + s, kt[:, s:s + 1], k_ref)
            patch_row(i * UNROLL + s, vt[:, s:s + 1], v_ref)
        kt_ref[...] = pltpu.roll(kt, 128 - UNROLL, axis=1)
        vt_ref[...] = pltpu.roll(vt, 128 - UNROLL, axis=1)
        return carry
    lax.fori_loop(0, steps, patch_step, 0)

    all_of(yall_ref, peers, y_sem.at[0], y_sem.at[1], sib).wait_recv()
    x_all = yall_ref[...].reshape(n * rows, width)
    units = win_ref.shape[2]
    e_wide = jnp.concatenate([e_all] * (2 * units // 128), axis=1)
    second = (lax.broadcasted_iota(jnp.int32, (1, 2 * units), 1) >= units).astype(jnp.int32)
    for e in range(0, experts, 2):
        w_pair = jnp.concatenate([win_ref[e], win_ref[e + 1]], axis=1)
        u = jnp.maximum(jnp.dot(x_all, w_pair, preferred_element_type=F32), 0.0)
        u_ref[:, e * units:(e + 2) * units] = jnp.where(e_wide == e + second, u, 0.0).astype(BF16)

    chunk = part_ref.shape[4]
    parts = width // chunk
    chip, core = me // 2, lax.rem(me, 2)
    w_all = wout_ref.reshape(experts * units, width)
    for c in range(parts):
        acc = jnp.dot(u_ref[...], w_all[:, c * chunk:(c + 1) * chunk], preferred_element_type=F32)
        part_ref[c] = acc.reshape(n // 2, 2, rows, chunk)
        remote(part_ref.at[c, :, 1 - core], pair_ref.at[c], d_send.at[0], d_recv.at[c], sib).start()
    for c in range(parts):
        remote(pair_ref.at[c], pair_ref.at[c], d_send.at[0], d_recv.at[c], sib).wait_recv()
        pair_sum_ref[c] = part_ref[c, :, core] + pair_ref[c]
        rs_ref[c, chip] = pair_sum_ref[c, chip]
        for step in (2, 1, 3):
            target = lax.rem(chip + step, n // 2)
            remote(pair_sum_ref.at[c, target], rs_ref.at[c, chip], rs_send.at[0], rs_recv.at[c],
                   2 * target + core).start()
    others = n // 2 - 1
    for c in range(parts):
        all_of(rs_ref.at[c], others, rs_send.at[0], rs_recv.at[c], sib).wait_recv()
        y = jnp.sum(rs_ref[c], axis=0).astype(BF16).astype(F32)
        cols = slice(c * chunk, (c + 1) * chunk)
        out_ref[:, cols] = (h2[:, cols] + y * keep_gate).astype(BF16)
    for ref, sem in ((xall_ref, x_sem), (qrecv_ref, q_sem), (yall_ref, y_sem), (wr_ref, r_sem), (eall_ref, e_sem),
                     (wall_ref, w_send)):
        all_of(ref, peers, sem.at[0], sem.at[0], sib).wait_send()
    sent = rs_ref.at[:, pl.ds(0, others)]
    remote(sent, sent, rs_send.at[0], rs_send.at[0], sib).wait_send()
    remote(pair_ref, pair_ref, d_send.at[0], d_send.at[0], sib).wait_send()


def write_kernel(hid_ref, k_ref, v_ref, out_hbm, newk_hbm, newv_hbm, sem):
    span = k_ref.shape[0] // 4
    copies = [pltpu.make_async_copy(hid_ref, out_hbm, sem.at[8])]
    for i in range(4):
        rows = pl.ds(i * span, span)
        copies.append(pltpu.make_async_copy(k_ref.at[rows], newk_hbm.at[rows], sem.at[2 * i]))
        copies.append(pltpu.make_async_copy(v_ref.at[rows], newv_hbm.at[rows], sem.at[2 * i + 1]))
    for copy in copies:
        copy.start()
    for copy in copies:
        copy.wait()


def solution(mesh):
    n = mesh.shape['ws']
    row_axes = ('dp', 'ws')
    row_vec = P(row_axes)
    row_mat = P(row_axes, None)
    cache_spec = P(row_axes, None, None, None)
    col_split = P(None, 'ws')
    in_specs = (row_mat, cache_spec, cache_spec, cache_spec, cache_spec, row_vec, row_mat, P(None, None), row_vec,
                P(None), P(None), P(None), col_split, col_split, col_split, col_split, col_split, col_split,
                col_split, P(None, None, 'ws'), P(None, 'ws', None))
    out_specs = (row_mat, cache_spec, cache_spec)

    def decoder_block(hidden, self_k, self_v, cross_k, cross_v, positions, enc_mask, rel_bias, expert_idx,
                      ln_self, ln_cross, ln_ffn, wq_self, wk_self, wv_self, wo_self, wq_cross, wo_cross,
                      w_router, w_in, w_out):
        rows, width = hidden.shape
        heads, length, head_dim = self_k.shape[1:]
        src_len = cross_k.shape[2]
        share = width // n
        heads_pad = -(-heads // 16) * 16
        experts, _, units = w_in.shape
        capacity = (2 * rows * n + experts - 1) // experts
        chunk = 256

        def flat(cache):
            return jnp.swapaxes(cache, 2, 3).reshape(rows, width, cache.shape[2])

        dma = pltpu.SemaphoreType.DMA
        vmem, big_cache, big_src = pltpu.VMEM, (rows, width, length), (rows, width, src_len)
        parts, smem = width // chunk, pltpu.SMEM
        hid_out, k_v, v_v = pl.pallas_call(
            functools.partial(main_kernel, n, head_dim, capacity),
            out_shape=(vmem((rows, width), BF16), vmem(big_cache, BF16), vmem(big_cache, BF16)),
            in_specs=[HBM] * 21,
            out_specs=(VM,) * 3,
            scratch_shapes=[
                vmem(big_src, BF16), vmem(big_src, BF16), vmem(w_in.shape, BF16), vmem(w_out.shape, BF16),
                vmem((n, 3 * share, width), BF16),
                smem((rows,), jnp.int32), smem((rows,), jnp.int32), vmem((width,), F32), vmem((width,), F32),
                vmem((width,), F32), vmem((heads, length), F32), vmem((rows, src_len), jnp.int32),
                vmem((n, 1, width), F32), vmem((n, 1, 128), jnp.int32), vmem((n, rows, width), BF16),
                vmem((n, rows, width), BF16), vmem((rows, width), BF16), vmem((3, share, width), BF16),
                vmem((n * rows, 384), BF16), vmem((n, rows, 384), BF16), vmem((rows, width), F32),
                vmem((2, rows, width), F32), vmem((width, 128), F32), vmem((width, 128), F32),
                vmem((rows, heads_pad, length), F32), vmem((rows, heads_pad, length), BF16),
                vmem((rows, heads_pad, src_len), F32), vmem((rows, heads_pad, src_len), BF16), vmem((rows, width), F32),
                vmem((heads_pad, length), F32), vmem((n * rows, experts * units), BF16),
                vmem((parts, n // 2, 2, rows, chunk), F32), vmem((parts, n // 2, rows, chunk), F32),
                vmem((parts, n // 2, rows, chunk), F32), vmem((parts, n // 2, rows, chunk), F32),
                dma((12,)), dma((6,)), dma((5,)), dma((2,)), dma((2,)), dma((2,)), dma((2,)), dma((1,)), dma((3, 6)),
                dma((3,)), dma((1,)), dma((parts,)), dma((1,)), dma((parts,)),
            ],
            compiler_params=pltpu.CompilerParams(collective_id=0, has_side_effects=True,
                                                 vmem_limit_bytes=34 * 2 ** 20),
            name='main_part',
        )(*in_hbm(positions, expert_idx, hidden, ln_self, ln_cross, ln_ffn, rel_bias, enc_mask, w_router.T, wq_self.T,
                  wk_self.T, wv_self.T, wo_self.T, wq_cross.T, wo_cross.T, flat(self_k), flat(self_v), flat(cross_k),
                  flat(cross_v), w_in, w_out))

        out, newk, newv = pl.pallas_call(
            write_kernel,
            out_shape=(pltpu.HBM((rows, width), BF16), pltpu.HBM(big_cache, BF16), pltpu.HBM(big_cache, BF16)),
            in_specs=[VM] * 3,
            out_specs=(HBM,) * 3,
            scratch_shapes=[dma((9,))],
            compiler_params=pltpu.CompilerParams(has_side_effects=True, vmem_limit_bytes=2 ** 20),
            name='write_part',
        )(*in_vmem(hid_out, k_v, v_v))

        def unflat(cache):
            return jnp.swapaxes(cache.reshape(rows, heads, head_dim, length), 2, 3)
        return out, unflat(newk), unflat(newv)

    return jax.shard_map(decoder_block, mesh=mesh, in_specs=in_specs, out_specs=out_specs, check_vma=False)
```

```python
import functools
import jax
import jax.numpy as jnp
from jax import lax
from jax.experimental import pallas as pl
from jax.experimental.pallas import tpu as pltpu
from jax.sharding import PartitionSpec as P

EPSILON = 1e-6
NEG_BIG = -1e30
F32, BF16 = jnp.float32, jnp.bfloat16
BF16_MAX = float(jnp.finfo(jnp.bfloat16).max)
MESH = pl.DeviceIdType.MESH
VM = pl.BlockSpec(memory_space=pltpu.VMEM)
HBM = pl.BlockSpec(memory_space=pltpu.HBM)
NT = (((1,), (1,)), ((), ()))
FROM_LEFT, FROM_RIGHT, FROM_FAR = 0, 1, 2
PEERS = ((2, 0), (2, 1), (1, 0), (3, 0), (1, 1), (3, 1), (0, 1))
UNROLL = 8


def in_hbm(*arrays):
    return [pltpu.with_memory_space_constraint(a, pltpu.HBM) for a in arrays]


def in_vmem(*arrays):
    return [pltpu.with_memory_space_constraint(a, pltpu.VMEM) for a in arrays]


def rms_norm(hid_f32, scale):
    inv_rms = lax.rsqrt(jnp.mean(hid_f32 * hid_f32, axis=-1, keepdims=True) + EPSILON)
    return (hid_f32 * inv_rms * scale).astype(BF16)


def dot_nt(a, b):
    return lax.dot_general(a, b, NT, preferred_element_type=F32)


def softmax_rows(scores):
    top = jnp.max(scores, axis=-1, keepdims=True)
    ex = jnp.exp(scores - top)
    return (ex / jnp.sum(ex, axis=-1, keepdims=True)).astype(BF16)


def make_dev(n):
    me = lax.axis_index('ws')
    chips = n // 2
    chip, core = me // 2, lax.rem(me, 2)

    def dev(step, other):
        return 2 * lax.rem(chip + step, chips) + ((1 - core) if other else core)
    return me, dev


def remote(src, dst, send_sem, recv_sem, dev):
    return pltpu.make_async_remote_copy(src_ref=src, dst_ref=dst, send_sem=send_sem, recv_sem=recv_sem,
                                        device_id={'ws': dev}, device_id_type=MESH)


def to_peers(dev, me, ref, send_sem, recv_sem):
    return [remote(ref.at[me], ref.at[me], send_sem, recv_sem, dev(*peer)) for peer in PEERS]


def all_of(ref, count, send_sem, recv_sem, dev):
    block = ref.at[pl.ds(0, count)]
    return remote(block, block, send_sem, recv_sem, dev)


def head_mask(heads_pad, width, head_dim):
    row = lax.broadcasted_iota(jnp.int32, (heads_pad, width), 0)
    col = lax.broadcasted_iota(jnp.int32, (heads_pad, width), 1)
    return (col // head_dim == row).astype(F32)


def main_kernel(n, head_dim, capacity, pos_hbm, eidx_hbm, hid_hbm, ln_hbm, lnc_hbm, lnf_hbm, rel_hbm, mask_hbm, wr_hbm,
                wq_hbm, wk_hbm, wv_hbm, wo_hbm, wqc_hbm, woc_hbm, k_hbm, v_hbm, ck_hbm, cv_hbm, win_hbm, wout_hbm,
                out_ref, k_ref, v_ref,
                ck_ref, cv_ref, win_ref, wout_ref, wall_ref, pos_ref, eidx_ref, ln_ref, lnc_ref, lnf_ref, rel_ref, mask_ref, wr_ref, eall_ref, xall_ref, yall_ref, hid_ref,
                wqkv_ref, qsend_ref, qrecv_ref, q_ref, kv_ref, kt_ref, vt_ref, s_ref, p_ref, s2_ref, p2_ref, ctx32_ref,
                rrev_ref, u_ref, part_ref, pair_ref, pair_sum_ref, rs_ref,
                in_sem, big_sem, x_sem, r_sem, e_sem, q_sem, y_sem, w_send, w_recv, pair_recv, d_send, d_recv, rs_send, rs_recv):
    me, dev = make_dev(n)
    rows, width, length = k_ref.shape
    heads_pad = s_ref.shape[1]
    share = width // n
    half = share // 2
    steps = rows // UNROLL
    peers = len(PEERS)

    barrier = pltpu.get_barrier_semaphore()
    for peer in PEERS:
        pl.semaphore_signal(barrier, inc=1, device_id={'ws': dev(*peer)}, device_id_type=MESH)

    mine = wall_ref.at[me]
    loads = [
        (hid_hbm, xall_ref.at[me], 0), (wr_hbm, wr_ref.at[me], 1), (ln_hbm, ln_ref, 2), (wq_hbm, wqkv_ref.at[0], 3),
        (wk_hbm, wqkv_ref.at[1], 3), (wv_hbm, wqkv_ref.at[2], 3), (rel_hbm, rel_ref, 4),
        (wo_hbm, mine.at[pl.ds(0, share)], 5), (wqc_hbm, mine.at[pl.ds(share, share)], 5),
        (woc_hbm, mine.at[pl.ds(2 * share, share)], 5), (eidx_hbm, eidx_ref, 6), (pos_hbm, pos_ref, 7),
        (lnc_hbm, lnc_ref, 8), (lnf_hbm, lnf_ref, 9), (mask_hbm, mask_ref, 10), (hid_hbm, hid_ref, 11),
    ]
    loads = [pltpu.make_async_copy(src, dst, in_sem.at[i]) for src, dst, i in loads]
    for load in loads:
        load.start()
    experts = win_ref.shape[0]
    lane_id = lax.broadcasted_iota(jnp.int32, (1, 128), 1)
    loads[0].wait()
    pl.semaphore_wait(barrier, n - 1)
    right, left, far, sib = dev(1, 0), dev(3, 0), dev(2, 0), dev(0, 1)

    def send_rows(owner, sem, target):
        remote(xall_ref.at[owner], xall_ref.at[owner], x_sem.at[0], x_sem.at[sem], target).start()

    def rows_over(owner, sem):
        remote(xall_ref.at[owner], xall_ref.at[owner], x_sem.at[0], x_sem.at[sem], sib).wait_recv()
        send_rows(owner, 4, sib)

    send_rows(me, 3, far)
    send_rows(me, 1, right)
    send_rows(me, 2, left)
    send_rows(me, 4, sib)
    pltpu.make_async_copy(mine, mine, in_sem.at[5]).wait()

    def half_of(owner, part):
        return wall_ref.at[owner, pl.ds(part * half, half)]

    def send_piece(owner, role, part, target):
        sem = pair_recv.at[part // 2] if role is None else w_recv.at[role, part]
        remote(half_of(owner, part), half_of(owner, part), w_send.at[0], sem, target).start()

    def wait_piece(owner, role, part):
        remote(half_of(owner, part), half_of(owner, part), w_send.at[0], w_recv.at[role, part], sib).wait_recv()

    def wait_pair(stage):
        block = wall_ref.at[pl.ds(0, n // 2), pl.ds(stage * share, share)]
        remote(block, block, w_send.at[0], pair_recv.at[stage], sib).wait_recv()

    def pass_on(first):
        wait_piece(left, FROM_LEFT, first)
        send_piece(left, FROM_FAR, first, right)
        wait_piece(right, FROM_RIGHT, first + 1)
        send_piece(right, FROM_FAR, first + 1, left)

    def send_own(*parts):
        for part in parts:
            send_piece(me, FROM_LEFT, part, right)
            send_piece(me, FROM_RIGHT, part + 1 if part % 2 == 0 else part - 1, left)

    send_own(0, 1, 2)
    loads[1].wait()
    loads[10].wait()
    e_row = jnp.zeros((1, 128), jnp.int32)
    for b in range(rows):
        e_row = jnp.where(lane_id == b, eidx_ref[b], e_row)
    eall_ref[me] = e_row
    big = [pltpu.make_async_copy(src, dst, big_sem.at[i]) for i, (src, dst) in
           enumerate([(k_hbm, k_ref), (v_hbm, v_ref), (ck_hbm, ck_ref), (cv_hbm, cv_ref), (win_hbm, win_ref), (wout_hbm, wout_ref)])]
    for load in big:
        load.start()

    loads[6].wait()
    rel = jnp.concatenate([rel_ref[...], jnp.zeros((heads_pad - rel_ref.shape[0], length), F32)], axis=0)
    flip = (lax.broadcasted_iota(jnp.int32, (length, length), 0) + lax.broadcasted_iota(jnp.int32, (length, length), 1)
            == length - 1).astype(F32).astype(BF16)
    hi = jnp.clip(rel, -BF16_MAX, BF16_MAX).astype(BF16)
    rest = rel - hi.astype(F32)
    mid = rest.astype(BF16)
    low = (rest - mid.astype(F32)).astype(BF16)
    rrev_ref[...] = (jnp.dot(hi, flip, preferred_element_type=F32) + jnp.dot(mid, flip, preferred_element_type=F32)
                     + jnp.dot(low, flip, preferred_element_type=F32))
    qsend_ref[...] = jnp.zeros_like(qsend_ref)

    rows_over(left, 1)
    rows_over(right, 2)
    for load in loads[2:3] + loads[11:]:
        load.wait()
    pltpu.make_async_copy(wqkv_ref, wqkv_ref, in_sem.at[3]).wait()
    rows_over(far, 3)
    all_of(xall_ref, n // 2, x_sem.at[0], x_sem.at[4], sib).wait_recv()
    x_norm = rms_norm(xall_ref[...].reshape(n * rows, width).astype(F32), ln_ref[...][None])
    for part in range(3):
        qsend_ref[:, part * 128:part * 128 + share] = dot_nt(x_norm, wqkv_ref[part]).astype(BF16)
    for peer in PEERS:
        dst = dev(*peer)
        remote(qsend_ref.at[pl.ds(dst * rows, rows)], qrecv_ref.at[me], q_sem.at[0], q_sem.at[1], dst).start()
    qrecv_ref[me] = qsend_ref[pl.ds(pl.multiple_of(me * rows, rows), rows), :]
    pass_on(0)
    send_own(3)
    for part in range(6):
        send_piece(me, None, part, sib)

    all_of(qrecv_ref, peers, q_sem.at[0], q_sem.at[1], sib).wait_recv()
    def far_over(first):
        for part in (first, first + 1):
            wait_piece(far, FROM_FAR, part)
            send_piece(far, None, part, sib)

    pass_on(2)
    send_own(4, 5)
    for copy in (to_peers(dev, me, wr_ref, r_sem.at[0], r_sem.at[1])
                 + to_peers(dev, me, eall_ref, e_sem.at[0], e_sem.at[1])):
        copy.start()
    wait_piece(left, FROM_LEFT, 1)
    wait_piece(right, FROM_RIGHT, 0)
    for part in (0, 1):
        send_piece(left, None, part, sib)
        send_piece(right, None, part, sib)
    send_piece(left, None, 2, sib)
    send_piece(right, None, 3, sib)

    def columns(part):
        return jnp.concatenate([qrecv_ref[s][:, part * 128:part * 128 + share] for s in range(n)], axis=1).astype(F32)
    q_ref[...] = columns(0)
    kv_ref[0] = columns(1)
    kv_ref[1] = columns(2)

    h_mask = head_mask(heads_pad, width, head_dim)
    lane = lax.broadcasted_iota(jnp.int32, (1, length), 1)

    big[0].wait()

    def score_step(i, carry):
        for s in range(UNROLL):
            b = i * UNROLL + s
            pos = pos_ref[b]
            q_diag = q_ref[pl.ds(b, 1), :] * h_mask
            scores = jnp.dot(q_diag.astype(BF16), k_ref[b], preferred_element_type=F32)
            new = jnp.sum(q_diag * kv_ref[0, pl.ds(b, 1), :], axis=1, keepdims=True)
            bias = pltpu.roll(rrev_ref[...], pos + 1, axis=1)
            s_ref[b] = jnp.where(lane <= pos, jnp.where(lane == pos, new, scores) + bias, NEG_BIG)
        return carry
    lax.fori_loop(0, steps, score_step, 0)

    p_ref[...] = softmax_rows(s_ref[...])

    big[1].wait()

    def value_step(i, carry):
        for s in range(UNROLL):
            b = i * UNROLL + s
            here = lane == pos_ref[b]
            probs = p_ref[b].astype(F32)
            new = jnp.sum(jnp.where(here, probs, 0.0), axis=1, keepdims=True)
            spread = dot_nt(jnp.where(here, 0.0, probs).astype(BF16), v_ref[b])
            spread = spread + new * kv_ref[1, pl.ds(b, 1), :]
            ctx32_ref[pl.ds(b, 1), :] = jnp.sum(jnp.where(h_mask > 0, spread, 0.0), axis=0, keepdims=True)
        return carry
    lax.fori_loop(0, steps // 2, value_step, 0)
    far_over(0)
    wait_piece(left, FROM_LEFT, 3)
    send_piece(left, None, 3, sib)
    wait_piece(right, FROM_RIGHT, 2)
    send_piece(right, None, 2, sib)
    lax.fori_loop(steps // 2, steps, value_step, 0)

    far_over(2)
    wait_pair(0)
    wo = wall_ref[:, 0:share, :].reshape(width, width)
    h1 = (hid_ref[...].astype(F32) + dot_nt(ctx32_ref[...].astype(BF16), wo)).astype(BF16).astype(F32)
    pass_on(4)
    send_piece(left, None, 4, sib)
    send_piece(right, None, 5, sib)
    wait_pair(1)
    wqc = wall_ref[:, share:2 * share, :].reshape(width, width)
    q_ref[...] = dot_nt(rms_norm(h1, lnc_ref[...][None]), wqc).astype(BF16).astype(F32)
    for load in big[2:]:
        load.wait()

    def cross_score(i, carry):
        for s in range(UNROLL):
            b = i * UNROLL + s
            q_diag = (q_ref[pl.ds(b, 1), :] * h_mask).astype(BF16)
            scores = jnp.dot(q_diag, ck_ref[b], preferred_element_type=F32)
            s2_ref[b] = jnp.where(mask_ref[pl.ds(b, 1), :] == 1, scores, NEG_BIG)
        return carry
    lax.fori_loop(0, steps, cross_score, 0)
    wait_piece(left, FROM_LEFT, 5)
    send_piece(left, None, 5, sib)
    wait_piece(right, FROM_RIGHT, 4)
    send_piece(right, None, 4, sib)
    p2_ref[...] = softmax_rows(s2_ref[...])

    def cross_value(i, carry):
        for s in range(UNROLL):
            b = i * UNROLL + s
            spread = dot_nt(p2_ref[b], cv_ref[b])
            ctx32_ref[pl.ds(b, 1), :] = jnp.sum(jnp.where(h_mask > 0, spread, 0.0), axis=0, keepdims=True)
        return carry
    lax.fori_loop(0, steps // 2, cross_value, 0)
    far_over(4)
    lax.fori_loop(steps // 2, steps, cross_value, 0)

    wait_pair(2)
    woc = wall_ref[:, 2 * share:3 * share, :].reshape(width, width)
    h2 = (h1 + dot_nt(ctx32_ref[...].astype(BF16), woc)).astype(BF16).astype(F32)
    x_own = rms_norm(h2, lnf_ref[...][None])
    yall_ref[me] = x_own
    for copy in to_peers(dev, me, yall_ref, y_sem.at[0], y_sem.at[1]):
        copy.start()

    all_of(wr_ref, peers, r_sem.at[0], r_sem.at[1], sib).wait_recv()
    all_of(eall_ref, peers, e_sem.at[0], e_sem.at[1], sib).wait_recv()
    x_f32 = x_own.astype(F32)
    logits = [jnp.sum(x_f32 * wr_ref[e], axis=-1, keepdims=True) for e in range(experts)]
    top = functools.reduce(jnp.maximum, logits)
    ex = [jnp.exp(v - top) for v in logits]
    total = functools.reduce(jnp.add, ex)
    e_pad = jnp.concatenate([eall_ref[...].reshape(n, 128), jnp.zeros((128 - n, 128), jnp.int32)], axis=0)
    e_cols = e_pad.astype(F32).T.astype(jnp.int32)
    e_all = jnp.concatenate([jnp.broadcast_to(e_cols[0:rows, s:s + 1], (rows, 128)) for s in range(n)], axis=0)
    row_id = lax.broadcasted_iota(jnp.int32, (rows, 128), 1)
    source = lax.broadcasted_iota(jnp.int32, (rows, 128), 1)
    e_own = jnp.sum(jnp.where(source == me, e_cols[0:rows, :], 0).astype(F32), axis=1, keepdims=True).astype(jnp.int32)
    gate = functools.reduce(jnp.add, [jnp.where(e_own == e, ex[e], 0.0) for e in range(experts)]) / total
    one_hot = (e_all == lax.broadcasted_iota(jnp.int32, (n * rows, 128), 1)).astype(F32).astype(BF16)
    earlier = (lax.broadcasted_iota(jnp.int32, (rows, n * rows), 1)
               < me * rows + lax.broadcasted_iota(jnp.int32, (rows, n * rows), 0)).astype(F32).astype(BF16)
    counts = jnp.dot(earlier, one_hot, preferred_element_type=F32)
    slot = jnp.sum(jnp.where(row_id == e_own, counts, 0.0), axis=-1, keepdims=True)
    keep_gate = jnp.where(slot < capacity, gate, 0.0)

    pad = jnp.zeros((128 - rows, width), F32)
    kt_ref[...] = jnp.concatenate([kv_ref[0], pad], axis=0).T
    vt_ref[...] = jnp.concatenate([kv_ref[1], pad], axis=0).T

    def patch_row(b, column, cache_ref):
        cache_ref[b] = jnp.where(lane == pos_ref[b], jnp.broadcast_to(column, (width, length)).astype(BF16), cache_ref[b])

    def patch_step(i, carry):
        kt = kt_ref[...]
        vt = vt_ref[...]
        for s in range(UNROLL):
            patch_row(i * UNROLL + s, kt[:, s:s + 1], k_ref)
            patch_row(i * UNROLL + s, vt[:, s:s + 1], v_ref)
        kt_ref[...] = pltpu.roll(kt, 128 - UNROLL, axis=1)
        vt_ref[...] = pltpu.roll(vt, 128 - UNROLL, axis=1)
        return carry
    lax.fori_loop(0, steps, patch_step, 0)

    all_of(yall_ref, peers, y_sem.at[0], y_sem.at[1], sib).wait_recv()
    x_all = yall_ref[...].reshape(n * rows, width)
    units = win_ref.shape[2]
    e_wide = jnp.concatenate([e_all] * (2 * units // 128), axis=1)
    second = (lax.broadcasted_iota(jnp.int32, (1, 2 * units), 1) >= units).astype(jnp.int32)
    for e in range(0, experts, 2):
        w_pair = jnp.concatenate([win_ref[e], win_ref[e + 1]], axis=1)
        u = jnp.maximum(jnp.dot(x_all, w_pair, preferred_element_type=F32), 0.0)
        u_ref[:, e * units:(e + 2) * units] = jnp.where(e_wide == e + second, u, 0.0).astype(BF16)

    chunk = part_ref.shape[4]
    parts = width // chunk
    chip, core = me // 2, lax.rem(me, 2)
    w_all = wout_ref.reshape(experts * units, width)
    for c in range(parts):
        acc = jnp.dot(u_ref[...], w_all[:, c * chunk:(c + 1) * chunk], preferred_element_type=F32)
        part_ref[c] = acc.reshape(n // 2, 2, rows, chunk)
        remote(part_ref.at[c, :, 1 - core], pair_ref.at[c], d_send.at[0], d_recv.at[c], sib).start()
    for c in range(parts):
        remote(pair_ref.at[c], pair_ref.at[c], d_send.at[0], d_recv.at[c], sib).wait_recv()
        pair_sum_ref[c] = part_ref[c, :, core] + pair_ref[c]
        rs_ref[c, chip] = pair_sum_ref[c, chip]
        for step in (2, 1, 3):
            target = lax.rem(chip + step, n // 2)
            remote(pair_sum_ref.at[c, target], rs_ref.at[c, chip], rs_send.at[0], rs_recv.at[c],
                   2 * target + core).start()
    others = n // 2 - 1
    for c in range(parts):
        all_of(rs_ref.at[c], others, rs_send.at[0], rs_recv.at[c], sib).wait_recv()
        y = jnp.sum(rs_ref[c], axis=0).astype(BF16).astype(F32)
        cols = slice(c * chunk, (c + 1) * chunk)
        out_ref[:, cols] = (h2[:, cols] + y * keep_gate).astype(BF16)
    for ref, sem in ((xall_ref, x_sem), (qrecv_ref, q_sem), (yall_ref, y_sem), (wr_ref, r_sem), (eall_ref, e_sem),
                     (wall_ref, w_send)):
        all_of(ref, peers, sem.at[0], sem.at[0], sib).wait_send()
    sent = rs_ref.at[:, pl.ds(0, others)]
    remote(sent, sent, rs_send.at[0], rs_send.at[0], sib).wait_send()
    remote(pair_ref, pair_ref, d_send.at[0], d_send.at[0], sib).wait_send()


def write_kernel(hid_ref, k_ref, v_ref, out_hbm, newk_hbm, newv_hbm, sem):
    span = k_ref.shape[0] // 4
    copies = [pltpu.make_async_copy(hid_ref, out_hbm, sem.at[8])]
    for i in range(4):
        rows = pl.ds(i * span, span)
        copies.append(pltpu.make_async_copy(k_ref.at[rows], newk_hbm.at[rows], sem.at[2 * i]))
        copies.append(pltpu.make_async_copy(v_ref.at[rows], newv_hbm.at[rows], sem.at[2 * i + 1]))
    for copy in copies:
        copy.start()
    for copy in copies:
        copy.wait()


def solution(mesh):
    n = mesh.shape['ws']
    row_axes = ('dp', 'ws')
    row_vec = P(row_axes)
    row_mat = P(row_axes, None)
    cache_spec = P(row_axes, None, None, None)
    col_split = P(None, 'ws')
    in_specs = (row_mat, cache_spec, cache_spec, cache_spec, cache_spec, row_vec, row_mat, P(None, None), row_vec,
                P(None), P(None), P(None), col_split, col_split, col_split, col_split, col_split, col_split,
                col_split, P(None, None, 'ws'), P(None, 'ws', None))
    out_specs = (row_mat, cache_spec, cache_spec)

    def decoder_block(hidden, self_k, self_v, cross_k, cross_v, positions, enc_mask, rel_bias, expert_idx,
                      ln_self, ln_cross, ln_ffn, wq_self, wk_self, wv_self, wo_self, wq_cross, wo_cross,
                      w_router, w_in, w_out):
        rows, width = hidden.shape
        heads, length, head_dim = self_k.shape[1:]
        src_len = cross_k.shape[2]
        share = width // n
        heads_pad = -(-heads // 16) * 16
        experts, _, units = w_in.shape
        capacity = (2 * rows * n + experts - 1) // experts
        chunk = 256

        def flat(cache):
            return jnp.swapaxes(cache, 2, 3).reshape(rows, width, cache.shape[2])

        dma = pltpu.SemaphoreType.DMA
        vmem, big_cache, big_src = pltpu.VMEM, (rows, width, length), (rows, width, src_len)
        parts, smem = width // chunk, pltpu.SMEM
        hid_out, k_v, v_v = pl.pallas_call(
            functools.partial(main_kernel, n, head_dim, capacity),
            out_shape=(vmem((rows, width), BF16), vmem(big_cache, BF16), vmem(big_cache, BF16)),
            in_specs=[HBM] * 21,
            out_specs=(VM,) * 3,
            scratch_shapes=[
                vmem(big_src, BF16), vmem(big_src, BF16), vmem(w_in.shape, BF16), vmem(w_out.shape, BF16),
                vmem((n, 3 * share, width), BF16),
                smem((rows,), jnp.int32), smem((rows,), jnp.int32), vmem((width,), F32), vmem((width,), F32),
                vmem((width,), F32), vmem((heads, length), F32), vmem((rows, src_len), jnp.int32),
                vmem((n, 1, width), F32), vmem((n, 1, 128), jnp.int32), vmem((n, rows, width), BF16),
                vmem((n, rows, width), BF16), vmem((rows, width), BF16), vmem((3, share, width), BF16),
                vmem((n * rows, 384), BF16), vmem((n, rows, 384), BF16), vmem((rows, width), F32),
                vmem((2, rows, width), F32), vmem((width, 128), F32), vmem((width, 128), F32),
                vmem((rows, heads_pad, length), F32), vmem((rows, heads_pad, length), BF16),
                vmem((rows, heads_pad, src_len), F32), vmem((rows, heads_pad, src_len), BF16), vmem((rows, width), F32),
                vmem((heads_pad, length), F32), vmem((n * rows, experts * units), BF16),
                vmem((parts, n // 2, 2, rows, chunk), F32), vmem((parts, n // 2, rows, chunk), F32),
                vmem((parts, n // 2, rows, chunk), F32), vmem((parts, n // 2, rows, chunk), F32),
                dma((12,)), dma((6,)), dma((5,)), dma((2,)), dma((2,)), dma((2,)), dma((2,)), dma((1,)), dma((3, 6)),
                dma((3,)), dma((1,)), dma((parts,)), dma((1,)), dma((parts,)),
            ],
            compiler_params=pltpu.CompilerParams(collective_id=0, has_side_effects=True,
                                                 vmem_limit_bytes=34 * 2 ** 20),
            name='main_part',
        )(*in_hbm(positions, expert_idx, hidden, ln_self, ln_cross, ln_ffn, rel_bias, enc_mask, w_router.T, wq_self.T,
                  wk_self.T, wv_self.T, wo_self.T, wq_cross.T, wo_cross.T, flat(self_k), flat(self_v), flat(cross_k),
                  flat(cross_v), w_in, w_out))

        out, newk, newv = pl.pallas_call(
            write_kernel,
            out_shape=(pltpu.HBM((rows, width), BF16), pltpu.HBM(big_cache, BF16), pltpu.HBM(big_cache, BF16)),
            in_specs=[VM] * 3,
            out_specs=(HBM,) * 3,
            scratch_shapes=[dma((9,))],
            compiler_params=pltpu.CompilerParams(has_side_effects=True, vmem_limit_bytes=2 ** 20),
            name='write_part',
        )(*in_vmem(hid_out, k_v, v_v))

        def unflat(cache):
            return jnp.swapaxes(cache.reshape(rows, heads, head_dim, length), 2, 3)
        return out, unflat(newk), unflat(newv)

    return jax.shard_map(decoder_block, mesh=mesh, in_specs=in_specs, out_specs=out_specs, check_vma=False)
```
